32 devices in a mesh: dp: 32 (over z, y, x, core).
Axes of the slice: x: 2, y: 2, z: 4, core: 2. Of those that a mesh axis runs over, the one named last changes fastest.
Arguments:
- weights: float32 [790528], P('dp')
- moment_one: float32 [790528], P('dp')
- moment_two: float32 [790528], P('dp')
- x_qkv: bfloat16 [131072, 256], P('dp')
- dy_qkv: bfloat16 [131072, 768], P('dp')
- x_proj: bfloat16 [131072, 256], P('dp')
- dy_proj: bfloat16 [131072, 256], P('dp')
- x_inter: bfloat16 [131072, 256], P('dp')
- dy_inter: bfloat16 [131072, 1024], P('dp')
- x_out: bfloat16 [131072, 1024], P('dp')
- dy_out: bfloat16 [131072, 256], P('dp')
- ln_grad: float32 [32, 4, 256], P('dp')
Outputs:
- output 1: float32 [790528], P('dp')
- output 2: float32 [790528], P('dp')
- output 3: float32 [790528], P('dp')
- output 4: bfloat16 [790528], replicated
All inputs are finite; a program needn't handle non-finite values.
Results may differ from the reference program's by a relative error of at most 0.001.
Values sent between devices are 32-bit elements.
A program may use at most 1 GiB of HBM per device.

```python
import jax
import jax.numpy as jnp

D = 256
REPLICAS = 32
TOKENS = 4096
NPAD = 790528
STEP = 10

LEARN_RATE = 0.5
BETA_ONE = 0.9
BETA_TWO = 0.999
EPSILON = 1e-6
DECAY = 0.01
CORR_ONE = 1.0 - BETA_ONE ** STEP
CORR_TWO = 1.0 - BETA_TWO ** STEP
TENSOR_SIZES = [3 * D * D, 3 * D, D * D, D, D, D, 4 * D * D, 4 * D, 4 * D * D, D, D, D]
NPARAM = sum(TENSOR_SIZES)
NUM_SEGS = len(TENSOR_SIZES) + 1
TENSOR_STARTS = [sum(TENSOR_SIZES[:tensor_index]) for tensor_index in range(len(TENSOR_SIZES))]
DECAY_FLAGS = [1.0, 0.0, 1.0, 0.0, 0.0, 0.0, 1.0, 0.0, 1.0, 0.0, 0.0, 0.0, 0.0]
WEIGHT_SCALES = [1.0, 0.1, 0.4, 0.2, 3.0, 0.3, 0.7, 0.15, 0.35, 0.25, 2.0, 0.5]
LN_BOOST = 30.0
GRAD_VAR = [1.0, 1.0, 1.0, 1.0, LN_BOOST ** 2, LN_BOOST ** 2, 1.0, 1.0, 1.0, 1.0, LN_BOOST ** 2, LN_BOOST ** 2]
GRAD_VAR_TOTAL = sum(tensor_size * var_factor for tensor_size, var_factor in zip(TENSOR_SIZES, GRAD_VAR))


def segment_ids():
    pieces = [jnp.full((tensor_size,), tensor_index, jnp.int32) for tensor_index, tensor_size in enumerate(TENSOR_SIZES)]
    pieces.append(jnp.full((NPAD - NPARAM,), NUM_SEGS - 1, jnp.int32))
    return jnp.concatenate(pieces)


def setup_inputs(seed: int = 0) -> dict:
    key_list = jax.random.split(jax.random.key(seed), 12)
    seg_ids = segment_ids()
    row_count = REPLICAS * TOKENS
    starts = jnp.asarray(TENSOR_STARTS + [NPARAM], jnp.float32)[seg_ids]
    lengths = jnp.asarray(TENSOR_SIZES + [1], jnp.float32)[seg_ids]
    position_frac = jnp.clip((jnp.arange(NPAD, dtype=jnp.float32) - starts) / lengths, 0.0, 1.0)
    weight_ramp = 0.25 + 3.0 * position_frac * position_frac
    weight_scale = jnp.asarray(WEIGHT_SCALES + [0.0], jnp.float32)[seg_ids] * weight_ramp * D ** -0.5
    grad_var = jnp.asarray(GRAD_VAR + [0.0], jnp.float32)[seg_ids] / GRAD_VAR_TOTAL
    weights = weight_scale * jax.random.normal(key_list[0], (NPAD,), jnp.float32)
    moment_one = 0.2 * jnp.sqrt(grad_var) * jax.random.normal(key_list[1], (NPAD,), jnp.float32)
    moment_two = 0.001 * grad_var * (0.5 + jax.random.uniform(key_list[2], (NPAD,), jnp.float32))
    act_widths = [D, 3 * D, D, D, D, 4 * D, 4 * D, D]
    act_list = [jax.random.normal(key_list[3 + act_index], (row_count, act_width), jnp.float32).astype(jnp.bfloat16) for act_index, act_width in enumerate(act_widths)]
    ln_grad = LN_BOOST * TOKENS ** 0.5 * jax.random.normal(key_list[11], (REPLICAS, 4, D), jnp.float32)
    return {'weights': weights, 'moment_one': moment_one, 'moment_two': moment_two,
            'x_qkv': act_list[0], 'dy_qkv': act_list[1], 'x_proj': act_list[2], 'dy_proj': act_list[3],
            'x_inter': act_list[4], 'dy_inter': act_list[5], 'x_out': act_list[6], 'dy_out': act_list[7],
            'ln_grad': ln_grad}


def weight_grad(x_rows, dy_rows):
    return jnp.dot(x_rows.T, dy_rows, preferred_element_type=jnp.float32)


def bias_grad(dy_rows):
    return jnp.sum(dy_rows.astype(jnp.float32), axis=0)


def reference(weights, moment_one, moment_two, x_qkv, dy_qkv, x_proj, dy_proj, x_inter, dy_inter, x_out, dy_out, ln_grad):
    ln_sum = jnp.sum(ln_grad, axis=0)
    pieces = [weight_grad(x_qkv, dy_qkv), bias_grad(dy_qkv), weight_grad(x_proj, dy_proj), bias_grad(dy_proj),
              ln_sum[0], ln_sum[1], weight_grad(x_inter, dy_inter), bias_grad(dy_inter),
              weight_grad(x_out, dy_out), bias_grad(dy_out), ln_sum[2], ln_sum[3]]
    flat_grad = jnp.concatenate([grad_piece.reshape(-1) for grad_piece in pieces] + [jnp.zeros((NPAD - NPARAM,), jnp.float32)])
    mean_grad = flat_grad / REPLICAS
    grad_norm = jnp.sqrt(jnp.sum(mean_grad * mean_grad))
    grad_hat = mean_grad / jnp.maximum(1.0, grad_norm)
    new_m = BETA_ONE * moment_one + (1.0 - BETA_ONE) * grad_hat
    new_v = BETA_TWO * moment_two + (1.0 - BETA_TWO) * grad_hat * grad_hat
    seg_ids = segment_ids()
    decay_mask = jnp.asarray(DECAY_FLAGS, jnp.float32)[seg_ids]
    update = (new_m / CORR_ONE) / (jnp.sqrt(new_v / CORR_TWO) + EPSILON) + DECAY * decay_mask * weights
    w_norm = jnp.sqrt(jax.ops.segment_sum(weights * weights, seg_ids, num_segments=NUM_SEGS))
    u_norm = jnp.sqrt(jax.ops.segment_sum(update * update, seg_ids, num_segments=NUM_SEGS))
    both_pos = (w_norm > 0) & (u_norm > 0)
    trust_vec = jnp.where(both_pos, w_norm / jnp.where(u_norm > 0, u_norm, 1.0), 1.0)
    new_w = weights - LEARN_RATE * trust_vec[seg_ids] * update
    return new_w, new_m, new_v, new_w.astype(jnp.bfloat16)
```

```python
import functools

import jax
import jax.numpy as jnp
from jax import lax
from jax.experimental import pallas as pl
from jax.experimental.pallas import tpu as pltpu
from jax.sharding import PartitionSpec as P

STEP = 10
LEARN_RATE = 0.5
BETA_ONE = 0.9
BETA_TWO = 0.999
EPSILON = 1e-6
DECAY = 0.01
CORR_ONE = 1.0 - BETA_ONE ** STEP
CORR_TWO = 1.0 - BETA_TWO ** STEP

LANES = 128
CHUNKS = 4
PARTS = 4
F32 = jnp.float32
BF16 = jnp.bfloat16


def tensor_sizes(width):
    return [3 * width * width, 3 * width, width * width, width, width, width,
            4 * width * width, 4 * width, 4 * width * width, width, width, width]


def row_ends(width):
    ends, total = [], 0
    for size in tensor_sizes(width):
        total += size // LANES
        ends.append(total)
    return ends


def comm_kernel(dims, x_qkv, dy_qkv, x_proj, dy_proj, x_inter, dy_inter, x_out, dy_out, ln, w_in, m_in, v_in,
                nw_out, nm_out, nv_out, par_out,
                bx_qkv, by_qkv, bx_proj, by_proj, bx_inter, by_inter, bx_out, by_out, ln_v, w_v, m_v, v_v,
                nw_v, nm_v, nv_v, acc, gflat, r_d, r_1, r_2, r_z, stat1, stat2, wfull, pbf,
                in_sem, st_sem, out_sem, sd_s, sd_r, s1_s, s1_r, s2_s, s2_r, sz_s, sz_r,
                t1_s, t1_r, t2_s, t2_r, ag_s, ag_r):
    width, shard, ndev, rows = dims
    tokens = x_qkv.shape[0]
    step = tokens // CHUNKS
    ends = row_ends(width)
    me = lax.axis_index('dp')
    core, xx, yy, zz = me % 2, (me // 2) % 2, (me // 4) % 2, me // 8
    partner = me + 1 - 2 * core
    first = xx * (1 - core) + yy * core
    second = yy * (1 - core) + xx * core
    peer1 = me + (1 - 2 * first) * (2 * (1 - core) + 4 * core)
    peer2 = me + (1 - 2 * second) * (4 * (1 - core) + 2 * core)

    def slot(a, b):
        return (1 - core) * (2 * b + a) + core * (2 * a + b)

    pairs = [(x_out, bx_out, dy_out, by_out), (x_inter, bx_inter, dy_inter, by_inter),
             (x_proj, bx_proj, dy_proj, by_proj), (x_qkv, bx_qkv, dy_qkv, by_qkv)]
    loads = {}
    for p, (xs, xd, ys, yd) in enumerate(pairs):
        for k in range(CHUNKS):
            at = pl.ds(k * step, step)
            for q, (src, dst) in enumerate(((xs, xd), (ys, yd))):
                copy = pltpu.make_async_copy(src.at[at], dst.at[at], in_sem.at[p, k, q])
                copy.start()
                loads[p, k, q] = copy
    small = [pltpu.make_async_copy(s, d, st_sem.at[i])
             for i, (s, d) in enumerate(((ln, ln_v), (w_in, w_v), (m_in, m_v), (v_in, v_v)))]
    for copy in small:
        copy.start()

    barrier = pltpu.get_barrier_semaphore()
    for i in range(1, ndev):
        pl.semaphore_signal(barrier, inc=1, device_id=((me + i) % ndev,), device_id_type=pl.DeviceIdType.MESH)

    def remote(src, dst, s_sem, r_sem, dev):
        return pltpu.make_async_remote_copy(src_ref=src, dst_ref=dst, send_sem=s_sem, recv_sem=r_sem,
                                            device_id=(dev,), device_id_type=pl.DeviceIdType.MESH)

    ones = jnp.ones((16, step), BF16)

    def matmul(p, xb, yb, n):
        for k in range(CHUNKS):
            loads[p, k, 0].wait()
            loads[p, k, 1].wait()
            at = pl.ds(k * step, step)
            lhs = jnp.concatenate([xb[at, :].T, ones], axis=0)
            part = jnp.dot(lhs, yb[at, :], preferred_element_type=F32)
            if k == 0:
                acc[:, :n] = part
            else:
                acc[:, :n] += part

    def spread(base, n):
        cols = n // LANES
        for j in range(cols):
            gflat[pl.ds(base + j, width, stride=cols), :] = acc[0:width, j * LANES:(j + 1) * LANES]
            gflat[pl.ds(base + cols * width + j, 1), :] = acc[width:width + 1, j * LANES:(j + 1) * LANES]

    def matmul_out():
        cols = width // LANES
        inner = x_out.shape[1]
        for k in range(CHUNKS):
            loads[0, k, 0].wait()
            loads[0, k, 1].wait()
            at = pl.ds(k * step, step)
            y = by_out[at, :]
            part = jnp.dot(y.T, bx_out[at, :], preferred_element_type=F32)
            bias = jnp.dot(ones, y, preferred_element_type=F32)[0:8]
            if k == 0:
                acc[0:width, :] = part
                acc[width:width + 8, 0:width] = bias
            else:
                acc[0:width, :] += part
                acc[width:width + 8, 0:width] += bias
        base = ends[7]
        for j in range(cols):
            gflat[pl.ds(base + j, inner, stride=cols), :] = acc[j * LANES:(j + 1) * LANES, :].T
            gflat[pl.ds(ends[8] + j, 1), :] = acc[width:width + 1, j * LANES:(j + 1) * LANES]

    def send_d(g):
        for q in range(4):
            s = g * 8 + q * 2 + 1 - core
            remote(gflat.at[pl.ds(s * shard, shard)], r_d.at[g * 4 + q, pl.ds(0, shard)],
                   sd_s.at[g * 4 + q], sd_r.at[g * 4 + q], partner).start()

    def copy_1(g, b):
        return remote(r_d.at[g * 4 + slot(1 - first, b), pl.ds(0, shard)], r_1.at[g * 2 + b, pl.ds(0, shard)],
                      s1_s.at[g * 2 + b], s1_r.at[g * 2 + b], peer1)

    def copy_2(g):
        return remote(r_1.at[g * 2 + 1 - second, pl.ds(0, shard)], r_2.at[g, pl.ds(0, shard)],
                      s2_s.at[g], s2_r.at[g], peer2)

    def recv_d(j, a, b, g):
        q = slot(a, b)
        i = g * 4 + q
        remote(gflat.at[pl.ds(0, shard)], r_d.at[i, pl.ds(0, shard)], sd_s.at[i], sd_r.at[i], partner).wait_recv()
        r_d[i, 0:shard, :] += gflat[pl.ds((g * 8 + q * 2 + core) * shard, shard), :]

    def d_to_1(g):
        for b in range(2):
            recv_d(0, 1 - first, b, g)
            copy_1(g, b).start()
        for b in range(2):
            recv_d(0, first, b, g)

    def one_to_2(g):
        for b in (1 - second, second):
            i = g * 2 + b
            remote(r_d.at[0, pl.ds(0, shard)], r_1.at[i, pl.ds(0, shard)], s1_s.at[i], s1_r.at[i], peer1).wait_recv()
            r_1[i, 0:shard, :] += r_d[g * 4 + slot(first, b), 0:shard, :]
            if b is not second:
                copy_2(g).start()

    def two_to_z(g):
        copy_2(g).wait_recv()
        r_2[g, 0:shard, :] += r_1[g * 2 + second, 0:shard, :]

        @pl.when(zz != g)
        def _():
            remote(r_2.at[g, pl.ds(0, shard)], r_z.at[zz, pl.ds(0, shard)], sz_s.at[g], sz_r.at[zz],
                   me + (g - zz) * 8).start()

    matmul_out()
    small[0].wait()
    half = 2 * width // LANES
    gflat[pl.ds(ends[3], half), :] = ln_v[0:half, :]
    gflat[pl.ds(ends[9], half), :] = ln_v[half:2 * half, :]
    gflat[pl.ds(ends[11], rows - ends[11]), :] = jnp.zeros((rows - ends[11], LANES), F32)
    pl.semaphore_wait(barrier, ndev - 1)
    send_d(3)
    matmul(1, bx_inter, by_inter, 4 * width)
    spread(ends[5], 4 * width)
    d_to_1(3)
    send_d(2)
    matmul(2, bx_proj, by_proj, width)
    spread(ends[1], width)
    one_to_2(3)
    d_to_1(2)
    send_d(1)
    matmul(3, bx_qkv, by_qkv, 3 * width)
    spread(0, 3 * width)
    send_d(0)
    two_to_z(3)
    one_to_2(2)
    d_to_1(1)
    d_to_1(0)
    two_to_z(2)
    one_to_2(1)
    one_to_2(0)
    two_to_z(1)
    two_to_z(0)

    for copy in small[1:]:
        copy.wait()
    lane = lax.broadcasted_iota(jnp.int32, (shard, LANES), 1)
    row = lax.broadcasted_iota(jnp.int32, (shard, LANES), 0) + me * shard
    seg = jnp.zeros((shard, LANES), jnp.int32)
    for end in ends:
        seg = seg + jnp.where(row >= end, 1, 0)
    mine = lane == seg
    w = w_v[...]

    def seg_sums(val):
        per_row = jnp.sum(val, axis=1, keepdims=True)
        return jnp.sum(jnp.where(mine, per_row, 0.0), axis=0, keepdims=True)

    w_sums = seg_sums(w * w)

    g = r_2[zz, 0:shard, :]
    for d in range(1, PARTS):
        src = (zz + d) % PARTS
        remote(r_2.at[0, pl.ds(0, shard)], r_z.at[src, pl.ds(0, shard)], sz_s.at[0], sz_r.at[src], me).wait_recv()
        g = g + r_z[src, 0:shard, :]
    g = g * (1.0 / ndev)

    def exchange(stat, value, s_sem, r_sem):
        stat[pl.ds(me, 1), :] = value
        for i in range(1, ndev):
            remote(stat.at[pl.ds(me, 1)], stat.at[pl.ds(me, 1)], s_sem.at[i], r_sem, (me + i) % ndev).start()
        pltpu.make_async_copy(stat.at[pl.ds(0, ndev - 1)], stat.at[pl.ds(0, ndev - 1)], r_sem).wait()
        return jnp.sum(stat[...], axis=0, keepdims=True)

    one_lane = lax.broadcasted_iota(jnp.int32, (1, LANES), 1)
    g_sq = jnp.sum(jnp.sum(g * g, axis=0, keepdims=True), axis=1, keepdims=True)
    total1 = exchange(stat1, jnp.where(one_lane == 64, g_sq, w_sums), t1_s, t1_r)
    gn = jnp.sqrt(jnp.sum(jnp.where(one_lane == 64, total1, 0.0), axis=1, keepdims=True))
    h = g / jnp.maximum(1.0, gn)
    new_m = BETA_ONE * m_v[...] + (1.0 - BETA_ONE) * h
    new_v = BETA_TWO * v_v[...] + (1.0 - BETA_TWO) * h * h
    decay = jnp.where((seg == 0) | (seg == 2) | (seg == 6) | (seg == 8), DECAY, 0.0)
    u = (new_m / CORR_ONE) / (jnp.sqrt(new_v / CORR_TWO) + EPSILON) + decay * w
    total2 = exchange(stat2, seg_sums(u * u), t2_s, t2_r)
    nm_v[...] = new_m
    nv_v[...] = new_v
    w_norm, u_norm = jnp.sqrt(total1), jnp.sqrt(total2)
    ratio = jnp.where((w_norm > 0) & (u_norm > 0), w_norm / jnp.where(u_norm > 0, u_norm, 1.0), 1.0)
    per_row = jnp.sum(jnp.where(mine, ratio, 0.0), axis=1, keepdims=True)
    new_w = w - LEARN_RATE * per_row * u
    nw_v[...] = new_w
    wfull[pl.ds(me * shard, shard), :] = new_w
    outs = [pltpu.make_async_copy(s, d, out_sem.at[i])
            for i, (s, d) in enumerate(((nw_v, nw_out), (nm_v, nm_out), (nv_v, nv_out)))]

    def shard_at(s):
        return wfull.at[pl.ds(s * shard, shard)]

    sent = []

    def push(s, dev, src=None):
        copy = remote(shard_at(s) if src is None else src, shard_at(s), ag_s.at[len(sent)], ag_r.at[s], dev)
        copy.start()
        sent.append(copy)

    def arrived(s):
        remote(shard_at(s), shard_at(s), ag_s.at[0], ag_r.at[s], me).wait_recv()

    zs = [zz, zz + 1 - 2 * (zz % 2), 3 - zz, zz + 2 - 4 * (zz // 2)]

    def shifted(s, j):
        return s + (zs[j] - zz) * 8

    push(me, peer2, nw_v)
    push(me, peer1, nw_v)
    for j in range(1, PARTS):
        push(me, shifted(me, j), nw_v)
    push(me, partner, nw_v)
    for copy in outs:
        copy.start()
    diag = peer1 + peer2 - me
    for j in range(PARTS):
        if j:
            arrived(shifted(me, j))
            for dev in (peer2, peer1, partner):
                push(shifted(me, j), dev)
        s = shifted(peer1, j)
        arrived(s)
        push(s, peer2)
        push(s, partner)
    for j in range(PARTS):
        for base in (peer2, diag):
            s = shifted(base, j)
            arrived(s)
            push(s, partner)
    other = partner - core + (1 - core)
    for k in range(ndev // 2):
        arrived(2 * k + 1 - core)
    block = rows // PARTS
    half_rows = [i * rows // 2 for i in range(3)]
    par = []
    for i in range(2):
        at = pl.ds(half_rows[i], rows // 2)
        pbf[at, :] = wfull[at, :].astype(BF16)
        copy = pltpu.make_async_copy(pbf.at[at], par_out.at[at], out_sem.at[3 + i])
        copy.start()
        par.append(copy)

    for g_ in range(PARTS):
        for q in range(4):
            i = g_ * 4 + q
            remote(gflat.at[pl.ds(0, shard)], r_d.at[i, pl.ds(0, shard)], sd_s.at[i], sd_r.at[i], partner).wait_send()
        for b in range(2):
            copy_1(g_, b).wait_send()
        copy_2(g_).wait_send()

        @pl.when(zz != g_)
        def _():
            remote(r_2.at[g_, pl.ds(0, shard)], r_z.at[0, pl.ds(0, shard)], sz_s.at[g_], sz_r.at[0], me).wait_send()
    for i in range(1, ndev):
        for stat, sem, rs in ((stat1, t1_s, t1_r), (stat2, t2_s, t2_r)):
            remote(stat.at[pl.ds(0, 1)], stat.at[pl.ds(0, 1)], sem.at[i], rs, me).wait_send()
    for copy in sent:
        copy.wait_send()
    for copy in outs + par:
        copy.wait()


def solution(mesh):
    ndev = mesh.shape['dp']

    def local_step(weights, moment_one, moment_two, x_qkv, dy_qkv, x_proj, dy_proj, x_inter, dy_inter, x_out, dy_out, ln_grad):
        width = x_qkv.shape[1]
        shard = weights.shape[0] // LANES
        rows = shard * ndev
        flat = lambda a: a.reshape(-1, LANES)
        acts = (x_qkv, dy_qkv, x_proj, dy_proj, x_inter, dy_inter, x_out, dy_out)
        vm = pltpu.VMEM
        pad = -(-shard // 8) * 8
        state = jax.ShapeDtypeStruct((shard, LANES), F32)
        dma = pltpu.SemaphoreType.DMA
        hbm = pl.BlockSpec(memory_space=pl.ANY)
        outs = pl.pallas_call(
            functools.partial(comm_kernel, (width, shard, ndev, rows)),
            out_shape=(state, state, state, jax.ShapeDtypeStruct((rows, LANES), BF16)),
            in_specs=[hbm] * 12,
            out_specs=(hbm,) * 4,
            scratch_shapes=[vm(a.shape, BF16) for a in acts] + [
                vm((4 * width // LANES, LANES), F32)] + [vm((shard, LANES), F32)] * 6 + [
                vm((width + 16, 4 * width), F32), vm((rows, LANES), F32),
                vm((16, pad, LANES), F32), vm((8, pad, LANES), F32), vm((4, pad, LANES), F32), vm((4, pad, LANES), F32),
                vm((ndev, LANES), F32), vm((ndev, LANES), F32), vm((rows, LANES), F32), vm((rows, LANES), BF16),
                dma((4, CHUNKS, 2)), dma((4,)), dma((5,)), dma((16,)), dma((16,)), dma((8,)), dma((8,)),
                dma((4,)), dma((4,)), dma((4,)), dma((4,)),
                dma((ndev,)), dma, dma((ndev,)), dma, dma((40,)), dma((ndev,))],
            compiler_params=pltpu.CompilerParams(collective_id=0, has_side_effects=True, vmem_limit_bytes=60 * 2 ** 20),
            name='lamb_step',
        )(*acts, flat(ln_grad), flat(weights), flat(moment_one), flat(moment_two))
        new_w, new_m, new_v, params = outs
        return new_w.reshape(-1), new_m.reshape(-1), new_v.reshape(-1), params.reshape(-1)

    row_spec = P('dp', None)
    in_specs = (P('dp'), P('dp'), P('dp'), row_spec, row_spec, row_spec, row_spec, row_spec, row_spec, row_spec, row_spec, P('dp', None, None))
    out_specs = (P('dp'), P('dp'), P('dp'), P())
    return jax.shard_map(local_step, mesh=mesh, in_specs=in_specs, out_specs=out_specs, check_vma=False)
```

```python
import functools

import jax
import jax.numpy as jnp
from jax import lax
from jax.experimental import pallas as pl
from jax.experimental.pallas import tpu as pltpu
from jax.sharding import PartitionSpec as P

STEP = 10
LEARN_RATE = 0.5
BETA_ONE = 0.9
BETA_TWO = 0.999
EPSILON = 1e-6
DECAY = 0.01
CORR_ONE = 1.0 - BETA_ONE ** STEP
CORR_TWO = 1.0 - BETA_TWO ** STEP

LANES = 128
CHUNKS = 4
PARTS = 4
F32 = jnp.float32
BF16 = jnp.bfloat16


def tensor_sizes(width):
    return [3 * width * width, 3 * width, width * width, width, width, width,
            4 * width * width, 4 * width, 4 * width * width, width, width, width]


def row_ends(width):
    ends, total = [], 0
    for size in tensor_sizes(width):
        total += size // LANES
        ends.append(total)
    return ends


def scoped(name, fn, *args):
    with jax.named_scope(name):
        return fn(*args)


def comm_kernel(dims, x_qkv, dy_qkv, x_proj, dy_proj, x_inter, dy_inter, x_out, dy_out, ln, w_in, m_in, v_in,
                nw_out, nm_out, nv_out, par_out,
                bx_qkv, by_qkv, bx_proj, by_proj, bx_inter, by_inter, bx_out, by_out, ln_v, w_v, m_v, v_v,
                acc, gflat, r_d, r_1, r_2, r_z, stat1, stat2, wfull,
                in_sem, st_sem, sd_s, sd_r, s1_s, s1_r, s2_s, s2_r, sz_s, sz_r,
                t1_s, t1_r, t2_s, t2_r, ag_s, ag_r):
    width, shard, ndev, rows = dims
    tokens = x_qkv.shape[0]
    step = tokens // CHUNKS
    ends = row_ends(width)
    me = lax.axis_index('dp')
    core, xx, yy, zz = me % 2, (me // 2) % 2, (me // 4) % 2, me // 8
    partner = me + 1 - 2 * core
    first = xx * (1 - core) + yy * core
    second = yy * (1 - core) + xx * core
    peer1 = me + (1 - 2 * first) * (2 * (1 - core) + 4 * core)
    peer2 = me + (1 - 2 * second) * (4 * (1 - core) + 2 * core)

    def slot(a, b):
        return (1 - core) * (2 * b + a) + core * (2 * a + b)

    small = [pltpu.make_async_copy(s, d, st_sem.at[i])
             for i, (s, d) in enumerate(((ln, ln_v), (w_in, w_v), (m_in, m_v), (v_in, v_v)))]
    for copy in small:
        copy.start()
    pairs = [(x_out, bx_out, dy_out, by_out), (x_inter, bx_inter, dy_inter, by_inter),
             (x_proj, bx_proj, dy_proj, by_proj), (x_qkv, bx_qkv, dy_qkv, by_qkv)]
    def load(p, k, q):
        src, dst = pairs[p][2 * q:2 * q + 2]
        at = pl.ds(pl.multiple_of(k * step, step), step)
        return pltpu.make_async_copy(src.at[at], dst.at[at], in_sem.at[p, k, q])

    for p in range(4):
        for k in range(CHUNKS):
            for q in range(2):
                load(p, k, q).start()

    barrier = pltpu.get_barrier_semaphore()
    for i in range(1, ndev):
        pl.semaphore_signal(barrier, inc=1, device_id=((me + i) % ndev,), device_id_type=pl.DeviceIdType.MESH)

    def remote(src, dst, s_sem, r_sem, dev):
        return pltpu.make_async_remote_copy(src_ref=src, dst_ref=dst, send_sem=s_sem, recv_sem=r_sem,
                                            device_id=(dev,), device_id_type=pl.DeviceIdType.MESH)

    ones = jnp.ones((16, step), BF16)

    def matmul(p, xb, yb, n, service=None):
        acc[:, :n] = jnp.zeros((width + 16, n), F32)

        def body(k, _):
            load(p, k, 0).wait()
            load(p, k, 1).wait()
            at = pl.ds(pl.multiple_of(k * step, step), step)
            lhs = jnp.concatenate([xb[at, :].T, ones], axis=0)
            acc[:, :n] += jnp.dot(lhs, yb[at, :], preferred_element_type=F32)
            if service is not None:
                pl.when(k == CHUNKS // 2 - 1)(service)
            return 0

        lax.fori_loop(0, CHUNKS, body, 0)

    def spread(base, n):
        cols = n // LANES
        for j in range(cols):
            gflat[pl.ds(base + j, width, stride=cols), :] = acc[0:width, j * LANES:(j + 1) * LANES]
            gflat[pl.ds(base + cols * width + j, 1), :] = acc[width:width + 1, j * LANES:(j + 1) * LANES]

    def matmul_out():
        cols = width // LANES
        inner = x_out.shape[1]
        acc[...] = jnp.zeros(acc.shape, F32)

        def body(k, _):
            load(0, k, 0).wait()
            load(0, k, 1).wait()
            at = pl.ds(pl.multiple_of(k * step, step), step)
            y = by_out[at, :]
            acc[0:width, :] += jnp.dot(y.T, bx_out[at, :], preferred_element_type=F32)
            acc[width:width + 16, 0:width] += jnp.dot(ones, y, preferred_element_type=F32)
            return 0

        lax.fori_loop(0, CHUNKS, body, 0)
        base = ends[7]
        for j in range(cols):
            gflat[pl.ds(base + j, inner, stride=cols), :] = acc[j * LANES:(j + 1) * LANES, :].T
            gflat[pl.ds(ends[8] + j, 1), :] = acc[width:width + 1, j * LANES:(j + 1) * LANES]

    def send_d(g):
        for q in range(4):
            s = g * 8 + q * 2 + 1 - core
            remote(gflat.at[pl.ds(s * shard, shard)], r_d.at[g * 4 + q, pl.ds(0, shard)],
                   sd_s, sd_r.at[g * 4 + q], partner).start()

    def copy_1(g, b):
        return remote(r_d.at[g * 4 + slot(1 - first, b), pl.ds(0, shard)], r_1.at[g * 2 + b, pl.ds(0, shard)],
                      s1_s, s1_r.at[g * 2 + b], peer1)

    def copy_2(g):
        return remote(r_1.at[g * 2 + 1 - second, pl.ds(0, shard)], r_2.at[g, pl.ds(0, shard)],
                      s2_s, s2_r.at[g], peer2)

    def recv_d(a, b, g):
        q = slot(a, b)
        i = g * 4 + q
        remote(gflat.at[pl.ds(0, shard)], r_d.at[i, pl.ds(0, shard)], sd_s, sd_r.at[i], partner).wait_recv()
        r_d[i, 0:shard, :] += gflat[pl.ds((g * 8 + q * 2 + core) * shard, shard), :]

    def d_to_1(g):
        for b in (1 - second, second):
            recv_d(1 - first, b, g)
            copy_1(g, b).start()
        for b in range(2):
            recv_d(first, b, g)

    def one_to_2(g):
        for b in (1 - second, second):
            i = g * 2 + b
            remote(r_d.at[0, pl.ds(0, shard)], r_1.at[i, pl.ds(0, shard)], s1_s, s1_r.at[i], peer1).wait_recv()
            r_1[i, 0:shard, :] += r_d[g * 4 + slot(first, b), 0:shard, :]
            if b is not second:
                copy_2(g).start()

    def two_to_z(g):
        copy_2(g).wait_recv()
        r_2[g, 0:shard, :] += r_1[g * 2 + second, 0:shard, :]

        @pl.when(zz != g)
        def _():
            remote(r_2.at[g, pl.ds(0, shard)], r_z.at[zz, pl.ds(0, shard)], sz_s, sz_r.at[zz],
                   me + (g - zz) * 8).start()

    scoped('matmul_out', matmul_out)
    small[0].wait()
    cols = width // LANES
    for r, start in enumerate((ends[3], ends[4], ends[9], ends[10])):
        for j in range(cols):
            gflat[pl.ds(start + j, 1), :] = ln_v[r:r + 1, j * LANES:(j + 1) * LANES]
    gflat[pl.ds(ends[11], rows - ends[11]), :] = jnp.zeros((rows - ends[11], LANES), F32)
    scoped('barrier_barrier', pl.semaphore_wait, barrier, ndev - 1)
    scoped('send_d_3', send_d, 3)
    scoped('matmul_1', matmul, 1, bx_inter, by_inter, 4 * width, lambda: scoped('in_d1_3', d_to_1, 3))
    scoped('spread_ends_5', spread, ends[5], 4 * width)
    scoped('send_d_2', send_d, 2)
    scoped('matmul_2', matmul, 2, bx_proj, by_proj, width)
    scoped('spread_ends_1', spread, ends[1], width)
    scoped('send_d_1', send_d, 1)
    scoped('d_to_1_2', d_to_1, 2)
    scoped('matmul_3', matmul, 3, bx_qkv, by_qkv, 3 * width, lambda: scoped('in_d1_1', d_to_1, 1))
    scoped('spread_0', spread, 0, 3 * width)
    scoped('send_d_0', send_d, 0)
    scoped('one_to_2_3', one_to_2, 3)
    scoped('d_to_1_0', d_to_1, 0)
    scoped('one_to_2_2', one_to_2, 2)
    scoped('two_to_z_3', two_to_z, 3)
    scoped('one_to_2_1', one_to_2, 1)
    scoped('two_to_z_2', two_to_z, 2)
    scoped('one_to_2_0', one_to_2, 0)
    scoped('two_to_z_1', two_to_z, 1)
    scoped('two_to_z_0', two_to_z, 0)

    for copy in small[1:]:
        scoped('wait_state', copy.wait)
    lane = lax.broadcasted_iota(jnp.int32, (shard, LANES), 1)
    row = lax.broadcasted_iota(jnp.int32, (shard, LANES), 0) + me * shard
    seg = jnp.zeros((shard, LANES), jnp.int32)
    for end in ends:
        seg = seg + jnp.where(row >= end, 1, 0)
    mine = lane == seg
    w = w_v[...]

    def seg_sums(val):
        per_row = jnp.sum(val, axis=1, keepdims=True)
        return jnp.sum(jnp.where(mine, per_row, 0.0), axis=0, keepdims=True)

    w_sums = seg_sums(w * w)

    g = r_2[zz, 0:shard, :]
    for d in range(1, PARTS):
        src = (zz + d) % PARTS
        scoped('wait_z', remote(r_2.at[0, pl.ds(0, shard)], r_z.at[src, pl.ds(0, shard)], sz_s, sz_r.at[src], me).wait_recv)
        g = g + r_z[src, 0:shard, :]
    g = g * (1.0 / ndev)

    def exchange(stat, value, s_sem, r_sem):
        stat[pl.ds(me, 1), :] = value
        for i in range(1, ndev):
            remote(stat.at[pl.ds(me, 1)], stat.at[pl.ds(me, 1)], s_sem, r_sem, (me + i) % ndev).start()
        scoped('wait_stat', pltpu.make_async_copy(stat.at[pl.ds(0, ndev - 1)], stat.at[pl.ds(0, ndev - 1)], r_sem).wait)
        return jnp.sum(stat[...], axis=0, keepdims=True)

    one_lane = lax.broadcasted_iota(jnp.int32, (1, LANES), 1)
    g_sq = jnp.sum(jnp.sum(g * g, axis=0, keepdims=True), axis=1, keepdims=True)
    total1 = exchange(stat1, jnp.where(one_lane == 64, g_sq, w_sums), t1_s, t1_r)
    gn = jnp.sqrt(jnp.sum(jnp.where(one_lane == 64, total1, 0.0), axis=1, keepdims=True))
    h = g / jnp.maximum(1.0, gn)
    new_m = BETA_ONE * m_v[...] + (1.0 - BETA_ONE) * h
    new_v = BETA_TWO * v_v[...] + (1.0 - BETA_TWO) * h * h
    decay = jnp.where((seg == 0) | (seg == 2) | (seg == 6) | (seg == 8), DECAY, 0.0)
    u = (new_m / CORR_ONE) / (jnp.sqrt(new_v / CORR_TWO) + EPSILON) + decay * w
    total2 = exchange(stat2, seg_sums(u * u), t2_s, t2_r)
    nm_out[...] = new_m
    nv_out[...] = new_v
    w_norm, u_norm = jnp.sqrt(total1), jnp.sqrt(total2)
    ratio = jnp.where((w_norm > 0) & (u_norm > 0), w_norm / jnp.where(u_norm > 0, u_norm, 1.0), 1.0)
    per_row = jnp.sum(jnp.where(mine, ratio, 0.0), axis=1, keepdims=True)
    new_w = w - LEARN_RATE * per_row * u
    nw_out[...] = new_w
    wfull[pl.ds(me * shard, shard), :] = new_w
    def shard_at(s):
        return wfull.at[pl.ds(s * shard, shard)]

    sent = []

    def push(s, dev, src=None):
        copy = remote(shard_at(s) if src is None else src, shard_at(s), ag_s, ag_r.at[s], dev)
        copy.start()
        sent.append(s)

    def arrived(s):
        scoped('arrived', remote(shard_at(s), shard_at(s), ag_s, ag_r.at[s], me).wait_recv)

    zs = [zz, zz + 1 - 2 * (zz % 2), 3 - zz, zz + 2 - 4 * (zz // 2)]

    def shifted(s, j):
        return s + (zs[j] - zz) * 8

    push(me, peer2, nw_out)
    push(me, peer1, nw_out)
    for j in range(1, PARTS):
        push(me, shifted(me, j), nw_out)
    push(me, partner, nw_out)
    diag = peer1 + peer2 - me
    for j in range(PARTS):
        if j:
            arrived(shifted(me, j))
            for dev in (peer2, peer1, partner):
                push(shifted(me, j), dev)
        s = shifted(peer1, j)
        arrived(s)
        push(s, peer2)
        push(s, partner)
    for j in range(PARTS):
        for base in (peer2, diag):
            s = shifted(base, j)
            arrived(s)
            push(s, partner)
    for k in range(ndev // 2):
        arrived(2 * k + 1 - core)
    par_out[...] = wfull[...].astype(BF16)

    def all_sent(buf, count, sem):
        pltpu.make_async_copy(buf.at[pl.ds(0, count)], buf.at[pl.ds(0, count)], sem).wait()

    scoped('all_sent_gflat', all_sent, gflat, 16 * shard, sd_s)
    scoped('all_sent_gflat', all_sent, gflat, 8 * shard, s1_s)
    scoped('all_sent_gflat', all_sent, gflat, 4 * shard, s2_s)
    scoped('all_sent_gflat', all_sent, gflat, 3 * shard, sz_s)
    scoped('all_sent_stat1', all_sent, stat1, ndev - 1, t1_s)
    scoped('all_sent_stat2', all_sent, stat2, ndev - 1, t2_s)
    scoped('all_sent_wfull', all_sent, wfull, len(sent) * shard, ag_s)


def write_kernel(*refs):
    half = len(refs) // 2
    for src, dst in zip(refs[:half], refs[half:]):
        dst[...] = src[...]


def solution(mesh):
    ndev = mesh.shape['dp']

    def local_step(weights, moment_one, moment_two, x_qkv, dy_qkv, x_proj, dy_proj, x_inter, dy_inter, x_out, dy_out, ln_grad):
        width = x_qkv.shape[1]
        shard = weights.shape[0] // LANES
        rows = shard * ndev
        flat = lambda a: a.reshape(-1, LANES)
        acts = (x_qkv, dy_qkv, x_proj, dy_proj, x_inter, dy_inter, x_out, dy_out)
        vm = pltpu.VMEM
        pad = -(-shard // 8) * 8
        state = jax.ShapeDtypeStruct((shard, LANES), F32)
        dma = pltpu.SemaphoreType.DMA
        hbm = pl.BlockSpec(memory_space=pltpu.HBM)
        whole = pl.BlockSpec(memory_space=pltpu.VMEM)
        out_shape = (state, state, state, jax.ShapeDtypeStruct((rows, LANES), BF16))
        outs = pl.pallas_call(
            functools.partial(comm_kernel, (width, shard, ndev, rows)),
            out_shape=out_shape,
            in_specs=[hbm] * 12,
            out_specs=(whole,) * 4,
            scratch_shapes=[vm(a.shape, BF16) for a in acts] + [
                vm((4, width), F32)] + [vm((shard, LANES), F32)] * 3 + [
                vm((width + 16, 4 * width), F32), vm((rows, LANES), F32),
                vm((16, pad, LANES), F32), vm((8, pad, LANES), F32), vm((4, pad, LANES), F32), vm((4, pad, LANES), F32),
                vm((ndev, LANES), F32), vm((ndev, LANES), F32), vm((rows, LANES), F32),
                dma((4, CHUNKS, 2)), dma((4,)), dma, dma((16,)), dma, dma((8,)), dma, dma((4,)), dma, dma((4,)),
                dma, dma, dma, dma, dma, dma((ndev,))],
            compiler_params=pltpu.CompilerParams(collective_id=0, has_side_effects=True, vmem_limit_bytes=61 * 2 ** 20),
            name='lamb_step',
        )(*acts, ln_grad.reshape(4, width), flat(weights), flat(moment_one), flat(moment_two))
        new_w, new_m, new_v, params = pl.pallas_call(
            write_kernel, out_shape=out_shape, in_specs=[whole] * 4, out_specs=(whole,) * 4, name='write_out')(*outs)
        return new_w.reshape(-1), new_m.reshape(-1), new_v.reshape(-1), params.reshape(-1)

    row_spec = P('dp', None)
    in_specs = (P('dp'), P('dp'), P('dp'), row_spec, row_spec, row_spec, row_spec, row_spec, row_spec, row_spec, row_spec, P('dp', None, None))
    out_specs = (P('dp'), P('dp'), P('dp'), P())
    return jax.shard_map(local_step, mesh=mesh, in_specs=in_specs, out_specs=out_specs, check_vma=False)
```

```python
import functools

import jax
import jax.numpy as jnp
from jax import lax
from jax.experimental import pallas as pl
from jax.experimental.pallas import tpu as pltpu
from jax.sharding import PartitionSpec as P

STEP = 10
LEARN_RATE = 0.5
BETA_ONE = 0.9
BETA_TWO = 0.999
EPSILON = 1e-6
DECAY = 0.01
CORR_ONE = 1.0 - BETA_ONE ** STEP
CORR_TWO = 1.0 - BETA_TWO ** STEP

LANES = 128
CHUNKS = 4
PARTS = 4
F32 = jnp.float32
BF16 = jnp.bfloat16


def tensor_sizes(width):
    return [3 * width * width, 3 * width, width * width, width, width, width,
            4 * width * width, 4 * width, 4 * width * width, width, width, width]


def row_ends(width):
    ends, total = [], 0
    for size in tensor_sizes(width):
        total += size // LANES
        ends.append(total)
    return ends


def scoped(name, fn, *args):
    with jax.named_scope(name):
        return fn(*args)


def comm_kernel(dims, x_qkv, dy_qkv, x_proj, dy_proj, x_inter, dy_inter, x_out, dy_out, ln, w_in, m_in, v_in,
                nw_out, nm_out, nv_out, par_out,
                bx_qkv, by_qkv, bx_proj, by_proj, bx_inter, by_inter, bx_out, by_out, ln_v, w_v, m_v, v_v,
                acc, gflat, r_d, r_1, r_2, r_z, stat1, stat2, wfull,
                in_sem, st_sem, sd_s, sd_r, s1_s, s1_r, s2_s, s2_r, sz_s, sz_r,
                t1_s, t1_r, t2_s, t2_r, ag_s, ag_r):
    width, shard, ndev, rows = dims
    tokens = x_qkv.shape[0]
    step = tokens // CHUNKS
    ends = row_ends(width)
    me = lax.axis_index('dp')
    core, xx, yy, zz = me % 2, (me // 2) % 2, (me // 4) % 2, me // 8
    partner = me + 1 - 2 * core
    first = xx * (1 - core) + yy * core
    second = yy * (1 - core) + xx * core
    peer1 = me + (1 - 2 * first) * (2 * (1 - core) + 4 * core)
    peer2 = me + (1 - 2 * second) * (4 * (1 - core) + 2 * core)

    def slot(a, b):
        return (1 - core) * (2 * b + a) + core * (2 * a + b)

    small = [pltpu.make_async_copy(s, d, st_sem.at[i])
             for i, (s, d) in enumerate(((ln, ln_v), (w_in, w_v), (m_in, m_v), (v_in, v_v)))]
    for copy in small:
        copy.start()
    pairs = [(x_out, bx_out, dy_out, by_out), (x_qkv, bx_qkv, dy_qkv, by_qkv),
             (x_proj, bx_proj, dy_proj, by_proj), (x_inter, bx_inter, dy_inter, by_inter)]
    def load(p, k, q):
        src, dst = pairs[p][2 * q:2 * q + 2]
        at = pl.ds(pl.multiple_of(k * step, step), step)
        return pltpu.make_async_copy(src.at[at], dst.at[at], in_sem.at[p, k, q])

    for p in range(4):
        def start(k, _, p=p):
            for q in range(2):
                load(p, k, q).start()
            return 0

        lax.fori_loop(0, CHUNKS, start, 0)

    barrier = pltpu.get_barrier_semaphore()
    stat2[...] = jnp.zeros(stat2.shape, F32)

    def hello(i, _):
        pl.semaphore_signal(barrier, inc=1, device_id=((me + i) % ndev,), device_id_type=pl.DeviceIdType.MESH)
        return 0

    lax.fori_loop(1, ndev, hello, 0)

    def remote(src, dst, s_sem, r_sem, dev):
        return pltpu.make_async_remote_copy(src_ref=src, dst_ref=dst, send_sem=s_sem, recv_sem=r_sem,
                                            device_id=(dev,), device_id_type=pl.DeviceIdType.MESH)

    ones = jnp.ones((16, step), BF16)

    def matmul(p, xb, yb, n, service=None):
        acc[:, :n] = jnp.zeros((width + 16, n), F32)

        def body(k, _):
            load(p, k, 0).wait()
            load(p, k, 1).wait()
            at = pl.ds(pl.multiple_of(k * step, step), step)
            lhs = jnp.concatenate([xb[at, :].T, ones], axis=0)
            acc[:, :n] += jnp.dot(lhs, yb[at, :], preferred_element_type=F32)
            for at_k, fn in (service or {}).items():
                pl.when(k == at_k)(fn)
            return 0

        lax.fori_loop(0, CHUNKS, body, 0)

    def spread(base, n):
        cols = n // LANES
        for j in range(cols):
            gflat[pl.ds(base + j, width, stride=cols), :] = acc[0:width, j * LANES:(j + 1) * LANES]
            gflat[pl.ds(base + cols * width + j, 1), :] = acc[width:width + 1, j * LANES:(j + 1) * LANES]

    def matmul_out():
        cols = width // LANES
        inner = x_out.shape[1]
        acc[...] = jnp.zeros(acc.shape, F32)

        def body(k, _):
            load(0, k, 0).wait()
            load(0, k, 1).wait()
            at = pl.ds(pl.multiple_of(k * step, step), step)
            y = by_out[at, :]
            acc[0:width, :] += jnp.dot(y.T, bx_out[at, :], preferred_element_type=F32)
            acc[width:width + 16, 0:width] += jnp.dot(ones, y, preferred_element_type=F32)
            return 0

        lax.fori_loop(0, CHUNKS, body, 0)
        base = ends[7]
        for j in range(cols):
            gflat[pl.ds(base + j, inner, stride=cols), :] = acc[j * LANES:(j + 1) * LANES, :].T
            gflat[pl.ds(ends[8] + j, 1), :] = acc[width:width + 1, j * LANES:(j + 1) * LANES]

    def send_d(g):
        for q in range(4):
            s = g * 8 + q * 2 + 1 - core
            remote(gflat.at[pl.ds(s * shard, shard)], r_d.at[g * 4 + q, pl.ds(0, shard)],
                   sd_s, sd_r.at[g * 4 + q], partner).start()

    def copy_1(g, b):
        return remote(r_d.at[g * 4 + slot(1 - first, b), pl.ds(0, shard)], r_1.at[g * 2 + b, pl.ds(0, shard)],
                      s1_s, s1_r.at[g * 2 + b], peer1)

    def copy_2(g):
        return remote(r_1.at[g * 2 + 1 - second, pl.ds(0, shard)], r_2.at[g, pl.ds(0, shard)],
                      s2_s, s2_r.at[g], peer2)

    def recv_d(a, b, g):
        q = slot(a, b)
        i = g * 4 + q
        remote(gflat.at[pl.ds(0, shard)], r_d.at[i, pl.ds(0, shard)], sd_s, sd_r.at[i], partner).wait_recv()
        r_d[i, 0:shard, :] += gflat[pl.ds((g * 8 + q * 2 + core) * shard, shard), :]

    def d_to_1(g):
        for b in (1 - second, second):
            recv_d(1 - first, b, g)
            copy_1(g, b).start()
        for b in range(2):
            recv_d(first, b, g)

    def one_to_2(g):
        for b in (1 - second, second):
            i = g * 2 + b
            remote(r_d.at[0, pl.ds(0, shard)], r_1.at[i, pl.ds(0, shard)], s1_s, s1_r.at[i], peer1).wait_recv()
            r_1[i, 0:shard, :] += r_d[g * 4 + slot(first, b), 0:shard, :]
            if b is not second:
                copy_2(g).start()

    def two_to_z(g):
        copy_2(g).wait_recv()
        r_2[g, 0:shard, :] += r_1[g * 2 + second, 0:shard, :]

        @pl.when(zz != g)
        def _():
            remote(r_2.at[g, pl.ds(0, shard)], r_z.at[zz, pl.ds(0, shard)], sz_s, sz_r.at[zz],
                   me + (g - zz) * 8).start()

    scoped('matmul_out', matmul_out)
    small[0].wait()
    cols = width // LANES
    for r, start in enumerate((ends[3], ends[4], ends[9], ends[10])):
        for j in range(cols):
            gflat[pl.ds(start + j, 1), :] = ln_v[r:r + 1, j * LANES:(j + 1) * LANES]
    gflat[pl.ds(ends[11], rows - ends[11]), :] = jnp.zeros((rows - ends[11], LANES), F32)
    scoped('barrier_barrier', pl.semaphore_wait, barrier, ndev - 1)
    scoped('send_d_3', send_d, 3)
    scoped('mm_qkv', matmul, 1, bx_qkv, by_qkv, 3 * width, {1: lambda: scoped('in_d1_3', d_to_1, 3)})
    scoped('spread_qkv', spread, 0, 3 * width)
    scoped('mm_proj', matmul, 2, bx_proj, by_proj, width)
    scoped('spread_proj', spread, ends[1], width)
    scoped('send_d_0', send_d, 0)
    scoped('mm_inter', matmul, 3, bx_inter, by_inter, 4 * width,
           {1: lambda: scoped('in_d1_0', d_to_1, 0), 2: lambda: scoped('in_12_3', one_to_2, 3)})
    scoped('spread_inter', spread, ends[5], 4 * width)
    scoped('send_d_1', send_d, 1)
    scoped('send_d_2', send_d, 2)
    scoped('one_to_2_0', one_to_2, 0)
    scoped('d_to_1_1', d_to_1, 1)
    scoped('two_to_z_3', two_to_z, 3)
    scoped('d_to_1_2', d_to_1, 2)
    scoped('two_to_z_0', two_to_z, 0)
    scoped('one_to_2_1', one_to_2, 1)
    scoped('one_to_2_2', one_to_2, 2)
    scoped('two_to_z_1', two_to_z, 1)
    scoped('two_to_z_2', two_to_z, 2)

    for copy in small[1:]:
        scoped('wait_state', copy.wait)
    lane = lax.broadcasted_iota(jnp.int32, (shard, LANES), 1)
    row = lax.broadcasted_iota(jnp.int32, (shard, LANES), 0) + me * shard
    seg = jnp.zeros((shard, LANES), jnp.int32)
    for end in ends:
        seg = seg + jnp.where(row >= end, 1, 0)
    mine = lane == seg
    w = w_v[...]

    def seg_sums(val):
        per_row = jnp.sum(val, axis=1, keepdims=True)
        return jnp.sum(jnp.where(mine, per_row, 0.0), axis=0, keepdims=True)

    w_sums = seg_sums(w * w)

    g = r_2[zz, 0:shard, :]
    for d in range(1, PARTS):
        src = (zz + d) % PARTS
        scoped('wait_z', remote(r_2.at[0, pl.ds(0, shard)], r_z.at[src, pl.ds(0, shard)], sz_s, sz_r.at[src], me).wait_recv)
        g = g + r_z[src, 0:shard, :]
    g = g * (1.0 / ndev)

    def put(stat, value, s_sem, r_sem, lo, hi):
        stat[pl.ds(me, 1), :] = value

        def send(i, _):
            remote(stat.at[pl.ds(me, 1)], stat.at[pl.ds(me, 1)], s_sem, r_sem, (me + i) % ndev).start()
            return 0

        lax.fori_loop(lo, hi, send, 0)

    def rows_in(stat, count, sem):
        return pltpu.make_async_copy(stat.at[pl.ds(0, count)], stat.at[pl.ds(0, count)], sem)

    one_lane = lax.broadcasted_iota(jnp.int32, (1, LANES), 1)
    g_sq = jnp.sum(jnp.sum(g * g, axis=0, keepdims=True), axis=1, keepdims=True)
    put(stat1, jnp.where(one_lane == 64, g_sq, w_sums), t1_s, t1_r, 1, ndev)
    scoped('wait_stat1', rows_in(stat1, ndev - 1, t1_r).wait)
    total1 = jnp.sum(stat1[...], axis=0, keepdims=True)
    gn = jnp.sqrt(jnp.sum(jnp.where(one_lane == 64, total1, 0.0), axis=1, keepdims=True))
    h = g / jnp.maximum(1.0, gn)
    new_m = BETA_ONE * m_v[...] + (1.0 - BETA_ONE) * h
    new_v = BETA_TWO * v_v[...] + (1.0 - BETA_TWO) * h * h
    decay = jnp.where((seg == 0) | (seg == 2) | (seg == 6) | (seg == 8), DECAY, 0.0)
    u = (new_m / CORR_ONE) / (jnp.sqrt(new_v / CORR_TWO) + EPSILON) + decay * w
    plane = ndev // PARTS
    starts = [0] + ends[:-1]
    assert all((end - 1) // (plane * shard) - start // (plane * shard) <= 1 for start, end in zip(starts, ends))
    stat2[pl.ds(me, 1), :] = seg_sums(u * u)

    def send2(i, _, d):
        to = zz * plane + i

        @pl.when((to >= 0) & (to < ndev) & (to != me))
        def _():
            remote(stat2.at[pl.ds(me, 1)], stat2.at[pl.ds(me, 1)], t2_s.at[d + 1], t2_r.at[zz], to).start()

        return 0

    for d in (-1, 1, 0):
        lax.fori_loop(d * plane, (d + 1) * plane, functools.partial(send2, d=d), 0)

    def each_plane(fn):
        fn(1, zz, plane - 1)
        pl.when(zz > 0)(lambda: fn(0, zz - 1, plane))
        pl.when(zz < PARTS - 1)(lambda: fn(2, zz + 1, plane))

    scoped('wait_stat2', each_plane, lambda d, src, count: rows_in(stat2, count, t2_r.at[src]).wait())
    total2 = jnp.sum(stat2[...], axis=0, keepdims=True)
    nm_out[...] = new_m
    nv_out[...] = new_v
    w_norm, u_norm = jnp.sqrt(total1), jnp.sqrt(total2)
    ratio = jnp.where((w_norm > 0) & (u_norm > 0), w_norm / jnp.where(u_norm > 0, u_norm, 1.0), 1.0)
    per_row = jnp.sum(jnp.where(mine, ratio, 0.0), axis=1, keepdims=True)
    new_w = w - LEARN_RATE * per_row * u
    nw_out[...] = new_w
    wfull[pl.ds(me * shard, shard), :] = new_w
    split = (shard + 1) // 2
    parts = ((0, split), (split, shard - split))

    def part_at(s, h):
        return wfull.at[pl.ds(s * shard + parts[h][0], parts[h][1])]

    sent = []

    def push(s, h, *devs):
        for dev in devs:
            remote(part_at(s, h), part_at(s, h), ag_s, ag_r.at[s, h], dev).start()
            sent.append(parts[h][1])

    def arrived(s, h):
        remote(part_at(s, h), part_at(s, h), ag_s, ag_r.at[s, h], me).wait_recv()

    zs = [zz, zz + 1 - 2 * (zz % 2), 3 - zz, zz + 2 - 4 * (zz // 2)]
    diag = peer1 + peer2 - me

    def shifted(s, j):
        return s + (zs[j] - zz) * 8

    for h in range(2):
        push(me, h, peer2, peer1, shifted(me, 1), shifted(me, 2), shifted(me, 3), partner)
    for kind, j in (('a', 0), ('z', 1), ('z', 2), ('a', 1), ('z', 3), ('a', 2), ('a', 3), ('b', 0), ('d', 0), ('b', 1),
                    ('d', 1), ('b', 2), ('d', 2), ('b', 3), ('d', 3)):
        s = shifted({'a': peer1, 'z': me, 'b': peer2, 'd': diag}[kind], j)
        for h in range(2):
            scoped('got_%s%d' % (kind, j), arrived, s, h)
            push(s, h, *{'a': (peer2, partner), 'z': (peer2, peer1, partner)}.get(kind, (partner,)))

    def rest(k, _):
        for h in range(2):
            arrived(2 * k + 1 - core, h)
        return 0

    scoped('got_rest', lax.fori_loop, 0, ndev // 2, rest, 0)
    par_out[...] = wfull[...].astype(BF16)

    def all_sent(buf, count, sem):
        pltpu.make_async_copy(buf.at[pl.ds(0, count)], buf.at[pl.ds(0, count)], sem).wait()

    scoped('all_sent_gflat', all_sent, gflat, 16 * shard, sd_s)
    scoped('all_sent_gflat', all_sent, gflat, 8 * shard, s1_s)
    scoped('all_sent_gflat', all_sent, gflat, 4 * shard, s2_s)
    scoped('all_sent_gflat', all_sent, gflat, 3 * shard, sz_s)
    scoped('all_sent_stat1', all_sent, stat1, ndev - 1, t1_s)
    each_plane(lambda d, src, count: rows_in(stat2, count, t2_s.at[d]).wait())
    scoped('all_sent_wfull', all_sent, wfull, sum(sent), ag_s)


def write_kernel(*refs):
    half = len(refs) // 2
    for src, dst in zip(refs[:half], refs[half:]):
        dst[...] = src[...]


def solution(mesh):
    ndev = mesh.shape['dp']

    def local_step(weights, moment_one, moment_two, x_qkv, dy_qkv, x_proj, dy_proj, x_inter, dy_inter, x_out, dy_out, ln_grad):
        width = x_qkv.shape[1]
        shard = weights.shape[0] // LANES
        rows = shard * ndev
        flat = lambda a: a.reshape(-1, LANES)
        acts = (x_qkv, dy_qkv, x_proj, dy_proj, x_inter, dy_inter, x_out, dy_out)
        vm = pltpu.VMEM
        pad = -(-shard // 8) * 8
        state = jax.ShapeDtypeStruct((shard, LANES), F32)
        dma = pltpu.SemaphoreType.DMA
        hbm = pl.BlockSpec(memory_space=pltpu.HBM)
        whole = pl.BlockSpec(memory_space=pltpu.VMEM)
        out_shape = (state, state, state, jax.ShapeDtypeStruct((rows, LANES), BF16))
        outs = pl.pallas_call(
            functools.partial(comm_kernel, (width, shard, ndev, rows)),
            out_shape=out_shape,
            in_specs=[hbm] * 12,
            out_specs=(whole,) * 4,
            scratch_shapes=[vm(a.shape, BF16) for a in acts] + [
                vm((4, width), F32)] + [vm((shard, LANES), F32)] * 3 + [
                vm((width + 16, 4 * width), F32), vm((rows, LANES), F32),
                vm((16, pad, LANES), F32), vm((8, pad, LANES), F32), vm((4, pad, LANES), F32), vm((4, pad, LANES), F32),
                vm((ndev, LANES), F32), vm((ndev, LANES), F32), vm((rows, LANES), F32),
                dma((4, CHUNKS, 2)), dma((4,)), dma, dma((16,)), dma, dma((8,)), dma, dma((4,)), dma, dma((4,)),
                dma, dma, dma((3,)), dma((PARTS,)), dma, dma((ndev, 2))],
            compiler_params=pltpu.CompilerParams(collective_id=0, has_side_effects=True, vmem_limit_bytes=61 * 2 ** 20),
            name='lamb_step',
        )(*acts, ln_grad.reshape(4, width), flat(weights), flat(moment_one), flat(moment_two))
        new_w, new_m, new_v, params = pl.pallas_call(
            write_kernel, out_shape=out_shape, in_specs=[whole] * 4, out_specs=(whole,) * 4, name='write_out')(*outs)
        return new_w.reshape(-1), new_m.reshape(-1), new_v.reshape(-1), params.reshape(-1)

    row_spec = P('dp', None)
    in_specs = (P('dp'), P('dp'), P('dp'), row_spec, row_spec, row_spec, row_spec, row_spec, row_spec, row_spec, row_spec, P('dp', None, None))
    out_specs = (P('dp'), P('dp'), P('dp'), P())
    return jax.shard_map(local_step, mesh=mesh, in_specs=in_specs, out_specs=out_specs, check_vma=False)
```

```python
import functools

import jax
import jax.numpy as jnp
from jax import lax
from jax.experimental import pallas as pl
from jax.experimental.pallas import tpu as pltpu
from jax.sharding import PartitionSpec as P

STEP = 10
LEARN_RATE = 0.5
BETA_ONE = 0.9
BETA_TWO = 0.999
EPSILON = 1e-6
DECAY = 0.01
CORR_ONE = 1.0 - BETA_ONE ** STEP
CORR_TWO = 1.0 - BETA_TWO ** STEP

LANES = 128
CHUNKS = 4
PARTS = 4
F32 = jnp.float32
BF16 = jnp.bfloat16


def tensor_sizes(width):
    return [3 * width * width, 3 * width, width * width, width, width, width,
            4 * width * width, 4 * width, 4 * width * width, width, width, width]


def row_ends(width):
    ends, total = [], 0
    for size in tensor_sizes(width):
        total += size // LANES
        ends.append(total)
    return ends


def scoped(name, fn, *args):
    with jax.named_scope(name):
        return fn(*args)


def comm_kernel(dims, x_qkv, dy_qkv, x_proj, dy_proj, x_inter, dy_inter, x_out, dy_out, ln, w_in, m_in, v_in,
                nw_out, nm_out, nv_out, par_out,
                bx_qkv, by_qkv, bx_proj, by_proj, bx_inter, by_inter, bx_out, by_out, ln_v, w_v, m_v, v_v,
                acc, gflat, r_d, r_1, r_2, r_z, stat1, stat2, wfull,
                in_sem, st_sem, sd_s, sd_r, s1_s, s1_r, s2_s, s2_r, sz_s, sz_r,
                t1_s, t1_r, t2_s, t2_r, ag_s, ag_r):
    width, shard, ndev, rows = dims
    tokens = x_qkv.shape[0]
    step = tokens // CHUNKS
    ends = row_ends(width)
    me = lax.axis_index('dp')
    core, xx, yy, zz = me % 2, (me // 2) % 2, (me // 4) % 2, me // 8
    partner = me + 1 - 2 * core
    first = xx * (1 - core) + yy * core
    second = yy * (1 - core) + xx * core
    peer1 = me + (1 - 2 * first) * (2 * (1 - core) + 4 * core)
    peer2 = me + (1 - 2 * second) * (4 * (1 - core) + 2 * core)

    def slot(a, b):
        return (1 - core) * (2 * b + a) + core * (2 * a + b)

    small = [pltpu.make_async_copy(s, d, st_sem.at[i])
             for i, (s, d) in enumerate(((ln, ln_v), (w_in, w_v), (m_in, m_v), (v_in, v_v)))]
    for copy in small:
        copy.start()
    pairs = [(x_out, bx_out, dy_out, by_out), (x_qkv, bx_qkv, dy_qkv, by_qkv),
             (x_proj, bx_proj, dy_proj, by_proj), (x_inter, bx_inter, dy_inter, by_inter)]
    def load(p, k, q):
        src, dst = pairs[p][2 * q:2 * q + 2]
        at = pl.ds(pl.multiple_of(k * step, step), step)
        return pltpu.make_async_copy(src.at[at], dst.at[at], in_sem.at[p, k, q])

    for p in range(4):
        def start(k, _, p=p):
            for q in range(2):
                load(p, k, q).start()
            return 0

        lax.fori_loop(0, CHUNKS, start, 0)

    barrier = pltpu.get_barrier_semaphore()
    stat2[...] = jnp.zeros(stat2.shape, F32)

    def hello(i, _):
        pl.semaphore_signal(barrier, inc=1, device_id=((me + i) % ndev,), device_id_type=pl.DeviceIdType.MESH)
        return 0

    lax.fori_loop(1, ndev, hello, 0)

    def remote(src, dst, s_sem, r_sem, dev):
        return pltpu.make_async_remote_copy(src_ref=src, dst_ref=dst, send_sem=s_sem, recv_sem=r_sem,
                                            device_id=(dev,), device_id_type=pl.DeviceIdType.MESH)

    ones = jnp.ones((16, step), BF16)

    def matmul(p, xb, yb, n, service=None):
        acc[:, :n] = jnp.zeros((width + 16, n), F32)

        def body(k, _):
            load(p, k, 0).wait()
            load(p, k, 1).wait()
            at = pl.ds(pl.multiple_of(k * step, step), step)
            lhs = jnp.concatenate([xb[at, :].T, ones], axis=0)
            acc[:, :n] += jnp.dot(lhs, yb[at, :], preferred_element_type=F32)
            for at_k, fn in (service or {}).items():
                pl.when(k == at_k)(fn)
            return 0

        lax.fori_loop(0, CHUNKS, body, 0)

    def spread(base, n):
        cols = n // LANES
        for j in range(cols):
            gflat[pl.ds(base + j, width, stride=cols), :] = acc[0:width, j * LANES:(j + 1) * LANES]
            gflat[pl.ds(base + cols * width + j, 1), :] = acc[width:width + 1, j * LANES:(j + 1) * LANES]

    def matmul_out():
        cols = width // LANES
        inner = x_out.shape[1]
        acc[...] = jnp.zeros(acc.shape, F32)

        def body(k, _):
            load(0, k, 0).wait()
            load(0, k, 1).wait()
            at = pl.ds(pl.multiple_of(k * step, step), step)
            y = by_out[at, :]
            acc[0:width, :] += jnp.dot(y.T, bx_out[at, :], preferred_element_type=F32)
            acc[width:width + 16, 0:width] += jnp.dot(ones, y, preferred_element_type=F32)
            return 0

        lax.fori_loop(0, CHUNKS, body, 0)
        base = ends[7]
        for j in range(cols):
            gflat[pl.ds(base + j, inner, stride=cols), :] = acc[j * LANES:(j + 1) * LANES, :].T
            gflat[pl.ds(ends[8] + j, 1), :] = acc[width:width + 1, j * LANES:(j + 1) * LANES]

    def send_d(g):
        for q in range(4):
            s = g * 8 + q * 2 + 1 - core
            remote(gflat.at[pl.ds(s * shard, shard)], r_d.at[g * 4 + q, pl.ds(0, shard)],
                   sd_s, sd_r.at[g * 4 + q], partner).start()

    def copy_1(g, b):
        return remote(r_d.at[g * 4 + slot(1 - first, b), pl.ds(0, shard)], r_1.at[g * 2 + b, pl.ds(0, shard)],
                      s1_s, s1_r.at[g * 2 + b], peer1)

    def copy_2(g):
        return remote(r_1.at[g * 2 + 1 - second, pl.ds(0, shard)], r_2.at[g, pl.ds(0, shard)],
                      s2_s, s2_r.at[g], peer2)

    def recv_d(a, b, g):
        q = slot(a, b)
        i = g * 4 + q
        remote(gflat.at[pl.ds(0, shard)], r_d.at[i, pl.ds(0, shard)], sd_s, sd_r.at[i], partner).wait_recv()
        r_d[i, 0:shard, :] += gflat[pl.ds((g * 8 + q * 2 + core) * shard, shard), :]

    def d_to_1(g):
        for b in (1 - second, second):
            recv_d(1 - first, b, g)
            copy_1(g, b).start()
        for b in range(2):
            recv_d(first, b, g)

    def one_to_2(g):
        for b in (1 - second, second):
            i = g * 2 + b
            remote(r_d.at[0, pl.ds(0, shard)], r_1.at[i, pl.ds(0, shard)], s1_s, s1_r.at[i], peer1).wait_recv()
            r_1[i, 0:shard, :] += r_d[g * 4 + slot(first, b), 0:shard, :]
            if b is not second:
                copy_2(g).start()

    def two_to_z(g):
        copy_2(g).wait_recv()
        r_2[g, 0:shard, :] += r_1[g * 2 + second, 0:shard, :]

        @pl.when(zz != g)
        def _():
            remote(r_2.at[g, pl.ds(0, shard)], r_z.at[zz, pl.ds(0, shard)], sz_s, sz_r.at[zz],
                   me + (g - zz) * 8).start()

    scoped('matmul_out', matmul_out)
    small[0].wait()
    cols = width // LANES
    for r, start in enumerate((ends[3], ends[4], ends[9], ends[10])):
        for j in range(cols):
            gflat[pl.ds(start + j, 1), :] = ln_v[r:r + 1, j * LANES:(j + 1) * LANES]
    gflat[pl.ds(ends[11], rows - ends[11]), :] = jnp.zeros((rows - ends[11], LANES), F32)
    def first_send():
        scoped('barrier', pl.semaphore_wait, barrier, ndev - 1)
        send_d(3)

    scoped('mm_qkv', matmul, 1, bx_qkv, by_qkv, 3 * width, {0: first_send, 2: lambda: scoped('in_d1_3', d_to_1, 3)})
    scoped('spread_qkv', spread, 0, 3 * width)
    scoped('mm_proj', matmul, 2, bx_proj, by_proj, width)
    scoped('spread_proj', spread, ends[1], width)
    scoped('send_d_0', send_d, 0)
    scoped('mm_inter', matmul, 3, bx_inter, by_inter, 4 * width,
           {1: lambda: scoped('in_d1_0', d_to_1, 0), 2: lambda: scoped('in_12_3', one_to_2, 3)})
    scoped('spread_inter', spread, ends[5], 4 * width)
    scoped('send_d_1', send_d, 1)
    scoped('send_d_2', send_d, 2)
    scoped('d_to_1_1', d_to_1, 1)
    scoped('d_to_1_2', d_to_1, 2)
    scoped('one_to_2_0', one_to_2, 0)
    scoped('two_to_z_3', two_to_z, 3)
    scoped('one_to_2_1', one_to_2, 1)
    scoped('two_to_z_0', two_to_z, 0)
    scoped('one_to_2_2', one_to_2, 2)
    scoped('two_to_z_1', two_to_z, 1)
    scoped('two_to_z_2', two_to_z, 2)

    for copy in small[1:]:
        scoped('wait_state', copy.wait)
    lane = lax.broadcasted_iota(jnp.int32, (shard, LANES), 1)
    row = lax.broadcasted_iota(jnp.int32, (shard, LANES), 0) + me * shard
    seg = jnp.zeros((shard, LANES), jnp.int32)
    for end in ends:
        seg = seg + jnp.where(row >= end, 1, 0)
    mine = lane == seg
    w = w_v[...]

    def seg_sums(val):
        per_row = jnp.sum(val, axis=1, keepdims=True)
        return jnp.sum(jnp.where(mine, per_row, 0.0), axis=0, keepdims=True)

    w_sums = seg_sums(w * w)

    g = r_2[zz, 0:shard, :]
    for d in range(1, PARTS):
        src = (zz + d) % PARTS
        scoped('wait_z', remote(r_2.at[0, pl.ds(0, shard)], r_z.at[src, pl.ds(0, shard)], sz_s, sz_r.at[src], me).wait_recv)
        g = g + r_z[src, 0:shard, :]
    g = g * (1.0 / ndev)

    def put(stat, value, s_sem, r_sem, lo, hi):
        stat[pl.ds(me, 1), :] = value

        def send(i, _):
            remote(stat.at[pl.ds(me, 1)], stat.at[pl.ds(me, 1)], s_sem, r_sem, (me + i) % ndev).start()
            return 0

        lax.fori_loop(lo, hi, send, 0)

    def rows_in(stat, count, sem):
        return pltpu.make_async_copy(stat.at[pl.ds(0, count)], stat.at[pl.ds(0, count)], sem)

    one_lane = lax.broadcasted_iota(jnp.int32, (1, LANES), 1)
    g_sq = jnp.sum(jnp.sum(g * g, axis=0, keepdims=True), axis=1, keepdims=True)
    put(stat1, jnp.where(one_lane == 64, g_sq, w_sums), t1_s, t1_r, 1, ndev)
    scoped('wait_stat1', rows_in(stat1, ndev - 1, t1_r).wait)
    total1 = jnp.sum(stat1[...], axis=0, keepdims=True)
    gn = jnp.sqrt(jnp.sum(jnp.where(one_lane == 64, total1, 0.0), axis=1, keepdims=True))
    h = g / jnp.maximum(1.0, gn)
    new_m = BETA_ONE * m_v[...] + (1.0 - BETA_ONE) * h
    new_v = BETA_TWO * v_v[...] + (1.0 - BETA_TWO) * h * h
    decay = jnp.where((seg == 0) | (seg == 2) | (seg == 6) | (seg == 8), DECAY, 0.0)
    u = (new_m / CORR_ONE) / (jnp.sqrt(new_v / CORR_TWO) + EPSILON) + decay * w
    plane = ndev // PARTS
    starts = [0] + ends[:-1]
    assert all((end - 1) // (plane * shard) - start // (plane * shard) <= 1 for start, end in zip(starts, ends))
    stat2[pl.ds(me, 1), :] = seg_sums(u * u)

    def send2(i, _, d):
        to = zz * plane + i

        @pl.when((to >= 0) & (to < ndev) & (to != me))
        def _():
            remote(stat2.at[pl.ds(me, 1)], stat2.at[pl.ds(me, 1)], t2_s.at[d + 1], t2_r.at[zz], to).start()

        return 0

    for d in (-1, 1, 0):
        lax.fori_loop(d * plane, (d + 1) * plane, functools.partial(send2, d=d), 0)

    def each_plane(fn):
        fn(1, zz, plane - 1)
        pl.when(zz > 0)(lambda: fn(0, zz - 1, plane))
        pl.when(zz < PARTS - 1)(lambda: fn(2, zz + 1, plane))

    scoped('wait_stat2', each_plane, lambda d, src, count: rows_in(stat2, count, t2_r.at[src]).wait())
    total2 = jnp.sum(stat2[...], axis=0, keepdims=True)
    nm_out[...] = new_m
    nv_out[...] = new_v
    w_norm, u_norm = jnp.sqrt(total1), jnp.sqrt(total2)
    ratio = jnp.where((w_norm > 0) & (u_norm > 0), w_norm / jnp.where(u_norm > 0, u_norm, 1.0), 1.0)
    per_row = jnp.sum(jnp.where(mine, ratio, 0.0), axis=1, keepdims=True)
    new_w = w - LEARN_RATE * per_row * u
    nw_out[...] = new_w
    wfull[pl.ds(me * shard, shard), :] = new_w
    split = (shard + 1) // 2
    parts = ((0, split), (split, shard - split))

    def part_at(s, h):
        return wfull.at[pl.ds(s * shard + parts[h][0], parts[h][1])]

    sent = []

    def push(s, h, *devs):
        for dev in devs:
            remote(part_at(s, h), part_at(s, h), ag_s, ag_r.at[s, h], dev).start()
            sent.append(parts[h][1])

    def arrived(s, h):
        remote(part_at(s, h), part_at(s, h), ag_s, ag_r.at[s, h], me).wait_recv()

    zs = [zz, zz + 1 - 2 * (zz % 2), 3 - zz, zz + 2 - 4 * (zz // 2)]
    diag = peer1 + peer2 - me

    def shifted(s, j):
        return s + (zs[j] - zz) * 8

    for h in range(2):
        push(me, h, peer2, peer1, shifted(me, 1), shifted(me, 2), shifted(me, 3), partner)
    for kind, j in (('a', 0), ('z', 1), ('z', 2), ('a', 1), ('z', 3), ('a', 2), ('a', 3), ('b', 0), ('d', 0), ('b', 1),
                    ('d', 1), ('b', 2), ('d', 2), ('b', 3), ('d', 3)):
        s = shifted({'a': peer1, 'z': me, 'b': peer2, 'd': diag}[kind], j)
        for h in range(2):
            scoped('got_%s%d' % (kind, j), arrived, s, h)
            push(s, h, *{'a': (peer2, partner), 'z': (peer2, peer1, partner)}.get(kind, (partner,)))

    def rest(k, _):
        for h in range(2):
            arrived(2 * k + 1 - core, h)
        return 0

    scoped('got_rest', lax.fori_loop, 0, ndev // 2, rest, 0)
    par_out[...] = wfull[...].astype(BF16)

    def all_sent(buf, count, sem):
        pltpu.make_async_copy(buf.at[pl.ds(0, count)], buf.at[pl.ds(0, count)], sem).wait()

    scoped('all_sent_gflat', all_sent, gflat, 16 * shard, sd_s)
    scoped('all_sent_gflat', all_sent, gflat, 8 * shard, s1_s)
    scoped('all_sent_gflat', all_sent, gflat, 4 * shard, s2_s)
    scoped('all_sent_gflat', all_sent, gflat, 3 * shard, sz_s)
    scoped('all_sent_stat1', all_sent, stat1, ndev - 1, t1_s)
    each_plane(lambda d, src, count: rows_in(stat2, count, t2_s.at[d]).wait())
    scoped('all_sent_wfull', all_sent, wfull, sum(sent), ag_s)


def write_kernel(*refs):
    sem = refs[-1]
    half = len(refs) // 2
    copies = [pltpu.make_async_copy(src, dst, sem.at[i]) for i, (src, dst) in enumerate(zip(refs[:half], refs[half:-1]))]
    for copy in reversed(copies):
        copy.start()
    for copy in copies:
        copy.wait()


def solution(mesh):
    ndev = mesh.shape['dp']

    def local_step(weights, moment_one, moment_two, x_qkv, dy_qkv, x_proj, dy_proj, x_inter, dy_inter, x_out, dy_out, ln_grad):
        width = x_qkv.shape[1]
        shard = weights.shape[0] // LANES
        rows = shard * ndev
        flat = lambda a: a.reshape(-1, LANES)
        acts = (x_qkv, dy_qkv, x_proj, dy_proj, x_inter, dy_inter, x_out, dy_out)
        vm = pltpu.VMEM
        pad = -(-shard // 8) * 8
        state = jax.ShapeDtypeStruct((shard, LANES), F32)
        mid = (vm((shard, LANES), F32),) * 3 + (vm((rows, LANES), BF16),)
        dma = pltpu.SemaphoreType.DMA
        hbm = pl.BlockSpec(memory_space=pltpu.HBM)
        whole = pl.BlockSpec(memory_space=pltpu.VMEM)
        out_shape = (state, state, state, jax.ShapeDtypeStruct((rows, LANES), BF16))
        outs = pl.pallas_call(
            functools.partial(comm_kernel, (width, shard, ndev, rows)),
            out_shape=mid,
            in_specs=[hbm] * 12,
            out_specs=(whole,) * 4,
            scratch_shapes=[vm(a.shape, BF16) for a in acts] + [
                vm((4, width), F32)] + [vm((shard, LANES), F32)] * 3 + [
                vm((width + 16, 4 * width), F32), vm((rows, LANES), F32),
                vm((16, pad, LANES), F32), vm((8, pad, LANES), F32), vm((4, pad, LANES), F32), vm((4, pad, LANES), F32),
                vm((ndev, LANES), F32), vm((ndev, LANES), F32), vm((rows, LANES), F32),
                dma((4, CHUNKS, 2)), dma((4,)), dma, dma((16,)), dma, dma((8,)), dma, dma((4,)), dma, dma((4,)),
                dma, dma, dma((3,)), dma((PARTS,)), dma, dma((ndev, 2))],
            compiler_params=pltpu.CompilerParams(collective_id=0, has_side_effects=True, vmem_limit_bytes=61 * 2 ** 20),
            name='lamb_step',
        )(*acts, ln_grad.reshape(4, width), flat(weights), flat(moment_one), flat(moment_two))
        new_w, new_m, new_v, params = pl.pallas_call(
            write_kernel, out_shape=out_shape, in_specs=[whole] * 4, out_specs=(hbm,) * 4,
            scratch_shapes=[dma((4,))], name='write_out')(*[pltpu.with_memory_space_constraint(a, pltpu.VMEM) for a in outs])
        return new_w.reshape(-1), new_m.reshape(-1), new_v.reshape(-1), params.reshape(-1)

    row_spec = P('dp', None)
    in_specs = (P('dp'), P('dp'), P('dp'), row_spec, row_spec, row_spec, row_spec, row_spec, row_spec, row_spec, row_spec, P('dp', None, None))
    out_specs = (P('dp'), P('dp'), P('dp'), P())
    return jax.shard_map(local_step, mesh=mesh, in_specs=in_specs, out_specs=out_specs, check_vma=False)
```

```python
import functools

import jax
import jax.numpy as jnp
from jax import lax
from jax.experimental import pallas as pl
from jax.experimental.pallas import tpu as pltpu
from jax.sharding import PartitionSpec as P

STEP = 10
LEARN_RATE = 0.5
BETA_ONE = 0.9
BETA_TWO = 0.999
EPSILON = 1e-6
DECAY = 0.01
CORR_ONE = 1.0 - BETA_ONE ** STEP
CORR_TWO = 1.0 - BETA_TWO ** STEP

LANES = 128
CHUNKS = 4
PARTS = 4
F32 = jnp.float32
BF16 = jnp.bfloat16


def tensor_sizes(width):
    return [3 * width * width, 3 * width, width * width, width, width, width,
            4 * width * width, 4 * width, 4 * width * width, width, width, width]


def row_ends(width):
    ends, total = [], 0
    for size in tensor_sizes(width):
        total += size // LANES
        ends.append(total)
    return ends


def scoped(name, fn, *args):
    with jax.named_scope(name):
        return fn(*args)


def comm_kernel(dims, x_qkv, dy_qkv, x_proj, dy_proj, x_inter, dy_inter, x_out, dy_out, ln, w_in, m_in, v_in,
                nw_out, nm_out, nv_out, par_out,
                xb, yb, ln_v, w_v, m_v, v_v, acc, bias_out, gflat, r_d, r_1, r_2, r_z, stat1, stat2, wfull,
                in_sem, in2_sem, st_sem, sd_s, sd_r, s1_s, s1_r, s2_s, s2_r, sz_s, sz_r,
                t1_s, t1_r, t2_s, t2_r, ag_s, ag_r, agp_r):
    width, shard, ndev, rows = dims
    tokens = x_qkv.shape[0]
    step = tokens // CHUNKS
    ends = row_ends(width)
    me = lax.axis_index('dp')
    core, xx, yy, zz = me % 2, (me // 2) % 2, (me // 4) % 2, me // 8
    partner = me + 1 - 2 * core
    first = xx * (1 - core) + yy * core
    second = yy * (1 - core) + xx * core
    peer1 = me + (1 - 2 * first) * (2 * (1 - core) + 4 * core)
    peer2 = me + (1 - 2 * second) * (4 * (1 - core) + 2 * core)

    def slot(a, b):
        return (1 - core) * (2 * b + a) + core * (2 * a + b)

    small = [pltpu.make_async_copy(s, d, st_sem.at[i])
             for i, (s, d) in enumerate(((ln, ln_v), (w_in, w_v), (m_in, m_v), (v_in, v_v)))]
    for copy in small:
        copy.start()
    wide = 4 * width
    cut = 3 * width
    groups = (((dy_out, xb, 0, 0), (x_out, yb, 0, 0)),
              ((x_qkv, xb, 1, 0), (x_proj, xb, 2, 0), (dy_qkv, yb, 1, 0), (dy_proj, yb, 1, cut)),
              ((x_inter, xb, 3, 0), (dy_inter, yb, 2, 0)))
    for m, group in enumerate(groups):
        def start(k, _, m=m, group=group):
            at = pl.ds(pl.multiple_of(k * step, step), step)
            for src, dst, slab, col in group:
                to = dst.at[slab, at] if src.shape[1] == dst.shape[2] else dst.at[slab, at, pl.ds(col, src.shape[1])]
                sem = in2_sem.at[k] if slab == 2 and dst is xb else in_sem.at[m * CHUNKS + k]
                pltpu.make_async_copy(src.at[at], to, sem).start()
            return 0

        lax.fori_loop(0, CHUNKS, start, 0)

    barrier = pltpu.get_barrier_semaphore()
    stat2[...] = jnp.zeros(stat2.shape, F32)

    def hello(i, _):
        pl.semaphore_signal(barrier, inc=1, device_id=((me + i) % ndev,), device_id_type=pl.DeviceIdType.MESH)
        return 0

    lax.fori_loop(1, ndev, hello, 0)

    def remote(src, dst, s_sem, r_sem, dev):
        return pltpu.make_async_remote_copy(src_ref=src, dst_ref=dst, send_sem=s_sem, recv_sem=r_sem,
                                            device_id=(dev,), device_id_type=pl.DeviceIdType.MESH)

    ones = jnp.ones((16, step), BF16)
    acc[...] = jnp.zeros(acc.shape, F32)
    bias_out[...] = jnp.zeros(bias_out.shape, F32)

    def products(i, _):
        m, k = i // CHUNKS, i % CHUNKS
        both = yb.at[0, pl.ds(0, step * 5 // 4)]
        pltpu.make_async_copy(both, both, in_sem.at[i]).wait()

        @pl.when(m == 1)
        def _():
            half = xb.at[2, pl.ds(0, step)]
            pltpu.make_async_copy(half, half, in2_sem.at[k]).wait()

        at = pl.ds(pl.multiple_of(k * step, step), step)
        lhs1 = jnp.concatenate([xb[m + m // 2, at, :].T, ones], axis=0)
        acc[m, :, 0:cut] += jnp.dot(lhs1, yb[m, at, 0:cut], preferred_element_type=F32)
        lhs2 = jnp.concatenate([xb[2 * m - m // 2, at, :].T, ones], axis=0)
        acc[m, :, cut:wide] += jnp.dot(lhs2, yb[m, at, cut:wide], preferred_element_type=F32)

        @pl.when(m == 0)
        def _():
            bias_out[...] += jnp.dot(ones, xb[0, at, :], preferred_element_type=F32)

        for at_i, fn in services.items():
            pl.when(i == at_i)(fn)
        return 0

    def spread(base, m, lo, n):
        cols = n // LANES
        for j in range(cols):
            at = slice(lo + j * LANES, lo + (j + 1) * LANES)
            gflat[pl.ds(base + j, width, stride=cols), :] = acc[m, 0:width, at]
            gflat[pl.ds(base + cols * width + j, 1), :] = acc[m, width:width + 1, at]

    def spread_out():
        cols = width // LANES
        for j in range(cols):
            at = slice(j * LANES, (j + 1) * LANES)
            gflat[pl.ds(ends[7] + j, wide, stride=cols), :] = acc[0, at, :].T
            gflat[pl.ds(ends[8] + j, 1), :] = bias_out[0:1, at]
        small[0].wait()
        for r, start in enumerate((ends[3], ends[4], ends[9], ends[10])):
            for j in range(cols):
                gflat[pl.ds(start + j, 1), :] = ln_v[r:r + 1, j * LANES:(j + 1) * LANES]
        gflat[pl.ds(ends[11], rows - ends[11]), :] = jnp.zeros((rows - ends[11], LANES), F32)

    def send_d(g):
        for q in range(4):
            s = g * 8 + q * 2 + 1 - core
            remote(gflat.at[pl.ds(s * shard, shard)], r_d.at[g * 4 + q, pl.ds(0, shard)],
                   sd_s, sd_r.at[g], partner).start()

    def copy_1(g, b):
        return remote(r_d.at[g * 4 + slot(1 - first, b), pl.ds(0, shard)], r_1.at[g * 2 + b, pl.ds(0, shard)],
                      s1_s, s1_r.at[g * 2 + b], peer1)

    def copy_2(g):
        return remote(r_1.at[g * 2 + 1 - second, pl.ds(0, shard)], r_2.at[g, pl.ds(0, shard)],
                      s2_s, s2_r.at[g], peer2)

    def add_d(a, b, g):
        q = slot(a, b)
        i = g * 4 + q
        r_d[i, 0:shard, :] += gflat[pl.ds((g * 8 + q * 2 + core) * shard, shard), :]

    def d_to_1(g):
        four = gflat.at[pl.ds(0, 4 * shard)]
        pltpu.make_async_copy(four, four, sd_r.at[g]).wait()
        for b in (1 - second, second):
            add_d(1 - first, b, g)
            copy_1(g, b).start()
        for b in range(2):
            add_d(first, b, g)

    def one_to_2(g):
        for b in (1 - second, second):
            i = g * 2 + b
            remote(r_d.at[0, pl.ds(0, shard)], r_1.at[i, pl.ds(0, shard)], s1_s, s1_r.at[i], peer1).wait_recv()
            r_1[i, 0:shard, :] += r_d[g * 4 + slot(first, b), 0:shard, :]
            if b is not second:
                copy_2(g).start()

    def two_to_z(g):
        copy_2(g).wait_recv()
        r_2[g, 0:shard, :] += r_1[g * 2 + second, 0:shard, :]

        @pl.when(zz != g)
        def _():
            remote(r_2.at[g, pl.ds(0, shard)], r_z.at[zz, pl.ds(0, shard)], sz_s, sz_r.at[zz],
                   me + (g - zz) * 8).start()

    def after_out():
        scoped('spread_out', spread_out)
        scoped('barrier', pl.semaphore_wait, barrier, ndev - 1)
        send_d(3)

    def after_qkv():
        scoped('spread_qkv', spread, 0, 1, 0, cut)
        scoped('spread_proj', spread, ends[1], 1, cut, width)
        send_d(0)

    services = {CHUNKS - 1: after_out,
                CHUNKS + 1: lambda: scoped('in_d1_3', d_to_1, 3),
                2 * CHUNKS - 1: after_qkv,
                2 * CHUNKS + 1: lambda: scoped('in_d1_0', d_to_1, 0),
                2 * CHUNKS + 2: lambda: scoped('in_12_3', one_to_2, 3)}
    scoped('products', lax.fori_loop, 0, 3 * CHUNKS, products, 0)
    scoped('spread_inter', spread, ends[5], 2, 0, wide)
    scoped('send_d_1', send_d, 1)
    scoped('send_d_2', send_d, 2)
    scoped('d_to_1_1', d_to_1, 1)
    scoped('d_to_1_2', d_to_1, 2)
    scoped('one_to_2_0', one_to_2, 0)
    scoped('two_to_z_3', two_to_z, 3)
    scoped('one_to_2_1', one_to_2, 1)
    scoped('two_to_z_0', two_to_z, 0)
    scoped('one_to_2_2', one_to_2, 2)
    scoped('two_to_z_1', two_to_z, 1)
    scoped('two_to_z_2', two_to_z, 2)

    for copy in small[1:]:
        scoped('wait_state', copy.wait)
    lane = lax.broadcasted_iota(jnp.int32, (shard, LANES), 1)
    row = lax.broadcasted_iota(jnp.int32, (shard, LANES), 0) + me * shard
    seg = jnp.zeros((shard, LANES), jnp.int32)
    for end in ends:
        seg = seg + jnp.where(row >= end, 1, 0)
    mine = lane == seg
    w = w_v[...]

    def seg_sums(val):
        per_row = jnp.sum(val, axis=1, keepdims=True)
        return jnp.sum(jnp.where(mine, per_row, 0.0), axis=0, keepdims=True)

    w_sums = seg_sums(w * w)

    g = r_2[zz, 0:shard, :]
    for d in range(1, PARTS):
        src = (zz + d) % PARTS
        scoped('wait_z', remote(r_2.at[0, pl.ds(0, shard)], r_z.at[src, pl.ds(0, shard)], sz_s, sz_r.at[src], me).wait_recv)
        g = g + r_z[src, 0:shard, :]
    g = g * (1.0 / ndev)

    def put(stat, value, s_sem, r_sem, lo, hi):
        stat[pl.ds(me, 1), :] = value

        def send(i, _):
            remote(stat.at[pl.ds(me, 1)], stat.at[pl.ds(me, 1)], s_sem, r_sem, (me + i) % ndev).start()
            return 0

        lax.fori_loop(lo, hi, send, 0)

    def rows_in(stat, count, sem):
        return pltpu.make_async_copy(stat.at[pl.ds(0, count)], stat.at[pl.ds(0, count)], sem)

    one_lane = lax.broadcasted_iota(jnp.int32, (1, LANES), 1)
    g_sq = jnp.sum(jnp.sum(g * g, axis=0, keepdims=True), axis=1, keepdims=True)
    put(stat1, jnp.where(one_lane == 64, g_sq, w_sums), t1_s, t1_r, 1, ndev)
    scoped('wait_stat1', rows_in(stat1, ndev - 1, t1_r).wait)
    total1 = jnp.sum(stat1[...], axis=0, keepdims=True)
    gn = jnp.sqrt(jnp.sum(jnp.where(one_lane == 64, total1, 0.0), axis=1, keepdims=True))
    h = g / jnp.maximum(1.0, gn)
    new_m = BETA_ONE * m_v[...] + (1.0 - BETA_ONE) * h
    new_v = BETA_TWO * v_v[...] + (1.0 - BETA_TWO) * h * h
    decay = jnp.where((seg == 0) | (seg == 2) | (seg == 6) | (seg == 8), DECAY, 0.0)
    u = (new_m / CORR_ONE) / (jnp.sqrt(new_v / CORR_TWO) + EPSILON) + decay * w
    plane = ndev // PARTS
    starts = [0] + ends[:-1]
    assert all((end - 1) // (plane * shard) - start // (plane * shard) <= 1 for start, end in zip(starts, ends))
    stat2[pl.ds(me, 1), :] = seg_sums(u * u)

    def send2(i, _, d):
        to = zz * plane + i

        @pl.when((to >= 0) & (to < ndev) & (to != me))
        def _():
            remote(stat2.at[pl.ds(me, 1)], stat2.at[pl.ds(me, 1)], t2_s.at[d + 1], t2_r.at[zz], to).start()

        return 0

    for d in (-1, 1, 0):
        lax.fori_loop(d * plane, (d + 1) * plane, functools.partial(send2, d=d), 0)

    def each_plane(fn):
        fn(1, zz, plane - 1)
        pl.when(zz > 0)(lambda: fn(0, zz - 1, plane))
        pl.when(zz < PARTS - 1)(lambda: fn(2, zz + 1, plane))

    scoped('wait_stat2', each_plane, lambda d, src, count: rows_in(stat2, count, t2_r.at[src]).wait())
    total2 = jnp.sum(stat2[...], axis=0, keepdims=True)
    nm_out[...] = new_m
    nv_out[...] = new_v
    w_norm, u_norm = jnp.sqrt(total1), jnp.sqrt(total2)
    ratio = jnp.where((w_norm > 0) & (u_norm > 0), w_norm / jnp.where(u_norm > 0, u_norm, 1.0), 1.0)
    per_row = jnp.sum(jnp.where(mine, ratio, 0.0), axis=1, keepdims=True)
    new_w = w - LEARN_RATE * per_row * u
    nw_out[...] = new_w
    wfull[pl.ds(me * shard, shard), :] = new_w
    split = (shard + 1) // 2
    parts = ((0, split), (split, shard - split))

    def part_at(s, h):
        return wfull.at[pl.ds(s * shard + parts[h][0], parts[h][1])]

    sent = []

    def push(s, h, *devs):
        for dev in devs:
            sem = agp_r if dev is partner else ag_r.at[s // 2, h]
            remote(part_at(s, h), part_at(s, h), ag_s, sem, dev).start()
            sent.append(parts[h][1])

    def arrived(s, h):
        remote(part_at(s, h), part_at(s, h), ag_s, ag_r.at[s // 2, h], me).wait_recv()

    zs = [zz, zz + 1 - 2 * (zz % 2), 3 - zz, zz + 2 - 4 * (zz // 2)]
    diag = peer1 + peer2 - me

    def shifted(s, j):
        return s + (zs[j] - zz) * 8

    for h in range(2):
        push(me, h, peer2, peer1, shifted(me, 1), shifted(me, 2), shifted(me, 3), partner)
    for kind, j in (('a', 0), ('z', 1), ('z', 2), ('a', 1), ('z', 3), ('a', 2), ('a', 3), ('b', 0), ('d', 0), ('b', 1),
                    ('d', 1), ('b', 2), ('d', 2), ('b', 3), ('d', 3)):
        s = shifted({'a': peer1, 'z': me, 'b': peer2, 'd': diag}[kind], j)
        for h in range(2):
            scoped('got_%s%d' % (kind, j), arrived, s, h)
            push(s, h, *{'a': (peer2, partner), 'z': (peer2, peer1, partner)}.get(kind, (partner,)))

    theirs = wfull.at[pl.ds(0, ndev // 2 * shard)]
    scoped('got_rest', pltpu.make_async_copy(theirs, theirs, agp_r).wait)
    par_out[...] = wfull[...].astype(BF16)

    def all_sent(buf, count, sem):
        pltpu.make_async_copy(buf.at[pl.ds(0, count)], buf.at[pl.ds(0, count)], sem).wait()

    scoped('all_sent_gflat', all_sent, gflat, 16 * shard, sd_s)
    scoped('all_sent_gflat', all_sent, gflat, 8 * shard, s1_s)
    scoped('all_sent_gflat', all_sent, gflat, 4 * shard, s2_s)
    scoped('all_sent_gflat', all_sent, gflat, 3 * shard, sz_s)
    scoped('all_sent_stat1', all_sent, stat1, ndev - 1, t1_s)
    each_plane(lambda d, src, count: rows_in(stat2, count, t2_s.at[d]).wait())
    scoped('all_sent_wfull', all_sent, wfull, sum(sent), ag_s)


def write_kernel(*refs):
    sem = refs[-1]
    half = len(refs) // 2
    copies = [pltpu.make_async_copy(src, dst, sem.at[i]) for i, (src, dst) in enumerate(zip(refs[:half], refs[half:-1]))]
    for copy in reversed(copies):
        copy.start()
    for copy in copies:
        copy.wait()


def solution(mesh):
    ndev = mesh.shape['dp']

    def local_step(weights, moment_one, moment_two, x_qkv, dy_qkv, x_proj, dy_proj, x_inter, dy_inter, x_out, dy_out, ln_grad):
        tokens, width = x_qkv.shape
        shard = weights.shape[0] // LANES
        rows = shard * ndev
        flat = lambda a: a.reshape(-1, LANES)
        acts = (x_qkv, dy_qkv, x_proj, dy_proj, x_inter, dy_inter, x_out, dy_out)
        vm = pltpu.VMEM
        pad = -(-shard // 8) * 8
        state = jax.ShapeDtypeStruct((shard, LANES), F32)
        mid = (vm((shard, LANES), F32),) * 3 + (vm((rows, LANES), BF16),)
        dma = pltpu.SemaphoreType.DMA
        hbm = pl.BlockSpec(memory_space=pltpu.HBM)
        whole = pl.BlockSpec(memory_space=pltpu.VMEM)
        out_shape = (state, state, state, jax.ShapeDtypeStruct((rows, LANES), BF16))
        outs = pl.pallas_call(
            functools.partial(comm_kernel, (width, shard, ndev, rows)),
            out_shape=mid,
            in_specs=[hbm] * 12,
            out_specs=(whole,) * 4,
            scratch_shapes=[
                vm((4, tokens, width), BF16), vm((3, tokens, 4 * width), BF16), vm((4, width), F32)] + [
                vm((shard, LANES), F32)] * 3 + [
                vm((3, width + 16, 4 * width), F32), vm((16, width), F32), vm((rows, LANES), F32),
                vm((16, pad, LANES), F32), vm((8, pad, LANES), F32), vm((4, pad, LANES), F32), vm((4, pad, LANES), F32),
                vm((ndev, LANES), F32), vm((ndev, LANES), F32), vm((rows, LANES), F32),
                dma((3 * CHUNKS,)), dma((CHUNKS,)), dma((4,)), dma, dma((4,)), dma, dma((8,)), dma, dma((4,)), dma, dma((4,)),
                dma, dma, dma((3,)), dma((PARTS,)), dma, dma((ndev // 2, 2)), dma],
            compiler_params=pltpu.CompilerParams(collective_id=0, has_side_effects=True, vmem_limit_bytes=61 * 2 ** 20),
            name='lamb_step',
        )(*acts, ln_grad.reshape(4, width), flat(weights), flat(moment_one), flat(moment_two))
        new_w, new_m, new_v, params = pl.pallas_call(
            write_kernel, out_shape=out_shape, in_specs=[whole] * 4, out_specs=(hbm,) * 4,
            scratch_shapes=[dma((4,))], name='write_out')(*[pltpu.with_memory_space_constraint(a, pltpu.VMEM) for a in outs])
        return new_w.reshape(-1), new_m.reshape(-1), new_v.reshape(-1), params.reshape(-1)

    row_spec = P('dp', None)
    in_specs = (P('dp'), P('dp'), P('dp'), row_spec, row_spec, row_spec, row_spec, row_spec, row_spec, row_spec, row_spec, P('dp', None, None))
    out_specs = (P('dp'), P('dp'), P('dp'), P())
    return jax.shard_map(local_step, mesh=mesh, in_specs=in_specs, out_specs=out_specs, check_vma=False)
```

```python
import functools

import jax
import jax.numpy as jnp
from jax import lax
from jax.experimental import pallas as pl
from jax.experimental.pallas import tpu as pltpu
from jax.sharding import PartitionSpec as P

STEP = 10
LEARN_RATE = 0.5
BETA_ONE = 0.9
BETA_TWO = 0.999
EPSILON = 1e-6
DECAY = 0.01
CORR_ONE = 1.0 - BETA_ONE ** STEP
CORR_TWO = 1.0 - BETA_TWO ** STEP

LANES = 128
CHUNKS = 2
PARTS = 4
F32 = jnp.float32
BF16 = jnp.bfloat16


def tensor_sizes(width):
    return [3 * width * width, 3 * width, width * width, width, width, width,
            4 * width * width, 4 * width, 4 * width * width, width, width, width]


def row_ends(width):
    ends, total = [], 0
    for size in tensor_sizes(width):
        total += size // LANES
        ends.append(total)
    return ends


def scoped(name, fn, *args):
    with jax.named_scope(name):
        return fn(*args)


def comm_kernel(dims, x_qkv, dy_qkv, x_proj, dy_proj, x_inter, dy_inter, x_out, dy_out, ln, w_in, m_in, v_in,
                nw_out, nm_out, nv_out, par_out,
                xb, yb, ln_v, w_v, m_v, v_v, acc, bias_out, gflat, r_d, r_1, r_2, r_z, stat1, stat2, wfull,
                in_sem, in2_sem, st_sem, sd_s, sd_r, s1_s, s1_r, s2_s, s2_r, sz_s, sz_r,
                t1_s, t1_r, t2_s, t2_r, ag_s, ag_r, agp_r):
    width, shard, ndev, rows = dims
    tokens = x_qkv.shape[0]
    step = tokens // CHUNKS
    ends = row_ends(width)
    me = lax.axis_index('dp')
    core, xx, yy, zz = me % 2, (me // 2) % 2, (me // 4) % 2, me // 8
    partner = me + 1 - 2 * core
    first = xx * (1 - core) + yy * core
    second = yy * (1 - core) + xx * core
    peer1 = me + (1 - 2 * first) * (2 * (1 - core) + 4 * core)
    peer2 = me + (1 - 2 * second) * (4 * (1 - core) + 2 * core)

    def slot(a, b):
        return (1 - core) * (2 * b + a) + core * (2 * a + b)

    small = [pltpu.make_async_copy(s, d, st_sem.at[i])
             for i, (s, d) in enumerate(((ln, ln_v), (w_in, w_v), (m_in, m_v), (v_in, v_v)))]
    for copy in small:
        copy.start()
    wide = 4 * width
    cut = 3 * width
    groups = (((dy_out, xb, 0, 0), (x_out, yb, 0, 0)),
              ((x_qkv, xb, 1, 0), (x_proj, xb, 2, 0), (dy_qkv, yb, 1, 0), (dy_proj, yb, 1, cut)),
              ((x_inter, xb, 3, 0), (dy_inter, yb, 2, 0)))
    for m, group in enumerate(groups):
        def start(k, _, m=m, group=group):
            at = pl.ds(pl.multiple_of(k * step, step), step)
            for src, dst, slab, col in group:
                to = dst.at[slab, at] if src.shape[1] == dst.shape[2] else dst.at[slab, at, pl.ds(col, src.shape[1])]
                sem = in2_sem.at[k] if slab == 2 and dst is xb else in_sem.at[m * CHUNKS + k]
                pltpu.make_async_copy(src.at[at], to, sem).start()
            return 0

        lax.fori_loop(0, CHUNKS, start, 0)

    barrier = pltpu.get_barrier_semaphore()
    stat2[...] = jnp.zeros(stat2.shape, F32)

    def hello(i, _):
        pl.semaphore_signal(barrier, inc=1, device_id=((me + i) % ndev,), device_id_type=pl.DeviceIdType.MESH)
        return 0

    lax.fori_loop(1, ndev, hello, 0)

    def remote(src, dst, s_sem, r_sem, dev):
        return pltpu.make_async_remote_copy(src_ref=src, dst_ref=dst, send_sem=s_sem, recv_sem=r_sem,
                                            device_id=(dev,), device_id_type=pl.DeviceIdType.MESH)

    ones = jnp.ones((16, step), BF16)
    acc[...] = jnp.zeros(acc.shape, F32)
    bias_out[...] = jnp.zeros(bias_out.shape, F32)

    def products(i, _):
        m, k = i // CHUNKS, i % CHUNKS
        both = yb.at[0, pl.ds(0, step * 5 // 4)]
        pltpu.make_async_copy(both, both, in_sem.at[i]).wait()

        @pl.when(m == 1)
        def _():
            half = xb.at[2, pl.ds(0, step)]
            pltpu.make_async_copy(half, half, in2_sem.at[k]).wait()

        at = pl.ds(pl.multiple_of(k * step, step), step)
        lhs1 = jnp.concatenate([xb[m + m // 2, at, :].T, ones], axis=0)
        acc[m, :, 0:cut] += jnp.dot(lhs1, yb[m, at, 0:cut], preferred_element_type=F32)
        lhs2 = jnp.concatenate([xb[2 * m - m // 2, at, :].T, ones], axis=0)
        acc[m, :, cut:wide] += jnp.dot(lhs2, yb[m, at, cut:wide], preferred_element_type=F32)

        @pl.when(m == 0)
        def _():
            bias_out[...] += jnp.dot(ones, xb[0, at, :], preferred_element_type=F32)

        for at_i, fn in services.items():
            pl.when(i == at_i)(fn)
        return 0

    def spread(base, m, lo, n):
        cols = n // LANES
        for j in range(cols):
            at = slice(lo + j * LANES, lo + (j + 1) * LANES)
            gflat[pl.ds(base + j, width, stride=cols), :] = acc[m, 0:width, at]
            gflat[pl.ds(base + cols * width + j, 1), :] = acc[m, width:width + 1, at]

    def spread_out():
        cols = width // LANES
        for j in range(cols):
            at = slice(j * LANES, (j + 1) * LANES)
            gflat[pl.ds(ends[7] + j, wide, stride=cols), :] = acc[0, at, :].T
            gflat[pl.ds(ends[8] + j, 1), :] = bias_out[0:1, at]
        small[0].wait()
        for r, start in enumerate((ends[3], ends[4], ends[9], ends[10])):
            for j in range(cols):
                gflat[pl.ds(start + j, 1), :] = ln_v[r:r + 1, j * LANES:(j + 1) * LANES]
        gflat[pl.ds(ends[11], rows - ends[11]), :] = jnp.zeros((rows - ends[11], LANES), F32)

    def send_d(g):
        for q in range(4):
            s = g * 8 + q * 2 + 1 - core
            remote(gflat.at[pl.ds(s * shard, shard)], r_d.at[g * 4 + q, pl.ds(0, shard)],
                   sd_s, sd_r.at[g], partner).start()

    def copy_1(g, b):
        return remote(r_d.at[g * 4 + slot(1 - first, b), pl.ds(0, shard)], r_1.at[g * 2 + b, pl.ds(0, shard)],
                      s1_s, s1_r.at[g * 2 + b], peer1)

    def copy_2(g):
        return remote(r_1.at[g * 2 + 1 - second, pl.ds(0, shard)], r_2.at[g, pl.ds(0, shard)],
                      s2_s, s2_r.at[g], peer2)

    def add_d(a, b, g):
        q = slot(a, b)
        i = g * 4 + q
        r_d[i, 0:shard, :] += gflat[pl.ds((g * 8 + q * 2 + core) * shard, shard), :]

    def d_to_1(g):
        four = gflat.at[pl.ds(0, 4 * shard)]
        pltpu.make_async_copy(four, four, sd_r.at[g]).wait()
        for b in (1 - second, second):
            add_d(1 - first, b, g)
            copy_1(g, b).start()
        for b in range(2):
            add_d(first, b, g)

    def one_to_2(g):
        for b in (1 - second, second):
            i = g * 2 + b
            remote(r_d.at[0, pl.ds(0, shard)], r_1.at[i, pl.ds(0, shard)], s1_s, s1_r.at[i], peer1).wait_recv()
            r_1[i, 0:shard, :] += r_d[g * 4 + slot(first, b), 0:shard, :]
            if b is not second:
                copy_2(g).start()

    def two_to_z(g):
        copy_2(g).wait_recv()
        r_2[g, 0:shard, :] += r_1[g * 2 + second, 0:shard, :]

        @pl.when(zz != g)
        def _():
            remote(r_2.at[g, pl.ds(0, shard)], r_z.at[zz, pl.ds(0, shard)], sz_s, sz_r.at[zz],
                   me + (g - zz) * 8).start()

    def after_out():
        scoped('spread_out', spread_out)
        scoped('barrier', pl.semaphore_wait, barrier, ndev - 1)
        send_d(3)

    def after_qkv():
        scoped('spread_qkv', spread, 0, 1, 0, cut)
        scoped('spread_proj', spread, ends[1], 1, cut, width)
        send_d(0)

    services = {CHUNKS - 1: after_out,
                CHUNKS: lambda: scoped('in_d1_3', d_to_1, 3),
                2 * CHUNKS - 1: after_qkv,
                2 * CHUNKS: lambda: scoped('in_d1_0', d_to_1, 0)}
    scoped('products', lax.fori_loop, 0, 3 * CHUNKS, products, 0)
    scoped('spread_inter', spread, ends[5], 2, 0, wide)
    scoped('send_d_1', send_d, 1)
    scoped('send_d_2', send_d, 2)
    scoped('one_to_2_3', one_to_2, 3)
    scoped('d_to_1_1', d_to_1, 1)
    scoped('d_to_1_2', d_to_1, 2)
    scoped('one_to_2_0', one_to_2, 0)
    scoped('two_to_z_3', two_to_z, 3)
    scoped('one_to_2_1', one_to_2, 1)
    scoped('two_to_z_0', two_to_z, 0)
    scoped('one_to_2_2', one_to_2, 2)
    scoped('two_to_z_1', two_to_z, 1)
    scoped('two_to_z_2', two_to_z, 2)

    for copy in small[1:]:
        scoped('wait_state', copy.wait)
    lane = lax.broadcasted_iota(jnp.int32, (shard, LANES), 1)
    row = lax.broadcasted_iota(jnp.int32, (shard, LANES), 0) + me * shard
    seg = jnp.zeros((shard, LANES), jnp.int32)
    for end in ends:
        seg = seg + jnp.where(row >= end, 1, 0)
    mine = lane == seg
    w = w_v[...]

    def seg_sums(val):
        per_row = jnp.sum(val, axis=1, keepdims=True)
        return jnp.sum(jnp.where(mine, per_row, 0.0), axis=0, keepdims=True)

    w_sums = seg_sums(w * w)

    g = r_2[zz, 0:shard, :]
    for d in range(1, PARTS):
        src = (zz + d) % PARTS
        scoped('wait_z', remote(r_2.at[0, pl.ds(0, shard)], r_z.at[src, pl.ds(0, shard)], sz_s, sz_r.at[src], me).wait_recv)
        g = g + r_z[src, 0:shard, :]
    g = g * (1.0 / ndev)

    def put(stat, value, s_sem, r_sem, lo, hi):
        stat[pl.ds(me, 1), :] = value

        def send(i, _):
            remote(stat.at[pl.ds(me, 1)], stat.at[pl.ds(me, 1)], s_sem, r_sem, (me + i) % ndev).start()
            return 0

        lax.fori_loop(lo, hi, send, 0)

    def rows_in(stat, count, sem):
        return pltpu.make_async_copy(stat.at[pl.ds(0, count)], stat.at[pl.ds(0, count)], sem)

    one_lane = lax.broadcasted_iota(jnp.int32, (1, LANES), 1)
    g_sq = jnp.sum(jnp.sum(g * g, axis=0, keepdims=True), axis=1, keepdims=True)
    put(stat1, jnp.where(one_lane == 64, g_sq, w_sums), t1_s, t1_r, 1, ndev)
    scoped('wait_stat1', rows_in(stat1, ndev - 1, t1_r).wait)
    total1 = jnp.sum(stat1[...], axis=0, keepdims=True)
    gn = jnp.sqrt(jnp.sum(jnp.where(one_lane == 64, total1, 0.0), axis=1, keepdims=True))
    h = g / jnp.maximum(1.0, gn)
    new_m = BETA_ONE * m_v[...] + (1.0 - BETA_ONE) * h
    new_v = BETA_TWO * v_v[...] + (1.0 - BETA_TWO) * h * h
    decay = jnp.where((seg == 0) | (seg == 2) | (seg == 6) | (seg == 8), DECAY, 0.0)
    u = (new_m / CORR_ONE) / (jnp.sqrt(new_v / CORR_TWO) + EPSILON) + decay * w
    plane = ndev // PARTS
    starts = [0] + ends[:-1]
    assert all((end - 1) // (plane * shard) - start // (plane * shard) <= 1 for start, end in zip(starts, ends))
    stat2[pl.ds(me, 1), :] = seg_sums(u * u)

    def send2(i, _, d):
        to = zz * plane + i

        @pl.when((to >= 0) & (to < ndev) & (to != me))
        def _():
            remote(stat2.at[pl.ds(me, 1)], stat2.at[pl.ds(me, 1)], t2_s.at[d + 1], t2_r.at[zz], to).start()

        return 0

    for d in (-1, 1, 0):
        lax.fori_loop(d * plane, (d + 1) * plane, functools.partial(send2, d=d), 0)

    def each_plane(fn):
        fn(1, zz, plane - 1)
        pl.when(zz > 0)(lambda: fn(0, zz - 1, plane))
        pl.when(zz < PARTS - 1)(lambda: fn(2, zz + 1, plane))

    scoped('wait_stat2', each_plane, lambda d, src, count: rows_in(stat2, count, t2_r.at[src]).wait())
    total2 = jnp.sum(stat2[...], axis=0, keepdims=True)
    nm_out[...] = new_m
    nv_out[...] = new_v
    w_norm, u_norm = jnp.sqrt(total1), jnp.sqrt(total2)
    ratio = jnp.where((w_norm > 0) & (u_norm > 0), w_norm / jnp.where(u_norm > 0, u_norm, 1.0), 1.0)
    per_row = jnp.sum(jnp.where(mine, ratio, 0.0), axis=1, keepdims=True)
    new_w = w - LEARN_RATE * per_row * u
    nw_out[...] = new_w
    wfull[pl.ds(me * shard, shard), :] = new_w
    split = (shard + 1) // 2
    parts = ((0, split), (split, shard - split))

    def part_at(s, h):
        return wfull.at[pl.ds(s * shard + parts[h][0], parts[h][1])]

    sent = []

    def push(s, h, *devs):
        for dev in devs:
            sem = agp_r if dev is partner else ag_r.at[s // 2, h]
            remote(part_at(s, h), part_at(s, h), ag_s, sem, dev).start()
            sent.append(parts[h][1])

    def arrived(s, h):
        remote(part_at(s, h), part_at(s, h), ag_s, ag_r.at[s // 2, h], me).wait_recv()

    zs = [zz, zz + 1 - 2 * (zz % 2), 3 - zz, zz + 2 - 4 * (zz // 2)]
    diag = peer1 + peer2 - me

    def shifted(s, j):
        return s + (zs[j] - zz) * 8

    for h in range(2):
        push(me, h, shifted(me, 1), peer2, peer1)
    for h in range(2):
        push(me, h, shifted(me, 2), partner)
    for h in range(2):
        push(me, h, shifted(me, 3))
    for kind, j in (('a', 0), ('z', 1), ('z', 2), ('a', 1), ('z', 3), ('a', 2), ('a', 3), ('b', 0), ('d', 0), ('b', 1),
                    ('d', 1), ('b', 2), ('d', 2), ('b', 3), ('d', 3)):
        s = shifted({'a': peer1, 'z': me, 'b': peer2, 'd': diag}[kind], j)
        for h in range(2):
            scoped('got_%s%d' % (kind, j), arrived, s, h)
            push(s, h, *{'a': (peer2, partner), 'z': (peer2, peer1, partner)}.get(kind, (partner,)))

    theirs = wfull.at[pl.ds(0, ndev // 2 * shard)]
    scoped('got_rest', pltpu.make_async_copy(theirs, theirs, agp_r).wait)
    par_out[...] = wfull[...].astype(BF16)

    def all_sent(buf, count, sem):
        pltpu.make_async_copy(buf.at[pl.ds(0, count)], buf.at[pl.ds(0, count)], sem).wait()

    scoped('all_sent_gflat', all_sent, gflat, 16 * shard, sd_s)
    scoped('all_sent_gflat', all_sent, gflat, 8 * shard, s1_s)
    scoped('all_sent_gflat', all_sent, gflat, 4 * shard, s2_s)
    scoped('all_sent_gflat', all_sent, gflat, 3 * shard, sz_s)
    scoped('all_sent_stat1', all_sent, stat1, ndev - 1, t1_s)
    each_plane(lambda d, src, count: rows_in(stat2, count, t2_s.at[d]).wait())
    scoped('all_sent_wfull', all_sent, wfull, sum(sent), ag_s)


def write_kernel(*refs):
    sem = refs[-1]
    half = len(refs) // 2
    copies = [pltpu.make_async_copy(src, dst, sem.at[i]) for i, (src, dst) in enumerate(zip(refs[:half], refs[half:-1]))]
    for copy in reversed(copies):
        copy.start()
    for copy in copies:
        copy.wait()


def solution(mesh):
    ndev = mesh.shape['dp']

    def local_step(weights, moment_one, moment_two, x_qkv, dy_qkv, x_proj, dy_proj, x_inter, dy_inter, x_out, dy_out, ln_grad):
        tokens, width = x_qkv.shape
        shard = weights.shape[0] // LANES
        rows = shard * ndev
        flat = lambda a: a.reshape(-1, LANES)
        acts = (x_qkv, dy_qkv, x_proj, dy_proj, x_inter, dy_inter, x_out, dy_out)
        vm = pltpu.VMEM
        pad = -(-shard // 8) * 8
        state = jax.ShapeDtypeStruct((shard, LANES), F32)
        mid = (vm((shard, LANES), F32),) * 3 + (vm((rows, LANES), BF16),)
        dma = pltpu.SemaphoreType.DMA
        hbm = pl.BlockSpec(memory_space=pltpu.HBM)
        whole = pl.BlockSpec(memory_space=pltpu.VMEM)
        out_shape = (state, state, state, jax.ShapeDtypeStruct((rows, LANES), BF16))
        outs = pl.pallas_call(
            functools.partial(comm_kernel, (width, shard, ndev, rows)),
            out_shape=mid,
            in_specs=[hbm] * 12,
            out_specs=(whole,) * 4,
            scratch_shapes=[
                vm((4, tokens, width), BF16), vm((3, tokens, 4 * width), BF16), vm((4, width), F32)] + [
                vm((shard, LANES), F32)] * 3 + [
                vm((3, width + 16, 4 * width), F32), vm((16, width), F32), vm((rows, LANES), F32),
                vm((16, pad, LANES), F32), vm((8, pad, LANES), F32), vm((4, pad, LANES), F32), vm((4, pad, LANES), F32),
                vm((ndev, LANES), F32), vm((ndev, LANES), F32), vm((rows, LANES), F32),
                dma((3 * CHUNKS,)), dma((CHUNKS,)), dma((4,)), dma, dma((4,)), dma, dma((8,)), dma, dma((4,)), dma, dma((4,)),
                dma, dma, dma((3,)), dma((PARTS,)), dma, dma((ndev // 2, 2)), dma],
            compiler_params=pltpu.CompilerParams(collective_id=0, has_side_effects=True, vmem_limit_bytes=61 * 2 ** 20),
            name='lamb_step',
        )(*acts, ln_grad.reshape(4, width), flat(weights), flat(moment_one), flat(moment_two))
        new_w, new_m, new_v, params = pl.pallas_call(
            write_kernel, out_shape=out_shape, in_specs=[whole] * 4, out_specs=(hbm,) * 4,
            scratch_shapes=[dma((4,))], name='write_out')(*[pltpu.with_memory_space_constraint(a, pltpu.VMEM) for a in outs])
        return new_w.reshape(-1), new_m.reshape(-1), new_v.reshape(-1), params.reshape(-1)

    row_spec = P('dp', None)
    in_specs = (P('dp'), P('dp'), P('dp'), row_spec, row_spec, row_spec, row_spec, row_spec, row_spec, row_spec, row_spec, P('dp', None, None))
    out_specs = (P('dp'), P('dp'), P('dp'), P())
    return jax.shard_map(local_step, mesh=mesh, in_specs=in_specs, out_specs=out_specs, check_vma=False)
```

```python
import functools

import jax
import jax.numpy as jnp
from jax import lax
from jax.experimental import pallas as pl
from jax.experimental.pallas import tpu as pltpu
from jax.sharding import PartitionSpec as P

STEP = 10
LEARN_RATE = 0.5
BETA_ONE = 0.9
BETA_TWO = 0.999
EPSILON = 1e-6
DECAY = 0.01
CORR_ONE = 1.0 - BETA_ONE ** STEP
CORR_TWO = 1.0 - BETA_TWO ** STEP

LANES = 128
CHUNKS = 2
PARTS = 4
F32 = jnp.float32
BF16 = jnp.bfloat16


def tensor_sizes(width):
    return [3 * width * width, 3 * width, width * width, width, width, width,
            4 * width * width, 4 * width, 4 * width * width, width, width, width]


def row_ends(width):
    ends, total = [], 0
    for size in tensor_sizes(width):
        total += size // LANES
        ends.append(total)
    return ends


def scoped(name, fn, *args):
    with jax.named_scope(name):
        return fn(*args)


def comm_kernel(dims, x_qkv, dy_qkv, x_proj, dy_proj, x_inter, dy_inter, x_out, dy_out, ln, w_in, m_in, v_in,
                nw_out, nm_out, nv_out, par_out,
                xb, yb, ln_v, w_v, m_v, v_v, acc, bias_out, gflat, r_d, r_1, r_2, r_z, stat1, stat2, wfull,
                in_sem, in2_sem, st_sem, sd_s, sd_r, s1_s, s1_r, s2_s, s2_r, sz_s, sz_r,
                t1_s, t1_r, t2_s, t2_r, ag_s, ag_r, agp_r, agz_s):
    width, shard, ndev, rows = dims
    tokens = x_qkv.shape[0]
    step = tokens // CHUNKS
    ends = row_ends(width)
    me = lax.axis_index('dp')
    core, xx, yy, zz = me % 2, (me // 2) % 2, (me // 4) % 2, me // 8
    partner = me + 1 - 2 * core
    first = xx * (1 - core) + yy * core
    second = yy * (1 - core) + xx * core
    peer1 = me + (1 - 2 * first) * (2 * (1 - core) + 4 * core)
    peer2 = me + (1 - 2 * second) * (4 * (1 - core) + 2 * core)

    def slot(a, b):
        return (1 - core) * (2 * b + a) + core * (2 * a + b)

    small = [pltpu.make_async_copy(s, d, st_sem.at[i])
             for i, (s, d) in enumerate(((ln, ln_v), (w_in, w_v), (m_in, m_v), (v_in, v_v)))]
    for copy in small:
        copy.start()
    wide = 4 * width
    cut = 3 * width
    groups = (((dy_out, xb, 0, 0), (x_out, yb, 0, 0)),
              ((x_qkv, xb, 1, 0), (x_proj, xb, 2, 0), (dy_qkv, yb, 1, 0), (dy_proj, yb, 1, cut)),
              ((x_inter, xb, 3, 0), (dy_inter, yb, 2, 0)))
    for m, group in enumerate(groups):
        def start(k, _, m=m, group=group):
            at = pl.ds(pl.multiple_of(k * step, step), step)
            for src, dst, slab, col in group:
                to = dst.at[slab, at] if src.shape[1] == dst.shape[2] else dst.at[slab, at, pl.ds(col, src.shape[1])]
                sem = in2_sem.at[k] if slab == 2 and dst is xb else in_sem.at[m * CHUNKS + k]
                pltpu.make_async_copy(src.at[at], to, sem).start()
            return 0

        lax.fori_loop(0, CHUNKS, start, 0)

    barrier = pltpu.get_barrier_semaphore()
    stat2[...] = jnp.zeros(stat2.shape, F32)

    def hello(i, _):
        pl.semaphore_signal(barrier, inc=1, device_id=((me + i) % ndev,), device_id_type=pl.DeviceIdType.MESH)
        return 0

    lax.fori_loop(1, ndev, hello, 0)

    def remote(src, dst, s_sem, r_sem, dev):
        return pltpu.make_async_remote_copy(src_ref=src, dst_ref=dst, send_sem=s_sem, recv_sem=r_sem,
                                            device_id=(dev,), device_id_type=pl.DeviceIdType.MESH)

    ones = jnp.ones((16, step), BF16)
    acc[...] = jnp.zeros(acc.shape, F32)
    bias_out[...] = jnp.zeros(bias_out.shape, F32)

    def products(i, _):
        m, k = i // CHUNKS, i % CHUNKS
        both = yb.at[0, pl.ds(0, step * 5 // 4)]
        pltpu.make_async_copy(both, both, in_sem.at[i]).wait()

        @pl.when(m == 1)
        def _():
            half = xb.at[2, pl.ds(0, step)]
            pltpu.make_async_copy(half, half, in2_sem.at[k]).wait()

        at = pl.ds(pl.multiple_of(k * step, step), step)
        lhs1 = jnp.concatenate([xb[m + m // 2, at, :].T, ones], axis=0)
        acc[m, :, 0:cut] += jnp.dot(lhs1, yb[m, at, 0:cut], preferred_element_type=F32)
        lhs2 = jnp.concatenate([xb[2 * m - m // 2, at, :].T, ones], axis=0)
        acc[m, :, cut:wide] += jnp.dot(lhs2, yb[m, at, cut:wide], preferred_element_type=F32)

        @pl.when(m == 0)
        def _():
            bias_out[...] += jnp.dot(ones, xb[0, at, :], preferred_element_type=F32)

        for at_i, fn in services.items():
            pl.when(i == at_i)(fn)
        return 0

    def spread(base, m, lo, n):
        cols = n // LANES
        for j in range(cols):
            at = slice(lo + j * LANES, lo + (j + 1) * LANES)
            gflat[pl.ds(base + j, width, stride=cols), :] = acc[m, 0:width, at]
            gflat[pl.ds(base + cols * width + j, 1), :] = acc[m, width:width + 1, at]

    def spread_out():
        cols = width // LANES
        for j in range(cols):
            at = slice(j * LANES, (j + 1) * LANES)
            gflat[pl.ds(ends[7] + j, wide, stride=cols), :] = acc[0, at, :].T
            gflat[pl.ds(ends[8] + j, 1), :] = bias_out[0:1, at]
        small[0].wait()
        for r, start in enumerate((ends[3], ends[4], ends[9], ends[10])):
            for j in range(cols):
                gflat[pl.ds(start + j, 1), :] = ln_v[r:r + 1, j * LANES:(j + 1) * LANES]
        gflat[pl.ds(ends[11], rows - ends[11]), :] = jnp.zeros((rows - ends[11], LANES), F32)

    def send_d(g):
        for q in range(4):
            s = g * 8 + q * 2 + 1 - core
            remote(gflat.at[pl.ds(s * shard, shard)], r_d.at[g * 4 + q, pl.ds(0, shard)],
                   sd_s, sd_r.at[g], partner).start()

    def copy_1(g, b):
        return remote(r_d.at[g * 4 + slot(1 - first, b), pl.ds(0, shard)], r_1.at[g * 2 + b, pl.ds(0, shard)],
                      s1_s, s1_r.at[g * 2 + b], peer1)

    def copy_2(g):
        return remote(r_1.at[g * 2 + 1 - second, pl.ds(0, shard)], r_2.at[g, pl.ds(0, shard)],
                      s2_s, s2_r.at[g], peer2)

    def add_d(a, b, g):
        q = slot(a, b)
        i = g * 4 + q
        r_d[i, 0:shard, :] += gflat[pl.ds((g * 8 + q * 2 + core) * shard, shard), :]

    def d_to_1(g):
        four = gflat.at[pl.ds(0, 4 * shard)]
        pltpu.make_async_copy(four, four, sd_r.at[g]).wait()
        for b in (1 - second, second):
            add_d(1 - first, b, g)
            copy_1(g, b).start()
        for b in range(2):
            add_d(first, b, g)

    def one_to_2(g):
        for b in (1 - second, second):
            i = g * 2 + b
            remote(r_d.at[0, pl.ds(0, shard)], r_1.at[i, pl.ds(0, shard)], s1_s, s1_r.at[i], peer1).wait_recv()
            r_1[i, 0:shard, :] += r_d[g * 4 + slot(first, b), 0:shard, :]
            if b is not second:
                copy_2(g).start()

    def two_to_z(g):
        copy_2(g).wait_recv()
        r_2[g, 0:shard, :] += r_1[g * 2 + second, 0:shard, :]

        @pl.when(zz != g)
        def _():
            remote(r_2.at[g, pl.ds(0, shard)], r_z.at[zz, pl.ds(0, shard)], sz_s, sz_r.at[zz],
                   me + (g - zz) * 8).start()

    def after_out():
        scoped('spread_out', spread_out)
        scoped('barrier', pl.semaphore_wait, barrier, ndev - 1)
        send_d(3)

    def after_qkv():
        scoped('spread_qkv', spread, 0, 1, 0, cut)
        scoped('spread_proj', spread, ends[1], 1, cut, width)
        send_d(0)

    services = {CHUNKS - 1: after_out,
                CHUNKS: lambda: scoped('in_d1_3', d_to_1, 3),
                2 * CHUNKS - 1: after_qkv,
                2 * CHUNKS: lambda: scoped('in_d1_0', d_to_1, 0)}
    scoped('products', lax.fori_loop, 0, 3 * CHUNKS, products, 0)
    scoped('spread_inter', spread, ends[5], 2, 0, wide)
    scoped('send_d_1', send_d, 1)
    scoped('send_d_2', send_d, 2)
    scoped('one_to_2_3', one_to_2, 3)
    scoped('d_to_1_1', d_to_1, 1)
    scoped('d_to_1_2', d_to_1, 2)
    scoped('one_to_2_0', one_to_2, 0)
    scoped('two_to_z_3', two_to_z, 3)
    scoped('one_to_2_1', one_to_2, 1)
    scoped('two_to_z_0', two_to_z, 0)
    scoped('one_to_2_2', one_to_2, 2)
    scoped('two_to_z_1', two_to_z, 1)
    scoped('two_to_z_2', two_to_z, 2)

    for copy in small[1:]:
        scoped('wait_state', copy.wait)
    lane = lax.broadcasted_iota(jnp.int32, (shard, LANES), 1)
    row = lax.broadcasted_iota(jnp.int32, (shard, LANES), 0) + me * shard
    seg = jnp.zeros((shard, LANES), jnp.int32)
    for end in ends:
        seg = seg + jnp.where(row >= end, 1, 0)
    mine = lane == seg
    w = w_v[...]

    def seg_sums(val):
        per_row = jnp.sum(val, axis=1, keepdims=True)
        return jnp.sum(jnp.where(mine, per_row, 0.0), axis=0, keepdims=True)

    w_sums = seg_sums(w * w)

    g = r_2[zz, 0:shard, :]
    for d in range(1, PARTS):
        src = (zz + d) % PARTS
        scoped('wait_z', remote(r_2.at[0, pl.ds(0, shard)], r_z.at[src, pl.ds(0, shard)], sz_s, sz_r.at[src], me).wait_recv)
        g = g + r_z[src, 0:shard, :]
    g = g * (1.0 / ndev)

    def put(stat, value, s_sem, r_sem, lo, hi):
        stat[pl.ds(me, 1), :] = value

        def send(i, _):
            remote(stat.at[pl.ds(me, 1)], stat.at[pl.ds(me, 1)], s_sem, r_sem, (me + i) % ndev).start()
            return 0

        lax.fori_loop(lo, hi, send, 0)

    def rows_in(stat, count, sem):
        return pltpu.make_async_copy(stat.at[pl.ds(0, count)], stat.at[pl.ds(0, count)], sem)

    one_lane = lax.broadcasted_iota(jnp.int32, (1, LANES), 1)
    g_sq = jnp.sum(jnp.sum(g * g, axis=0, keepdims=True), axis=1, keepdims=True)
    put(stat1, jnp.where(one_lane == 64, g_sq, w_sums), t1_s, t1_r, 1, ndev)
    scoped('wait_stat1', rows_in(stat1, ndev - 1, t1_r).wait)
    total1 = jnp.sum(stat1[...], axis=0, keepdims=True)
    gn = jnp.sqrt(jnp.sum(jnp.where(one_lane == 64, total1, 0.0), axis=1, keepdims=True))
    h = g / jnp.maximum(1.0, gn)
    new_m = BETA_ONE * m_v[...] + (1.0 - BETA_ONE) * h
    new_v = BETA_TWO * v_v[...] + (1.0 - BETA_TWO) * h * h
    decay = jnp.where((seg == 0) | (seg == 2) | (seg == 6) | (seg == 8), DECAY, 0.0)
    u = (new_m / CORR_ONE) / (jnp.sqrt(new_v / CORR_TWO) + EPSILON) + decay * w
    plane = ndev // PARTS
    starts = [0] + ends[:-1]
    assert all((end - 1) // (plane * shard) - start // (plane * shard) <= 1 for start, end in zip(starts, ends))
    stat2[pl.ds(me, 1), :] = seg_sums(u * u)

    def send2(i, _, d):
        to = zz * plane + i

        @pl.when((to >= 0) & (to < ndev) & (to != me))
        def _():
            remote(stat2.at[pl.ds(me, 1)], stat2.at[pl.ds(me, 1)], t2_s.at[d + 1], t2_r.at[zz], to).start()

        return 0

    for d in (-1, 1, 0):
        lax.fori_loop(d * plane, (d + 1) * plane, functools.partial(send2, d=d), 0)

    def each_plane(fn):
        fn(1, zz, plane - 1)
        pl.when(zz > 0)(lambda: fn(0, zz - 1, plane))
        pl.when(zz < PARTS - 1)(lambda: fn(2, zz + 1, plane))

    scoped('wait_stat2', each_plane, lambda d, src, count: rows_in(stat2, count, t2_r.at[src]).wait())
    total2 = jnp.sum(stat2[...], axis=0, keepdims=True)
    nm_out[...] = new_m
    nv_out[...] = new_v
    w_norm, u_norm = jnp.sqrt(total1), jnp.sqrt(total2)
    ratio = jnp.where((w_norm > 0) & (u_norm > 0), w_norm / jnp.where(u_norm > 0, u_norm, 1.0), 1.0)
    per_row = jnp.sum(jnp.where(mine, ratio, 0.0), axis=1, keepdims=True)
    new_w = w - LEARN_RATE * per_row * u
    nw_out[...] = new_w
    wfull[pl.ds(me * shard, shard), :] = new_w
    split = (shard + 1) // 2
    parts = ((0, split), (split, shard - split))

    def part_at(s, h):
        return wfull.at[pl.ds(s * shard + parts[h][0], parts[h][1])]

    sent = []

    def push(s, h, *devs):
        for dev in devs:
            sem = agp_r if dev is partner else ag_r.at[s // 2, h]
            remote(part_at(s, h), part_at(s, h), ag_s, sem, dev).start()
            sent.append(parts[h][1])

    def arrived(s, h):
        remote(part_at(s, h), part_at(s, h), ag_s, ag_r.at[s // 2, h], me).wait_recv()

    zs = [zz, zz + 1 - 2 * (zz % 2), 2 - zz // 2, 3 - 3 * (zz // 2)]
    inner = (zz == 1) | (zz == 2)
    diag = peer1 + peer2 - me

    def shifted(s, j):
        return s + (zs[j] - zz) * 8

    for h in range(2):
        push(me, h, shifted(me, 1), peer2, peer1)
    for h in range(2):
        push(me, h, shifted(me, 2), partner)
    for kind, j in (('a', 0), ('z', 1), ('z', 2), ('a', 1), ('z', 3), ('a', 2), ('a', 3), ('b', 0), ('d', 0), ('b', 1),
                    ('d', 1), ('b', 2), ('d', 2), ('b', 3), ('d', 3)):
        s = shifted({'a': peer1, 'z': me, 'b': peer2, 'd': diag}[kind], j)
        for h in range(2):
            scoped('got_%s%d' % (kind, j), arrived, s, h)
            if kind == 'z' and j > 1:
                @pl.when(inner)
                def _():
                    remote(part_at(s, h), part_at(s, h), agz_s, ag_r.at[s // 2, h], shifted(me, 1)).start()

            push(s, h, *{'a': (peer2, partner), 'z': (peer2, peer1, partner)}.get(kind, (partner,)))

    theirs = wfull.at[pl.ds(0, ndev // 2 * shard)]
    scoped('got_rest', pltpu.make_async_copy(theirs, theirs, agp_r).wait)
    par_out[...] = wfull[...].astype(BF16)

    def all_sent(buf, count, sem):
        pltpu.make_async_copy(buf.at[pl.ds(0, count)], buf.at[pl.ds(0, count)], sem).wait()

    scoped('all_sent_gflat', all_sent, gflat, 16 * shard, sd_s)
    scoped('all_sent_gflat', all_sent, gflat, 8 * shard, s1_s)
    scoped('all_sent_gflat', all_sent, gflat, 4 * shard, s2_s)
    scoped('all_sent_gflat', all_sent, gflat, 3 * shard, sz_s)
    scoped('all_sent_stat1', all_sent, stat1, ndev - 1, t1_s)
    each_plane(lambda d, src, count: rows_in(stat2, count, t2_s.at[d]).wait())
    scoped('all_sent_wfull', all_sent, wfull, sum(sent), ag_s)
    pl.when(inner)(lambda: all_sent(wfull, 2 * shard, agz_s))


def write_kernel(*refs):
    sem = refs[-1]
    half = len(refs) // 2
    copies = [pltpu.make_async_copy(src, dst, sem.at[i]) for i, (src, dst) in enumerate(zip(refs[:half], refs[half:-1]))]
    for copy in reversed(copies):
        copy.start()
    for copy in copies:
        copy.wait()


def solution(mesh):
    ndev = mesh.shape['dp']

    def local_step(weights, moment_one, moment_two, x_qkv, dy_qkv, x_proj, dy_proj, x_inter, dy_inter, x_out, dy_out, ln_grad):
        tokens, width = x_qkv.shape
        shard = weights.shape[0] // LANES
        rows = shard * ndev
        flat = lambda a: a.reshape(-1, LANES)
        acts = (x_qkv, dy_qkv, x_proj, dy_proj, x_inter, dy_inter, x_out, dy_out)
        vm = pltpu.VMEM
        pad = -(-shard // 8) * 8
        state = jax.ShapeDtypeStruct((shard, LANES), F32)
        mid = (vm((shard, LANES), F32),) * 3 + (vm((rows, LANES), BF16),)
        dma = pltpu.SemaphoreType.DMA
        hbm = pl.BlockSpec(memory_space=pltpu.HBM)
        whole = pl.BlockSpec(memory_space=pltpu.VMEM)
        out_shape = (state, state, state, jax.ShapeDtypeStruct((rows, LANES), BF16))
        outs = pl.pallas_call(
            functools.partial(comm_kernel, (width, shard, ndev, rows)),
            out_shape=mid,
            in_specs=[hbm] * 12,
            out_specs=(whole,) * 4,
            scratch_shapes=[
                vm((4, tokens, width), BF16), vm((3, tokens, 4 * width), BF16), vm((4, width), F32)] + [
                vm((shard, LANES), F32)] * 3 + [
                vm((3, width + 16, 4 * width), F32), vm((16, width), F32), vm((rows, LANES), F32),
                vm((16, pad, LANES), F32), vm((8, pad, LANES), F32), vm((4, pad, LANES), F32), vm((4, pad, LANES), F32),
                vm((ndev, LANES), F32), vm((ndev, LANES), F32), vm((rows, LANES), F32),
                dma((3 * CHUNKS,)), dma((CHUNKS,)), dma((4,)), dma, dma((4,)), dma, dma((8,)), dma, dma((4,)), dma, dma((4,)),
                dma, dma, dma((3,)), dma((PARTS,)), dma, dma((ndev // 2, 2)), dma, dma],
            compiler_params=pltpu.CompilerParams(collective_id=0, has_side_effects=True, vmem_limit_bytes=61 * 2 ** 20),
            name='lamb_step',
        )(*acts, ln_grad.reshape(4, width), flat(weights), flat(moment_one), flat(moment_two))
        new_w, new_m, new_v, params = pl.pallas_call(
            write_kernel, out_shape=out_shape, in_specs=[whole] * 4, out_specs=(hbm,) * 4,
            scratch_shapes=[dma((4,))], name='write_out')(*[pltpu.with_memory_space_constraint(a, pltpu.VMEM) for a in outs])
        return new_w.reshape(-1), new_m.reshape(-1), new_v.reshape(-1), params.reshape(-1)

    row_spec = P('dp', None)
    in_specs = (P('dp'), P('dp'), P('dp'), row_spec, row_spec, row_spec, row_spec, row_spec, row_spec, row_spec, row_spec, P('dp', None, None))
    out_specs = (P('dp'), P('dp'), P('dp'), P())
    return jax.shard_map(local_step, mesh=mesh, in_specs=in_specs, out_specs=out_specs, check_vma=False)
```

```python
import functools

import jax
import jax.numpy as jnp
from jax import lax
from jax.experimental import pallas as pl
from jax.experimental.pallas import tpu as pltpu
from jax.sharding import PartitionSpec as P

STEP = 10
LEARN_RATE = 0.5
BETA_ONE = 0.9
BETA_TWO = 0.999
EPSILON = 1e-6
DECAY = 0.01
CORR_ONE = 1.0 - BETA_ONE ** STEP
CORR_TWO = 1.0 - BETA_TWO ** STEP

LANES = 128
CHUNKS = 2
PARTS = 4
F32 = jnp.float32
BF16 = jnp.bfloat16


def tensor_sizes(width):
    return [3 * width * width, 3 * width, width * width, width, width, width,
            4 * width * width, 4 * width, 4 * width * width, width, width, width]


def row_ends(width):
    ends, total = [], 0
    for size in tensor_sizes(width):
        total += size // LANES
        ends.append(total)
    return ends


def scoped(name, fn, *args):
    with jax.named_scope(name):
        return fn(*args)


def comm_kernel(dims, x_qkv, dy_qkv, x_proj, dy_proj, x_inter, dy_inter, x_out, dy_out, ln, w_in, m_in, v_in,
                nw_out, nm_out, nv_out, par_out,
                xb, yb, ln_v, w_v, m_v, v_v, acc, bias_out, gflat, r_d, r_1, r_2, r_z, stat1, stat2, wfull,
                in_sem, in2_sem, st_sem, sd_s, sd_r, s1_s, s1_r, s2_s, s2_r, sz_s, sz_r,
                t1_s, t1_r, t2_s, t2_r, ag_s, ag_r, agp_r, agz_s):
    width, shard, ndev, rows = dims
    tokens = x_qkv.shape[0]
    step = tokens // CHUNKS
    ends = row_ends(width)
    me = lax.axis_index('dp')
    core, xx, yy, zz = me % 2, (me // 2) % 2, (me // 4) % 2, me // 8
    partner = me + 1 - 2 * core
    first = xx * (1 - core) + yy * core
    second = yy * (1 - core) + xx * core
    peer1 = me + (1 - 2 * first) * (2 * (1 - core) + 4 * core)
    peer2 = me + (1 - 2 * second) * (4 * (1 - core) + 2 * core)

    def slot(a, b):
        return (1 - core) * (2 * b + a) + core * (2 * a + b)

    small = [pltpu.make_async_copy(s, d, st_sem.at[i])
             for i, (s, d) in enumerate(((ln, ln_v), (w_in, w_v), (m_in, m_v), (v_in, v_v)))]
    for copy in small:
        copy.start()
    wide = 4 * width
    cut = 3 * width
    groups = (((dy_out, xb, 0, 0), (x_out, yb, 0, 0)),
              ((x_qkv, xb, 1, 0), (x_proj, xb, 2, 0), (dy_qkv, yb, 1, 0), (dy_proj, yb, 1, cut)),
              ((x_inter, xb, 3, 0), (dy_inter, yb, 2, 0)))
    for m, group in enumerate(groups):
        def start(k, _, m=m, group=group):
            at = pl.ds(pl.multiple_of(k * step, step), step)
            for src, dst, slab, col in group:
                to = dst.at[slab, at] if src.shape[1] == dst.shape[2] else dst.at[slab, at, pl.ds(col, src.shape[1])]
                sem = in2_sem.at[k] if slab == 2 and dst is xb else in_sem.at[m * CHUNKS + k]
                pltpu.make_async_copy(src.at[at], to, sem).start()
            return 0

        lax.fori_loop(0, CHUNKS, start, 0)

    barrier = pltpu.get_barrier_semaphore()
    stat2[...] = jnp.zeros(stat2.shape, F32)

    def hello(i, _):
        pl.semaphore_signal(barrier, inc=1, device_id=((me + i) % ndev,), device_id_type=pl.DeviceIdType.MESH)
        return 0

    lax.fori_loop(1, ndev, hello, 0)

    def remote(src, dst, s_sem, r_sem, dev):
        return pltpu.make_async_remote_copy(src_ref=src, dst_ref=dst, send_sem=s_sem, recv_sem=r_sem,
                                            device_id=(dev,), device_id_type=pl.DeviceIdType.MESH)

    ones = jnp.ones((16, step), BF16)
    acc[...] = jnp.zeros(acc.shape, F32)
    bias_out[...] = jnp.zeros(bias_out.shape, F32)

    def products(i, _):
        m, k = i // CHUNKS, i % CHUNKS
        both = yb.at[0, pl.ds(0, step * 5 // 4)]
        pltpu.make_async_copy(both, both, in_sem.at[i]).wait()

        @pl.when(m == 1)
        def _():
            half = xb.at[2, pl.ds(0, step)]
            pltpu.make_async_copy(half, half, in2_sem.at[k]).wait()

        at = pl.ds(pl.multiple_of(k * step, step), step)
        lhs1 = jnp.concatenate([xb[m + m // 2, at, :].T, ones], axis=0)
        acc[m, :, 0:cut] += jnp.dot(lhs1, yb[m, at, 0:cut], preferred_element_type=F32)
        lhs2 = jnp.concatenate([xb[2 * m - m // 2, at, :].T, ones], axis=0)
        acc[m, :, cut:wide] += jnp.dot(lhs2, yb[m, at, cut:wide], preferred_element_type=F32)

        @pl.when(m == 0)
        def _():
            bias_out[...] += jnp.dot(ones, xb[0, at, :], preferred_element_type=F32)

        for at_i, fn in services.items():
            pl.when(i == at_i)(fn)
        return 0

    def spread(base, m, lo, n):
        cols = n // LANES
        for j in range(cols):
            at = slice(lo + j * LANES, lo + (j + 1) * LANES)
            gflat[pl.ds(base + j, width, stride=cols), :] = acc[m, 0:width, at]
            gflat[pl.ds(base + cols * width + j, 1), :] = acc[m, width:width + 1, at]

    def spread_out():
        cols = width // LANES
        for j in range(cols):
            at = slice(j * LANES, (j + 1) * LANES)
            gflat[pl.ds(ends[7] + j, wide, stride=cols), :] = acc[0, at, :].T
            gflat[pl.ds(ends[8] + j, 1), :] = bias_out[0:1, at]
        small[0].wait()
        for r, start in enumerate((ends[3], ends[4], ends[9], ends[10])):
            for j in range(cols):
                gflat[pl.ds(start + j, 1), :] = ln_v[r:r + 1, j * LANES:(j + 1) * LANES]
        gflat[pl.ds(ends[11], rows - ends[11]), :] = jnp.zeros((rows - ends[11], LANES), F32)

    def send_d(g):
        for q in range(4):
            s = g * 8 + q * 2 + 1 - core
            remote(gflat.at[pl.ds(s * shard, shard)], r_d.at[g * 4 + q, pl.ds(0, shard)],
                   sd_s, sd_r.at[g], partner).start()

    def copy_1(g, b):
        return remote(r_d.at[g * 4 + slot(1 - first, b), pl.ds(0, shard)], r_1.at[g * 2 + b, pl.ds(0, shard)],
                      s1_s, s1_r.at[g * 2 + b], peer1)

    def copy_2(g):
        return remote(r_1.at[g * 2 + 1 - second, pl.ds(0, shard)], r_2.at[g, pl.ds(0, shard)],
                      s2_s, s2_r.at[g], peer2)

    def add_d(a, b, g):
        q = slot(a, b)
        i = g * 4 + q
        r_d[i, 0:shard, :] += gflat[pl.ds((g * 8 + q * 2 + core) * shard, shard), :]

    def d_to_1(g):
        four = gflat.at[pl.ds(0, 4 * shard)]
        pltpu.make_async_copy(four, four, sd_r.at[g]).wait()
        for b in (1 - second, second):
            add_d(1 - first, b, g)
            copy_1(g, b).start()
        for b in range(2):
            add_d(first, b, g)

    def one_to_2(g):
        for b in (1 - second, second):
            i = g * 2 + b
            remote(r_d.at[0, pl.ds(0, shard)], r_1.at[i, pl.ds(0, shard)], s1_s, s1_r.at[i], peer1).wait_recv()
            r_1[i, 0:shard, :] += r_d[g * 4 + slot(first, b), 0:shard, :]
            if b is not second:
                copy_2(g).start()

    def two_to_z(g):
        copy_2(g).wait_recv()
        r_2[g, 0:shard, :] += r_1[g * 2 + second, 0:shard, :]

        @pl.when(zz != g)
        def _():
            remote(r_2.at[g, pl.ds(0, shard)], r_z.at[zz, pl.ds(0, shard)], sz_s, sz_r.at[zz],
                   me + (g - zz) * 8).start()

    def after_out():
        scoped('spread_out', spread_out)
        scoped('barrier', pl.semaphore_wait, barrier, ndev - 1)
        send_d(3)

    def after_qkv():
        scoped('spread_qkv', spread, 0, 1, 0, cut)
        scoped('spread_proj', spread, ends[1], 1, cut, width)
        send_d(0)

    services = {CHUNKS - 1: after_out,
                CHUNKS: lambda: scoped('in_d1_3', d_to_1, 3),
                2 * CHUNKS - 1: after_qkv,
                2 * CHUNKS: lambda: scoped('in_d1_0', d_to_1, 0)}
    scoped('products', lax.fori_loop, 0, 3 * CHUNKS, products, 0)
    scoped('spread_inter', spread, ends[5], 2, 0, wide)
    scoped('send_d_1', send_d, 1)
    scoped('send_d_2', send_d, 2)
    scoped('one_to_2_3', one_to_2, 3)
    scoped('d_to_1_1', d_to_1, 1)
    scoped('d_to_1_2', d_to_1, 2)
    scoped('one_to_2_0', one_to_2, 0)
    scoped('two_to_z_3', two_to_z, 3)
    scoped('one_to_2_1', one_to_2, 1)
    scoped('two_to_z_0', two_to_z, 0)
    scoped('one_to_2_2', one_to_2, 2)
    scoped('two_to_z_1', two_to_z, 1)
    scoped('two_to_z_2', two_to_z, 2)

    for copy in small[1:]:
        scoped('wait_state', copy.wait)
    lane = lax.broadcasted_iota(jnp.int32, (shard, LANES), 1)
    row = lax.broadcasted_iota(jnp.int32, (shard, LANES), 0) + me * shard
    seg = jnp.zeros((shard, LANES), jnp.int32)
    for end in ends:
        seg = seg + jnp.where(row >= end, 1, 0)
    mine = lane == seg
    w = w_v[...]

    def seg_sums(val):
        per_row = jnp.sum(val, axis=1, keepdims=True)
        return jnp.sum(jnp.where(mine, per_row, 0.0), axis=0, keepdims=True)

    w_sums = seg_sums(w * w)

    g = r_2[zz, 0:shard, :]
    for d in range(1, PARTS):
        src = (zz + d) % PARTS
        scoped('wait_z', remote(r_2.at[0, pl.ds(0, shard)], r_z.at[src, pl.ds(0, shard)], sz_s, sz_r.at[src], me).wait_recv)
        g = g + r_z[src, 0:shard, :]
    g = g * (1.0 / ndev)

    def put(stat, value, s_sem, r_sem, lo, hi):
        stat[pl.ds(me, 1), :] = value

        def send(i, _):
            remote(stat.at[pl.ds(me, 1)], stat.at[pl.ds(me, 1)], s_sem, r_sem, (me + i) % ndev).start()
            return 0

        lax.fori_loop(lo, hi, send, 0)

    def rows_in(stat, count, sem):
        return pltpu.make_async_copy(stat.at[pl.ds(0, count)], stat.at[pl.ds(0, count)], sem)

    one_lane = lax.broadcasted_iota(jnp.int32, (1, LANES), 1)
    g_sq = jnp.sum(jnp.sum(g * g, axis=0, keepdims=True), axis=1, keepdims=True)
    put(stat1, jnp.where(one_lane == 64, g_sq, w_sums), t1_s, t1_r, 1, ndev)
    scoped('wait_stat1', rows_in(stat1, ndev - 1, t1_r).wait)
    total1 = jnp.sum(stat1[...], axis=0, keepdims=True)
    gn = jnp.sqrt(jnp.sum(jnp.where(one_lane == 64, total1, 0.0), axis=1, keepdims=True))
    h = g / jnp.maximum(1.0, gn)
    new_m = BETA_ONE * m_v[...] + (1.0 - BETA_ONE) * h
    new_v = BETA_TWO * v_v[...] + (1.0 - BETA_TWO) * h * h
    decay = jnp.where((seg == 0) | (seg == 2) | (seg == 6) | (seg == 8), DECAY, 0.0)
    u = (new_m / CORR_ONE) / (jnp.sqrt(new_v / CORR_TWO) + EPSILON) + decay * w
    plane = ndev // PARTS
    starts = [0] + ends[:-1]
    assert all((end - 1) // (plane * shard) - start // (plane * shard) <= 1 for start, end in zip(starts, ends))
    stat2[pl.ds(me, 1), :] = seg_sums(u * u)

    def send2(i, _, d):
        to = zz * plane + i

        @pl.when((to >= 0) & (to < ndev) & (to != me))
        def _():
            remote(stat2.at[pl.ds(me, 1)], stat2.at[pl.ds(me, 1)], t2_s.at[d + 1], t2_r.at[zz], to).start()

        return 0

    for d in (-1, 1, 0):
        lax.fori_loop(d * plane, (d + 1) * plane, functools.partial(send2, d=d), 0)

    def each_plane(fn):
        fn(1, zz, plane - 1)
        pl.when(zz > 0)(lambda: fn(0, zz - 1, plane))
        pl.when(zz < PARTS - 1)(lambda: fn(2, zz + 1, plane))

    scoped('wait_stat2', each_plane, lambda d, src, count: rows_in(stat2, count, t2_r.at[src]).wait())
    total2 = jnp.sum(stat2[...], axis=0, keepdims=True)
    nm_out[...] = new_m
    nv_out[...] = new_v
    w_norm, u_norm = jnp.sqrt(total1), jnp.sqrt(total2)
    ratio = jnp.where((w_norm > 0) & (u_norm > 0), w_norm / jnp.where(u_norm > 0, u_norm, 1.0), 1.0)
    per_row = jnp.sum(jnp.where(mine, ratio, 0.0), axis=1, keepdims=True)
    new_w = w - LEARN_RATE * per_row * u
    nw_out[...] = new_w
    wfull[pl.ds(me * shard, shard), :] = new_w
    split = (shard + 1) // 2
    parts = ((0, split), (split, shard - split))

    def part_at(s, h):
        return wfull.at[pl.ds(s * shard + parts[h][0], parts[h][1])]

    sent = []

    def push(s, h, *devs):
        for dev in devs:
            sem = agp_r if dev is partner else ag_r.at[s // 2, h]
            remote(part_at(s, h), part_at(s, h), ag_s, sem, dev).start()
            sent.append(parts[h][1])

    def arrived(s, h):
        remote(part_at(s, h), part_at(s, h), ag_s, ag_r.at[s // 2, h], me).wait_recv()

    zs = [zz, zz + 1 - 2 * (zz % 2), 2 - zz // 2, 3 - 3 * (zz // 2)]
    inner = (zz == 1) | (zz == 2)
    diag = peer1 + peer2 - me

    def shifted(s, j):
        return s + (zs[j] - zz) * 8

    for h in range(2):
        push(me, h, shifted(me, 1), peer2, peer1)
    for h in range(2):
        push(me, h, shifted(me, 2), partner)
    def relay(j):
        @pl.when(inner)
        def _():
            s = shifted(me, j)
            for h in range(2):
                scoped('relay_%d' % j, arrived, s, h)
                remote(part_at(s, h), part_at(s, h), agz_s, ag_r.at[s // 2, h], shifted(me, 1)).start()

    relay(2)
    for kind, j in (('a', 0), ('z', 1), ('z', 2), ('r', 3), ('a', 1), ('z', 3), ('a', 2), ('a', 3), ('b', 0), ('d', 0),
                    ('b', 1), ('d', 1), ('b', 2), ('d', 2), ('b', 3), ('d', 3)):
        if kind == 'r':
            relay(j)
            continue
        s = shifted({'a': peer1, 'z': me, 'b': peer2, 'd': diag}[kind], j)
        for h in range(2):
            if kind == 'z' and j > 1:
                pl.when(jnp.logical_not(inner))(lambda: scoped('got_z%d' % j, arrived, s, h))
            else:
                scoped('got_%s%d' % (kind, j), arrived, s, h)
            push(s, h, *{'a': (peer2, partner), 'z': (peer2, peer1, partner)}.get(kind, (partner,)))

    theirs = wfull.at[pl.ds(0, ndev // 2 * shard)]
    scoped('got_rest', pltpu.make_async_copy(theirs, theirs, agp_r).wait)
    par_out[...] = wfull[...].astype(BF16)

    def all_sent(buf, count, sem):
        pltpu.make_async_copy(buf.at[pl.ds(0, count)], buf.at[pl.ds(0, count)], sem).wait()

    scoped('all_sent_gflat', all_sent, gflat, 16 * shard, sd_s)
    scoped('all_sent_gflat', all_sent, gflat, 8 * shard, s1_s)
    scoped('all_sent_gflat', all_sent, gflat, 4 * shard, s2_s)
    scoped('all_sent_gflat', all_sent, gflat, 3 * shard, sz_s)
    scoped('all_sent_stat1', all_sent, stat1, ndev - 1, t1_s)
    each_plane(lambda d, src, count: rows_in(stat2, count, t2_s.at[d]).wait())
    scoped('all_sent_wfull', all_sent, wfull, sum(sent), ag_s)
    pl.when(inner)(lambda: all_sent(wfull, 2 * shard, agz_s))


def write_kernel(*refs):
    sem = refs[-1]
    half = len(refs) // 2
    copies = [pltpu.make_async_copy(src, dst, sem.at[i]) for i, (src, dst) in enumerate(zip(refs[:half], refs[half:-1]))]
    for copy in reversed(copies):
        copy.start()
    for copy in copies:
        copy.wait()


def solution(mesh):
    ndev = mesh.shape['dp']

    def local_step(weights, moment_one, moment_two, x_qkv, dy_qkv, x_proj, dy_proj, x_inter, dy_inter, x_out, dy_out, ln_grad):
        tokens, width = x_qkv.shape
        shard = weights.shape[0] // LANES
        rows = shard * ndev
        flat = lambda a: a.reshape(-1, LANES)
        acts = (x_qkv, dy_qkv, x_proj, dy_proj, x_inter, dy_inter, x_out, dy_out)
        vm = pltpu.VMEM
        pad = -(-shard // 8) * 8
        state = jax.ShapeDtypeStruct((shard, LANES), F32)
        mid = (vm((shard, LANES), F32),) * 3 + (vm((rows, LANES), BF16),)
        dma = pltpu.SemaphoreType.DMA
        hbm = pl.BlockSpec(memory_space=pltpu.HBM)
        whole = pl.BlockSpec(memory_space=pltpu.VMEM)
        out_shape = (state, state, state, jax.ShapeDtypeStruct((rows, LANES), BF16))
        outs = pl.pallas_call(
            functools.partial(comm_kernel, (width, shard, ndev, rows)),
            out_shape=mid,
            in_specs=[hbm] * 12,
            out_specs=(whole,) * 4,
            scratch_shapes=[
                vm((4, tokens, width), BF16), vm((3, tokens, 4 * width), BF16), vm((4, width), F32)] + [
                vm((shard, LANES), F32)] * 3 + [
                vm((3, width + 16, 4 * width), F32), vm((16, width), F32), vm((rows, LANES), F32),
                vm((16, pad, LANES), F32), vm((8, pad, LANES), F32), vm((4, pad, LANES), F32), vm((4, pad, LANES), F32),
                vm((ndev, LANES), F32), vm((ndev, LANES), F32), vm((rows, LANES), F32),
                dma((3 * CHUNKS,)), dma((CHUNKS,)), dma((4,)), dma, dma((4,)), dma, dma((8,)), dma, dma((4,)), dma, dma((4,)),
                dma, dma, dma((3,)), dma((PARTS,)), dma, dma((ndev // 2, 2)), dma, dma],
            compiler_params=pltpu.CompilerParams(collective_id=0, has_side_effects=True, vmem_limit_bytes=61 * 2 ** 20),
            name='lamb_step',
        )(*acts, ln_grad.reshape(4, width), flat(weights), flat(moment_one), flat(moment_two))
        new_w, new_m, new_v, params = pl.pallas_call(
            write_kernel, out_shape=out_shape, in_specs=[whole] * 4, out_specs=(hbm,) * 4,
            scratch_shapes=[dma((4,))], name='write_out')(*[pltpu.with_memory_space_constraint(a, pltpu.VMEM) for a in outs])
        return new_w.reshape(-1), new_m.reshape(-1), new_v.reshape(-1), params.reshape(-1)

    row_spec = P('dp', None)
    in_specs = (P('dp'), P('dp'), P('dp'), row_spec, row_spec, row_spec, row_spec, row_spec, row_spec, row_spec, row_spec, P('dp', None, None))
    out_specs = (P('dp'), P('dp'), P('dp'), P())
    return jax.shard_map(local_step, mesh=mesh, in_specs=in_specs, out_specs=out_specs, check_vma=False)
```

```python
import functools

import jax
import jax.numpy as jnp
from jax import lax
from jax.experimental import pallas as pl
from jax.experimental.pallas import tpu as pltpu
from jax.sharding import PartitionSpec as P

STEP = 10
LEARN_RATE = 0.5
BETA_ONE = 0.9
BETA_TWO = 0.999
EPSILON = 1e-6
DECAY = 0.01
CORR_ONE = 1.0 - BETA_ONE ** STEP
CORR_TWO = 1.0 - BETA_TWO ** STEP

LANES = 128
CHUNKS = 2
PARTS = 4
F32 = jnp.float32
BF16 = jnp.bfloat16


def tensor_sizes(width):
    return [3 * width * width, 3 * width, width * width, width, width, width,
            4 * width * width, 4 * width, 4 * width * width, width, width, width]


def row_ends(width):
    ends, total = [], 0
    for size in tensor_sizes(width):
        total += size // LANES
        ends.append(total)
    return ends


def scoped(name, fn, *args):
    with jax.named_scope(name):
        return fn(*args)


def comm_kernel(dims, x_qkv, dy_qkv, x_proj, dy_proj, x_inter, dy_inter, x_out, dy_out, ln, w_in, m_in, v_in,
                nw_out, nm_out, nv_out, par_out,
                xb, yb, ln_v, w_v, m_v, v_v, acc, bias_out, gflat, r_d, r_1, r_2, r_z, stat1, stat2, wfull,
                in_sem, in2_sem, st_sem, sd_s, sd_r, s1_s, s1_r, s2_s, s2_r, sz_s, sz_r,
                t1_s, t1_r, t2_s, t2_r, ag_s, ag_r, agp_r, agz_s):
    width, shard, ndev, rows = dims
    tokens = x_qkv.shape[0]
    step = tokens // CHUNKS
    ends = row_ends(width)
    me = lax.axis_index('dp')
    core, xx, yy, zz = me % 2, (me // 2) % 2, (me // 4) % 2, me // 8
    partner = me + 1 - 2 * core
    first = xx * (1 - core) + yy * core
    second = yy * (1 - core) + xx * core
    peer1 = me + (1 - 2 * first) * (2 * (1 - core) + 4 * core)
    peer2 = me + (1 - 2 * second) * (4 * (1 - core) + 2 * core)

    def slot(a, b):
        return (1 - core) * (2 * b + a) + core * (2 * a + b)

    small = [pltpu.make_async_copy(s, d, st_sem.at[i])
             for i, (s, d) in enumerate(((ln, ln_v), (w_in, w_v), (m_in, m_v), (v_in, v_v)))]
    for copy in small:
        copy.start()
    wide = 4 * width
    cut = 3 * width
    groups = (((dy_out, xb, 0, 0), (x_out, yb, 0, 0)),
              ((x_qkv, xb, 1, 0), (x_proj, xb, 2, 0), (dy_qkv, yb, 1, 0), (dy_proj, yb, 1, cut)),
              ((x_inter, xb, 3, 0), (dy_inter, yb, 2, 0)))
    for m, group in enumerate(groups):
        def start(k, _, m=m, group=group):
            at = pl.ds(pl.multiple_of(k * step, step), step)
            for src, dst, slab, col in group:
                to = dst.at[slab, at] if src.shape[1] == dst.shape[2] else dst.at[slab, at, pl.ds(col, src.shape[1])]
                sem = in2_sem.at[k] if slab == 2 and dst is xb else in_sem.at[m * CHUNKS + k]
                pltpu.make_async_copy(src.at[at], to, sem).start()
            return 0

        lax.fori_loop(0, CHUNKS, start, 0)

    barrier = pltpu.get_barrier_semaphore()
    stat2[...] = jnp.zeros(stat2.shape, F32)

    def hello(i, _):
        pl.semaphore_signal(barrier, inc=1, device_id=((me + i) % ndev,), device_id_type=pl.DeviceIdType.MESH)
        return 0

    lax.fori_loop(1, ndev, hello, 0)

    def remote(src, dst, s_sem, r_sem, dev):
        return pltpu.make_async_remote_copy(src_ref=src, dst_ref=dst, send_sem=s_sem, recv_sem=r_sem,
                                            device_id=(dev,), device_id_type=pl.DeviceIdType.MESH)

    ones = jnp.ones((16, step), BF16)
    acc[...] = jnp.zeros(acc.shape, F32)
    bias_out[...] = jnp.zeros(bias_out.shape, F32)

    def products(i, _):
        m, k = i // CHUNKS, i % CHUNKS
        both = yb.at[0, pl.ds(0, step * 5 // 4)]
        pltpu.make_async_copy(both, both, in_sem.at[i]).wait()

        @pl.when(m == 1)
        def _():
            half = xb.at[2, pl.ds(0, step)]
            pltpu.make_async_copy(half, half, in2_sem.at[k]).wait()

        at = pl.ds(pl.multiple_of(k * step, step), step)
        lhs1 = jnp.concatenate([xb[m + m // 2, at, :].T, ones], axis=0)
        acc[m, :, 0:cut] += jnp.dot(lhs1, yb[m, at, 0:cut], preferred_element_type=F32)
        lhs2 = jnp.concatenate([xb[2 * m - m // 2, at, :].T, ones], axis=0)
        acc[m, :, cut:wide] += jnp.dot(lhs2, yb[m, at, cut:wide], preferred_element_type=F32)

        @pl.when(m == 0)
        def _():
            bias_out[...] += jnp.dot(ones, xb[0, at, :], preferred_element_type=F32)

        for at_i, fn in services.items():
            pl.when(i == at_i)(fn)
        return 0

    def spread(base, m, lo, n):
        cols = n // LANES
        for j in range(cols):
            at = slice(lo + j * LANES, lo + (j + 1) * LANES)
            gflat[pl.ds(base + j, width, stride=cols), :] = acc[m, 0:width, at]
            gflat[pl.ds(base + cols * width + j, 1), :] = acc[m, width:width + 1, at]

    def spread_out():
        cols = width // LANES
        for j in range(cols):
            at = slice(j * LANES, (j + 1) * LANES)
            gflat[pl.ds(ends[7] + j, wide, stride=cols), :] = acc[0, at, :].T
            gflat[pl.ds(ends[8] + j, 1), :] = bias_out[0:1, at]
        small[0].wait()
        for r, start in enumerate((ends[3], ends[4], ends[9], ends[10])):
            for j in range(cols):
                gflat[pl.ds(start + j, 1), :] = ln_v[r:r + 1, j * LANES:(j + 1) * LANES]
        gflat[pl.ds(ends[11], rows - ends[11]), :] = jnp.zeros((rows - ends[11], LANES), F32)

    def send_d(g):
        for q in range(4):
            s = g * 8 + q * 2 + 1 - core
            remote(gflat.at[pl.ds(s * shard, shard)], r_d.at[g * 4 + q, pl.ds(0, shard)],
                   sd_s, sd_r.at[g], partner).start()

    def copy_1(g, b):
        return remote(r_d.at[g * 4 + slot(1 - first, b), pl.ds(0, shard)], r_1.at[g * 2 + b, pl.ds(0, shard)],
                      s1_s, s1_r.at[g * 2 + b], peer1)

    def copy_2(g):
        return remote(r_1.at[g * 2 + 1 - second, pl.ds(0, shard)], r_2.at[g, pl.ds(0, shard)],
                      s2_s, s2_r.at[g], peer2)

    def add_d(a, b, g):
        q = slot(a, b)
        i = g * 4 + q
        r_d[i, 0:shard, :] += gflat[pl.ds((g * 8 + q * 2 + core) * shard, shard), :]

    def d_to_1(g):
        four = gflat.at[pl.ds(0, 4 * shard)]
        pltpu.make_async_copy(four, four, sd_r.at[g]).wait()
        for b in (1 - second, second):
            add_d(1 - first, b, g)
            copy_1(g, b).start()
        for b in range(2):
            add_d(first, b, g)

    def one_to_2(g):
        for b in (1 - second, second):
            i = g * 2 + b
            remote(r_d.at[0, pl.ds(0, shard)], r_1.at[i, pl.ds(0, shard)], s1_s, s1_r.at[i], peer1).wait_recv()
            r_1[i, 0:shard, :] += r_d[g * 4 + slot(first, b), 0:shard, :]
            if b is not second:
                copy_2(g).start()

    def two_to_z(g):
        copy_2(g).wait_recv()
        r_2[g, 0:shard, :] += r_1[g * 2 + second, 0:shard, :]

        @pl.when(zz != g)
        def _():
            remote(r_2.at[g, pl.ds(0, shard)], r_z.at[zz, pl.ds(0, shard)], sz_s, sz_r.at[zz],
                   me + (g - zz) * 8).start()

    def after_out():
        scoped('spread_out', spread_out)
        scoped('barrier', pl.semaphore_wait, barrier, ndev - 1)
        send_d(3)

    def after_qkv():
        scoped('spread_qkv', spread, 0, 1, 0, cut)
        scoped('spread_proj', spread, ends[1], 1, cut, width)
        send_d(0)

    services = {CHUNKS - 1: after_out,
                CHUNKS: lambda: scoped('in_d1_3', d_to_1, 3),
                2 * CHUNKS - 1: after_qkv,
                2 * CHUNKS: lambda: scoped('in_d1_0', d_to_1, 0)}
    scoped('products', lax.fori_loop, 0, 3 * CHUNKS, products, 0)
    scoped('spread_inter', spread, ends[5], 2, 0, wide)
    scoped('send_d_1', send_d, 1)
    scoped('send_d_2', send_d, 2)
    scoped('one_to_2_3', one_to_2, 3)
    scoped('d_to_1_1', d_to_1, 1)
    scoped('d_to_1_2', d_to_1, 2)
    scoped('one_to_2_0', one_to_2, 0)
    scoped('two_to_z_3', two_to_z, 3)
    scoped('one_to_2_1', one_to_2, 1)
    scoped('two_to_z_0', two_to_z, 0)
    scoped('one_to_2_2', one_to_2, 2)
    scoped('two_to_z_1', two_to_z, 1)
    scoped('two_to_z_2', two_to_z, 2)

    for copy in small[1:]:
        scoped('wait_state', copy.wait)
    lane = lax.broadcasted_iota(jnp.int32, (shard, LANES), 1)
    row = lax.broadcasted_iota(jnp.int32, (shard, LANES), 0) + me * shard
    seg = jnp.zeros((shard, LANES), jnp.int32)
    for end in ends:
        seg = seg + jnp.where(row >= end, 1, 0)
    mine = lane == seg
    w = w_v[...]

    def seg_sums(val):
        per_row = jnp.sum(val, axis=1, keepdims=True)
        return jnp.sum(jnp.where(mine, per_row, 0.0), axis=0, keepdims=True)

    w_sums = seg_sums(w * w)

    g = r_2[zz, 0:shard, :]
    for d in range(1, PARTS):
        src = (zz + d) % PARTS
        scoped('wait_z', remote(r_2.at[0, pl.ds(0, shard)], r_z.at[src, pl.ds(0, shard)], sz_s, sz_r.at[src], me).wait_recv)
        g = g + r_z[src, 0:shard, :]
    g = g * (1.0 / ndev)

    def put(stat, value, s_sem, r_sem, lo, hi):
        stat[pl.ds(me, 1), :] = value

        def send(i, _):
            remote(stat.at[pl.ds(me, 1)], stat.at[pl.ds(me, 1)], s_sem, r_sem, (me + i) % ndev).start()
            return 0

        lax.fori_loop(lo, hi, send, 0)

    def rows_in(stat, count, sem):
        return pltpu.make_async_copy(stat.at[pl.ds(0, count)], stat.at[pl.ds(0, count)], sem)

    one_lane = lax.broadcasted_iota(jnp.int32, (1, LANES), 1)
    g_sq = jnp.sum(jnp.sum(g * g, axis=0, keepdims=True), axis=1, keepdims=True)
    put(stat1, jnp.where(one_lane == 64, g_sq, w_sums), t1_s, t1_r, 1, ndev)
    scoped('wait_stat1', rows_in(stat1, ndev - 1, t1_r).wait)
    total1 = jnp.sum(stat1[...], axis=0, keepdims=True)
    gn = jnp.sqrt(jnp.sum(jnp.where(one_lane == 64, total1, 0.0), axis=1, keepdims=True))
    h = g / jnp.maximum(1.0, gn)
    new_m = BETA_ONE * m_v[...] + (1.0 - BETA_ONE) * h
    new_v = BETA_TWO * v_v[...] + (1.0 - BETA_TWO) * h * h
    decay = jnp.where((seg == 0) | (seg == 2) | (seg == 6) | (seg == 8), DECAY, 0.0)
    u = (new_m / CORR_ONE) / (jnp.sqrt(new_v / CORR_TWO) + EPSILON) + decay * w
    plane = ndev // PARTS
    starts = [0] + ends[:-1]
    assert all((end - 1) // (plane * shard) - start // (plane * shard) <= 1 for start, end in zip(starts, ends))
    stat2[pl.ds(me, 1), :] = seg_sums(u * u)

    def send2(i, _, d):
        to = zz * plane + i

        @pl.when((to >= 0) & (to < ndev) & (to != me))
        def _():
            remote(stat2.at[pl.ds(me, 1)], stat2.at[pl.ds(me, 1)], t2_s.at[d + 1], t2_r.at[zz], to).start()

        return 0

    for d in (-1, 1, 0):
        lax.fori_loop(d * plane, (d + 1) * plane, functools.partial(send2, d=d), 0)

    def each_plane(fn):
        fn(1, zz, plane - 1)
        pl.when(zz > 0)(lambda: fn(0, zz - 1, plane))
        pl.when(zz < PARTS - 1)(lambda: fn(2, zz + 1, plane))

    scoped('wait_stat2', each_plane, lambda d, src, count: rows_in(stat2, count, t2_r.at[src]).wait())
    total2 = jnp.sum(stat2[...], axis=0, keepdims=True)
    nm_out[...] = new_m
    nv_out[...] = new_v
    w_norm, u_norm = jnp.sqrt(total1), jnp.sqrt(total2)
    ratio = jnp.where((w_norm > 0) & (u_norm > 0), w_norm / jnp.where(u_norm > 0, u_norm, 1.0), 1.0)
    per_row = jnp.sum(jnp.where(mine, ratio, 0.0), axis=1, keepdims=True)
    new_w = w - LEARN_RATE * per_row * u
    nw_out[...] = new_w
    wfull[pl.ds(me * shard, shard), :] = new_w
    late = shard // 5 + 1
    split = (shard - late + 1) // 2
    parts = ((0, split), (split, shard - late - split), (shard - late, late))

    def part_at(s, h):
        return wfull.at[pl.ds(s * shard + parts[h][0], parts[h][1])]

    sent = []

    def push(s, h, *devs):
        for dev in devs:
            sem = agp_r if dev is partner else ag_r.at[s // 2, h]
            remote(part_at(s, h), part_at(s, h), ag_s, sem, dev).start()
            sent.append(parts[h][1])

    def arrived(s, h):
        remote(part_at(s, h), part_at(s, h), ag_s, ag_r.at[s // 2, h], me).wait_recv()

    zs = [zz, zz + 1 - 2 * (zz % 2), 2 - zz // 2, 3 - 3 * (zz // 2)]
    inner = (zz == 1) | (zz == 2)
    diag = peer1 + peer2 - me

    def shifted(s, j):
        return s + (zs[j] - zz) * 8

    push(me, 2, peer2, peer1)
    for h in range(2):
        push(me, h, shifted(me, 1), peer2, peer1)
    for h in range(2):
        push(me, h, shifted(me, 2), partner)
    push(me, 2, partner)

    passed = []

    def relay(base, j, h):
        passed.append(parts[h][1])

        @pl.when(inner)
        def _():
            s = shifted(base, j)
            scoped('relay_%d%d' % (j, h), arrived, s, h)
            remote(part_at(s, h), part_at(s, h), agz_s, ag_r.at[s // 2, h], shifted(me, 1)).start()

    def got(base, j, h, name, relayed=False):
        s = shifted(base, j)
        if relayed:
            pl.when(jnp.logical_not(inner))(lambda: scoped('got_%s%d%d' % (name, j, h), arrived, s, h))
        else:
            scoped('got_%s%d%d' % (name, j, h), arrived, s, h)
        return s

    column = (me, peer1, peer2, diag)
    for h in range(2):
        relay(me, 2, h)
    push(got(peer1, 0, 2, 'a'), 2, peer2, partner)
    for h in range(2):
        push(got(peer1, 0, h, 'a'), h, peer2, partner)
    for j in (1, 2):
        for h in range(2):
            push(got(me, j, h, 'z', j > 1), h, peer2, peer1, partner)
    for base in (peer2, diag):
        push(got(base, 0, 2, 'b'), 2, partner)
    for base in column:
        for j in (1, 2):
            push(base, 2, shifted(me, j))
    for h in range(2):
        relay(me, 3, h)
    for h in range(2):
        push(got(peer1, 1, h, 'a'), h, peer2, partner)
    for h in range(2):
        push(got(me, 3, h, 'z', True), h, peer2, peer1, partner)
    for base in column:
        relay(base, 2, 2)
    for h in range(2):
        push(got(peer1, 2, h, 'a'), h, peer2, partner)
    for base in column:
        relay(base, 3, 2)
    for h in range(2):
        push(got(peer1, 3, h, 'a'), h, peer2, partner)
    for j in range(1, PARTS):
        for base in column:
            push(got(base, j, 2, 'c', j > 1), 2, partner)
    for j in range(PARTS):
        for base, name in ((peer2, 'b'), (diag, 'd')):
            for h in range(2):
                push(got(base, j, h, name), h, partner)

    theirs = wfull.at[pl.ds(0, ndev // 2 * shard)]
    scoped('got_rest', pltpu.make_async_copy(theirs, theirs, agp_r).wait)
    par_out[...] = wfull[...].astype(BF16)

    def all_sent(buf, count, sem):
        pltpu.make_async_copy(buf.at[pl.ds(0, count)], buf.at[pl.ds(0, count)], sem).wait()

    scoped('all_sent_gflat', all_sent, gflat, 16 * shard, sd_s)
    scoped('all_sent_gflat', all_sent, gflat, 8 * shard, s1_s)
    scoped('all_sent_gflat', all_sent, gflat, 4 * shard, s2_s)
    scoped('all_sent_gflat', all_sent, gflat, 3 * shard, sz_s)
    scoped('all_sent_stat1', all_sent, stat1, ndev - 1, t1_s)
    each_plane(lambda d, src, count: rows_in(stat2, count, t2_s.at[d]).wait())
    scoped('all_sent_wfull', all_sent, wfull, sum(sent), ag_s)
    pl.when(inner)(lambda: all_sent(wfull, sum(passed), agz_s))


def write_kernel(*refs):
    sem = refs[-1]
    half = len(refs) // 2
    copies = [pltpu.make_async_copy(src, dst, sem.at[i]) for i, (src, dst) in enumerate(zip(refs[:half], refs[half:-1]))]
    for copy in reversed(copies):
        copy.start()
    for copy in copies:
        copy.wait()


def solution(mesh):
    ndev = mesh.shape['dp']

    def local_step(weights, moment_one, moment_two, x_qkv, dy_qkv, x_proj, dy_proj, x_inter, dy_inter, x_out, dy_out, ln_grad):
        tokens, width = x_qkv.shape
        shard = weights.shape[0] // LANES
        rows = shard * ndev
        flat = lambda a: a.reshape(-1, LANES)
        acts = (x_qkv, dy_qkv, x_proj, dy_proj, x_inter, dy_inter, x_out, dy_out)
        vm = pltpu.VMEM
        pad = -(-shard // 8) * 8
        state = jax.ShapeDtypeStruct((shard, LANES), F32)
        mid = (vm((shard, LANES), F32),) * 3 + (vm((rows, LANES), BF16),)
        dma = pltpu.SemaphoreType.DMA
        hbm = pl.BlockSpec(memory_space=pltpu.HBM)
        whole = pl.BlockSpec(memory_space=pltpu.VMEM)
        out_shape = (state, state, state, jax.ShapeDtypeStruct((rows, LANES), BF16))
        outs = pl.pallas_call(
            functools.partial(comm_kernel, (width, shard, ndev, rows)),
            out_shape=mid,
            in_specs=[hbm] * 12,
            out_specs=(whole,) * 4,
            scratch_shapes=[
                vm((4, tokens, width), BF16), vm((3, tokens, 4 * width), BF16), vm((4, width), F32)] + [
                vm((shard, LANES), F32)] * 3 + [
                vm((3, width + 16, 4 * width), F32), vm((16, width), F32), vm((rows, LANES), F32),
                vm((16, pad, LANES), F32), vm((8, pad, LANES), F32), vm((4, pad, LANES), F32), vm((4, pad, LANES), F32),
                vm((ndev, LANES), F32), vm((ndev, LANES), F32), vm((rows, LANES), F32),
                dma((3 * CHUNKS,)), dma((CHUNKS,)), dma((4,)), dma, dma((4,)), dma, dma((8,)), dma, dma((4,)), dma, dma((4,)),
                dma, dma, dma((3,)), dma((PARTS,)), dma, dma((ndev // 2, 3)), dma, dma],
            compiler_params=pltpu.CompilerParams(collective_id=0, has_side_effects=True, vmem_limit_bytes=61 * 2 ** 20),
            name='lamb_step',
        )(*acts, ln_grad.reshape(4, width), flat(weights), flat(moment_one), flat(moment_two))
        new_w, new_m, new_v, params = pl.pallas_call(
            write_kernel, out_shape=out_shape, in_specs=[whole] * 4, out_specs=(hbm,) * 4,
            scratch_shapes=[dma((4,))], name='write_out')(*[pltpu.with_memory_space_constraint(a, pltpu.VMEM) for a in outs])
        return new_w.reshape(-1), new_m.reshape(-1), new_v.reshape(-1), params.reshape(-1)

    row_spec = P('dp', None)
    in_specs = (P('dp'), P('dp'), P('dp'), row_spec, row_spec, row_spec, row_spec, row_spec, row_spec, row_spec, row_spec, P('dp', None, None))
    out_specs = (P('dp'), P('dp'), P('dp'), P())
    return jax.shard_map(local_step, mesh=mesh, in_specs=in_specs, out_specs=out_specs, check_vma=False)
```

```python
import functools

import jax
import jax.numpy as jnp
from jax import lax
from jax.experimental import pallas as pl
from jax.experimental.pallas import tpu as pltpu
from jax.sharding import PartitionSpec as P

STEP = 10
LEARN_RATE = 0.5
BETA_ONE = 0.9
BETA_TWO = 0.999
EPSILON = 1e-6
DECAY = 0.01
CORR_ONE = 1.0 - BETA_ONE ** STEP
CORR_TWO = 1.0 - BETA_TWO ** STEP

LANES = 128
CHUNKS = 2
PARTS = 4
F32 = jnp.float32
BF16 = jnp.bfloat16


def tensor_sizes(width):
    return [3 * width * width, 3 * width, width * width, width, width, width,
            4 * width * width, 4 * width, 4 * width * width, width, width, width]


def row_ends(width):
    ends, total = [], 0
    for size in tensor_sizes(width):
        total += size // LANES
        ends.append(total)
    return ends


def scoped(name, fn, *args):
    with jax.named_scope(name):
        return fn(*args)


def comm_kernel(dims, x_qkv, dy_qkv, x_proj, dy_proj, x_inter, dy_inter, x_out, dy_out, ln, w_in, m_in, v_in,
                nw_out, nm_out, nv_out, par_out,
                xb, yb, ln_v, w_v, m_v, v_v, acc, bias_out, gflat, r_d, r_1, r_2, r_z, stat1, stat2, wfull,
                in_sem, in2_sem, st_sem, sd_s, sd_r, s1_s, s1_r, s2_s, s2_r, sz_s, sz_r,
                t1_s, t1_r, t2_s, t2_r, ag_s, ag_r, agp_r, agz_s):
    width, shard, ndev, rows = dims
    tokens = x_qkv.shape[0]
    step = tokens // CHUNKS
    ends = row_ends(width)
    me = lax.axis_index('dp')
    core, xx, yy, zz = me % 2, (me // 2) % 2, (me // 4) % 2, me // 8
    partner = me + 1 - 2 * core
    first = xx * (1 - core) + yy * core
    second = yy * (1 - core) + xx * core
    peer1 = me + (1 - 2 * first) * (2 * (1 - core) + 4 * core)
    peer2 = me + (1 - 2 * second) * (4 * (1 - core) + 2 * core)

    def slot(a, b):
        return (1 - core) * (2 * b + a) + core * (2 * a + b)

    small = [pltpu.make_async_copy(s, d, st_sem.at[i])
             for i, (s, d) in enumerate(((ln, ln_v), (w_in, w_v), (m_in, m_v), (v_in, v_v)))]
    for copy in small:
        copy.start()
    wide = 4 * width
    cut = 3 * width
    groups = (((dy_out, xb, 0, 0), (x_out, yb, 0, 0)),
              ((x_qkv, xb, 1, 0), (x_proj, xb, 2, 0), (dy_qkv, yb, 1, 0), (dy_proj, yb, 1, cut)),
              ((x_inter, xb, 3, 0), (dy_inter, yb, 2, 0)))
    for m, group in enumerate(groups):
        def start(k, _, m=m, group=group):
            at = pl.ds(pl.multiple_of(k * step, step), step)
            for src, dst, slab, col in group:
                to = dst.at[slab, at] if src.shape[1] == dst.shape[2] else dst.at[slab, at, pl.ds(col, src.shape[1])]
                sem = in2_sem.at[k] if slab == 2 and dst is xb else in_sem.at[m * CHUNKS + k]
                pltpu.make_async_copy(src.at[at], to, sem).start()
            return 0

        lax.fori_loop(0, CHUNKS, start, 0)

    barrier = pltpu.get_barrier_semaphore()
    stat2[...] = jnp.zeros(stat2.shape, F32)

    def hello(i, _):
        pl.semaphore_signal(barrier, inc=1, device_id=((me + i) % ndev,), device_id_type=pl.DeviceIdType.MESH)
        return 0

    lax.fori_loop(1, ndev, hello, 0)

    def remote(src, dst, s_sem, r_sem, dev):
        return pltpu.make_async_remote_copy(src_ref=src, dst_ref=dst, send_sem=s_sem, recv_sem=r_sem,
                                            device_id=(dev,), device_id_type=pl.DeviceIdType.MESH)

    ones = jnp.ones((16, step), BF16)
    acc[...] = jnp.zeros(acc.shape, F32)
    bias_out[...] = jnp.zeros(bias_out.shape, F32)

    def products(i, _):
        m, k = i // CHUNKS, i % CHUNKS
        both = yb.at[0, pl.ds(0, step * 5 // 4)]
        pltpu.make_async_copy(both, both, in_sem.at[i]).wait()

        @pl.when(m == 1)
        def _():
            half = xb.at[2, pl.ds(0, step)]
            pltpu.make_async_copy(half, half, in2_sem.at[k]).wait()

        at = pl.ds(pl.multiple_of(k * step, step), step)
        lhs1 = jnp.concatenate([xb[m + m // 2, at, :].T, ones], axis=0)
        acc[m, :, 0:cut] += jnp.dot(lhs1, yb[m, at, 0:cut], preferred_element_type=F32)
        lhs2 = jnp.concatenate([xb[2 * m - m // 2, at, :].T, ones], axis=0)
        acc[m, :, cut:wide] += jnp.dot(lhs2, yb[m, at, cut:wide], preferred_element_type=F32)

        @pl.when(m == 0)
        def _():
            bias_out[...] += jnp.dot(ones, xb[0, at, :], preferred_element_type=F32)

        for at_i, fn in services.items():
            pl.when(i == at_i)(fn)
        return 0

    def spread(base, m, lo, n):
        cols = n // LANES
        for j in range(cols):
            at = slice(lo + j * LANES, lo + (j + 1) * LANES)
            gflat[pl.ds(base + j, width, stride=cols), :] = acc[m, 0:width, at]
            gflat[pl.ds(base + cols * width + j, 1), :] = acc[m, width:width + 1, at]

    def spread_out():
        cols = width // LANES
        for j in range(cols):
            at = slice(j * LANES, (j + 1) * LANES)
            gflat[pl.ds(ends[7] + j, wide, stride=cols), :] = acc[0, at, :].T
            gflat[pl.ds(ends[8] + j, 1), :] = bias_out[0:1, at]
        small[0].wait()
        for r, start in enumerate((ends[3], ends[4], ends[9], ends[10])):
            for j in range(cols):
                gflat[pl.ds(start + j, 1), :] = ln_v[r:r + 1, j * LANES:(j + 1) * LANES]
        gflat[pl.ds(ends[11], rows - ends[11]), :] = jnp.zeros((rows - ends[11], LANES), F32)

    def send_d(g):
        for q in range(4):
            s = g * 8 + q * 2 + 1 - core
            remote(gflat.at[pl.ds(s * shard, shard)], r_d.at[g * 4 + q, pl.ds(0, shard)],
                   sd_s, sd_r.at[g], partner).start()

    def copy_1(g, b):
        return remote(r_d.at[g * 4 + slot(1 - first, b), pl.ds(0, shard)], r_1.at[g * 2 + b, pl.ds(0, shard)],
                      s1_s, s1_r.at[g * 2 + b], peer1)

    def copy_2(g):
        return remote(r_1.at[g * 2 + 1 - second, pl.ds(0, shard)], r_2.at[g, pl.ds(0, shard)],
                      s2_s, s2_r.at[g], peer2)

    def add_d(a, b, g):
        q = slot(a, b)
        i = g * 4 + q
        r_d[i, 0:shard, :] += gflat[pl.ds((g * 8 + q * 2 + core) * shard, shard), :]

    def d_to_1(g):
        four = gflat.at[pl.ds(0, 4 * shard)]
        pltpu.make_async_copy(four, four, sd_r.at[g]).wait()
        for b in (1 - second, second):
            add_d(1 - first, b, g)
            copy_1(g, b).start()
        for b in range(2):
            add_d(first, b, g)

    def one_to_2(g):
        for b in (1 - second, second):
            i = g * 2 + b
            remote(r_d.at[0, pl.ds(0, shard)], r_1.at[i, pl.ds(0, shard)], s1_s, s1_r.at[i], peer1).wait_recv()
            r_1[i, 0:shard, :] += r_d[g * 4 + slot(first, b), 0:shard, :]
            if b is not second:
                copy_2(g).start()

    def two_to_z(g):
        copy_2(g).wait_recv()
        r_2[g, 0:shard, :] += r_1[g * 2 + second, 0:shard, :]

        @pl.when(zz != g)
        def _():
            remote(r_2.at[g, pl.ds(0, shard)], r_z.at[zz, pl.ds(0, shard)], sz_s, sz_r.at[zz],
                   me + (g - zz) * 8).start()

    def after_out():
        scoped('spread_out', spread_out)
        scoped('barrier', pl.semaphore_wait, barrier, ndev - 1)
        send_d(3)

    def after_qkv():
        scoped('spread_qkv', spread, 0, 1, 0, cut)
        scoped('spread_proj', spread, ends[1], 1, cut, width)
        send_d(0)

    services = {CHUNKS - 1: after_out,
                CHUNKS: lambda: scoped('in_d1_3', d_to_1, 3),
                2 * CHUNKS - 1: after_qkv,
                2 * CHUNKS: lambda: scoped('in_d1_0', d_to_1, 0)}
    scoped('products', lax.fori_loop, 0, 3 * CHUNKS, products, 0)
    scoped('spread_inter', spread, ends[5], 2, 0, wide)
    scoped('send_d_1', send_d, 1)
    scoped('send_d_2', send_d, 2)
    scoped('one_to_2_3', one_to_2, 3)
    scoped('d_to_1_1', d_to_1, 1)
    scoped('d_to_1_2', d_to_1, 2)
    scoped('one_to_2_0', one_to_2, 0)
    scoped('two_to_z_3', two_to_z, 3)
    scoped('one_to_2_1', one_to_2, 1)
    scoped('two_to_z_0', two_to_z, 0)
    scoped('one_to_2_2', one_to_2, 2)
    scoped('two_to_z_1', two_to_z, 1)
    scoped('two_to_z_2', two_to_z, 2)

    for copy in small[1:]:
        scoped('wait_state', copy.wait)
    lane = lax.broadcasted_iota(jnp.int32, (shard, LANES), 1)
    row = lax.broadcasted_iota(jnp.int32, (shard, LANES), 0) + me * shard
    seg = jnp.zeros((shard, LANES), jnp.int32)
    for end in ends:
        seg = seg + jnp.where(row >= end, 1, 0)
    mine = lane == seg
    w = w_v[...]

    def seg_sums(val):
        per_row = jnp.sum(val, axis=1, keepdims=True)
        return jnp.sum(jnp.where(mine, per_row, 0.0), axis=0, keepdims=True)

    w_sums = seg_sums(w * w)

    g = r_2[zz, 0:shard, :]
    for d in range(1, PARTS):
        src = (zz + d) % PARTS
        scoped('wait_z', remote(r_2.at[0, pl.ds(0, shard)], r_z.at[src, pl.ds(0, shard)], sz_s, sz_r.at[src], me).wait_recv)
        g = g + r_z[src, 0:shard, :]
    g = g * (1.0 / ndev)

    def put(stat, value, s_sem, r_sem, lo, hi):
        stat[pl.ds(me, 1), :] = value

        def send(i, _):
            remote(stat.at[pl.ds(me, 1)], stat.at[pl.ds(me, 1)], s_sem, r_sem, (me + i) % ndev).start()
            return 0

        lax.fori_loop(lo, hi, send, 0)

    def rows_in(stat, count, sem):
        return pltpu.make_async_copy(stat.at[pl.ds(0, count)], stat.at[pl.ds(0, count)], sem)

    one_lane = lax.broadcasted_iota(jnp.int32, (1, LANES), 1)
    g_sq = jnp.sum(jnp.sum(g * g, axis=0, keepdims=True), axis=1, keepdims=True)
    put(stat1, jnp.where(one_lane == 64, g_sq, w_sums), t1_s, t1_r, 1, ndev)
    scoped('wait_stat1', rows_in(stat1, ndev - 1, t1_r).wait)
    total1 = jnp.sum(stat1[...], axis=0, keepdims=True)
    gn = jnp.sqrt(jnp.sum(jnp.where(one_lane == 64, total1, 0.0), axis=1, keepdims=True))
    h = g / jnp.maximum(1.0, gn)
    new_m = BETA_ONE * m_v[...] + (1.0 - BETA_ONE) * h
    new_v = BETA_TWO * v_v[...] + (1.0 - BETA_TWO) * h * h
    decay = jnp.where((seg == 0) | (seg == 2) | (seg == 6) | (seg == 8), DECAY, 0.0)
    u = (new_m / CORR_ONE) / (jnp.sqrt(new_v / CORR_TWO) + EPSILON) + decay * w
    plane = ndev // PARTS
    starts = [0] + ends[:-1]
    assert all((end - 1) // (plane * shard) - start // (plane * shard) <= 1 for start, end in zip(starts, ends))
    stat2[pl.ds(me, 1), :] = seg_sums(u * u)

    def send2(i, _, d):
        to = zz * plane + i

        @pl.when((to >= 0) & (to < ndev) & (to != me))
        def _():
            remote(stat2.at[pl.ds(me, 1)], stat2.at[pl.ds(me, 1)], t2_s.at[d + 1], t2_r.at[zz], to).start()

        return 0

    for d in (-1, 1, 0):
        lax.fori_loop(d * plane, (d + 1) * plane, functools.partial(send2, d=d), 0)

    def each_plane(fn):
        fn(1, zz, plane - 1)
        pl.when(zz > 0)(lambda: fn(0, zz - 1, plane))
        pl.when(zz < PARTS - 1)(lambda: fn(2, zz + 1, plane))

    scoped('wait_stat2', each_plane, lambda d, src, count: rows_in(stat2, count, t2_r.at[src]).wait())
    total2 = jnp.sum(stat2[...], axis=0, keepdims=True)
    nm_out[...] = new_m
    nv_out[...] = new_v
    w_norm, u_norm = jnp.sqrt(total1), jnp.sqrt(total2)
    ratio = jnp.where((w_norm > 0) & (u_norm > 0), w_norm / jnp.where(u_norm > 0, u_norm, 1.0), 1.0)
    per_row = jnp.sum(jnp.where(mine, ratio, 0.0), axis=1, keepdims=True)
    new_w = w - LEARN_RATE * per_row * u
    nw_out[...] = new_w
    wfull[pl.ds(me * shard, shard), :] = new_w
    late = shard // 5 + 1
    split = (shard - late + 1) // 2
    parts = ((0, split), (split, shard - late - split), (shard - late, late))

    def part_at(s, h):
        return wfull.at[pl.ds(s * shard + parts[h][0], parts[h][1])]

    sent = []

    def push(s, h, *devs):
        for dev in devs:
            sem = agp_r if dev is partner else ag_r.at[s // 2, h]
            remote(part_at(s, h), part_at(s, h), ag_s, sem, dev).start()
            sent.append(parts[h][1])

    def arrived(s, h):
        remote(part_at(s, h), part_at(s, h), ag_s, ag_r.at[s // 2, h], me).wait_recv()

    zs = [zz, zz + 1 - 2 * (zz % 2), 2 - zz // 2, 3 - 3 * (zz // 2)]
    inner = (zz == 1) | (zz == 2)
    diag = peer1 + peer2 - me

    def shifted(s, j):
        return s + (zs[j] - zz) * 8

    push(me, 2, peer2, peer1)
    for h in range(2):
        push(me, h, shifted(me, 1), peer2, peer1)
    for h in range(2):
        push(me, h, shifted(me, 2), partner)
    push(me, 2, partner)

    passed = []

    def relay(base, j, h):
        passed.append(parts[h][1])

        @pl.when(inner)
        def _():
            s = shifted(base, j)
            scoped('relay_%d%d' % (j, h), arrived, s, h)
            remote(part_at(s, h), part_at(s, h), agz_s, ag_r.at[s // 2, h], shifted(me, 1)).start()

    def got(base, j, h, name, relayed=False):
        s = shifted(base, j)
        if relayed:
            pl.when(jnp.logical_not(inner))(lambda: scoped('got_%s%d%d' % (name, j, h), arrived, s, h))
        else:
            scoped('got_%s%d%d' % (name, j, h), arrived, s, h)
        return s

    column = (me, peer1, peer2, diag)
    for h in range(2):
        relay(me, 2, h)
    push(got(peer1, 0, 2, 'a'), 2, peer2, partner)
    for h in range(2):
        push(got(peer1, 0, h, 'a'), h, peer2, partner)
    for j in (1, 2):
        for h in range(2):
            push(got(me, j, h, 'z', j > 1), h, peer2, peer1, partner)
    for h in range(2):
        relay(me, 3, h)
    for base in (peer2, diag):
        push(got(base, 0, 2, 'b'), 2, partner)
    for base in column:
        for j in (1, 2):
            push(base, 2, shifted(me, j))
    for h in range(2):
        push(got(peer1, 1, h, 'a'), h, peer2, partner)
    for h in range(2):
        push(got(me, 3, h, 'z', True), h, peer2, peer1, partner)
    for base in column:
        relay(base, 2, 2)
    for h in range(2):
        push(got(peer1, 2, h, 'a'), h, peer2, partner)
    for base in column:
        relay(base, 3, 2)
    for h in range(2):
        push(got(peer1, 3, h, 'a'), h, peer2, partner)
    for j in range(1, PARTS):
        for base in column:
            push(got(base, j, 2, 'c', j > 1), 2, partner)
    for j in range(PARTS):
        for base, name in ((peer2, 'b'), (diag, 'd')):
            for h in range(2):
                push(got(base, j, h, name), h, partner)

    theirs = wfull.at[pl.ds(0, ndev // 2 * shard)]
    scoped('got_rest', pltpu.make_async_copy(theirs, theirs, agp_r).wait)
    par_out[...] = wfull[...].astype(BF16)

    def all_sent(buf, count, sem):
        pltpu.make_async_copy(buf.at[pl.ds(0, count)], buf.at[pl.ds(0, count)], sem).wait()

    scoped('all_sent_gflat', all_sent, gflat, 16 * shard, sd_s)
    scoped('all_sent_gflat', all_sent, gflat, 8 * shard, s1_s)
    scoped('all_sent_gflat', all_sent, gflat, 4 * shard, s2_s)
    scoped('all_sent_gflat', all_sent, gflat, 3 * shard, sz_s)
    scoped('all_sent_stat1', all_sent, stat1, ndev - 1, t1_s)
    each_plane(lambda d, src, count: rows_in(stat2, count, t2_s.at[d]).wait())
    scoped('all_sent_wfull', all_sent, wfull, sum(sent), ag_s)
    pl.when(inner)(lambda: all_sent(wfull, sum(passed), agz_s))


def write_kernel(*refs):
    sem = refs[-1]
    half = len(refs) // 2
    copies = [pltpu.make_async_copy(src, dst, sem.at[i]) for i, (src, dst) in enumerate(zip(refs[:half], refs[half:-1]))]
    for copy in reversed(copies):
        copy.start()
    for copy in copies:
        copy.wait()


def solution(mesh):
    ndev = mesh.shape['dp']

    def local_step(weights, moment_one, moment_two, x_qkv, dy_qkv, x_proj, dy_proj, x_inter, dy_inter, x_out, dy_out, ln_grad):
        tokens, width = x_qkv.shape
        shard = weights.shape[0] // LANES
        rows = shard * ndev
        flat = lambda a: a.reshape(-1, LANES)
        acts = (x_qkv, dy_qkv, x_proj, dy_proj, x_inter, dy_inter, x_out, dy_out)
        vm = pltpu.VMEM
        pad = -(-shard // 8) * 8
        state = jax.ShapeDtypeStruct((shard, LANES), F32)
        mid = (vm((shard, LANES), F32),) * 3 + (vm((rows, LANES), BF16),)
        dma = pltpu.SemaphoreType.DMA
        hbm = pl.BlockSpec(memory_space=pltpu.HBM)
        whole = pl.BlockSpec(memory_space=pltpu.VMEM)
        out_shape = (state, state, state, jax.ShapeDtypeStruct((rows, LANES), BF16))
        outs = pl.pallas_call(
            functools.partial(comm_kernel, (width, shard, ndev, rows)),
            out_shape=mid,
            in_specs=[hbm] * 12,
            out_specs=(whole,) * 4,
            scratch_shapes=[
                vm((4, tokens, width), BF16), vm((3, tokens, 4 * width), BF16), vm((4, width), F32)] + [
                vm((shard, LANES), F32)] * 3 + [
                vm((3, width + 16, 4 * width), F32), vm((16, width), F32), vm((rows, LANES), F32),
                vm((16, pad, LANES), F32), vm((8, pad, LANES), F32), vm((4, pad, LANES), F32), vm((4, pad, LANES), F32),
                vm((ndev, LANES), F32), vm((ndev, LANES), F32), vm((rows, LANES), F32),
                dma((3 * CHUNKS,)), dma((CHUNKS,)), dma((4,)), dma, dma((4,)), dma, dma((8,)), dma, dma((4,)), dma, dma((4,)),
                dma, dma, dma((3,)), dma((PARTS,)), dma, dma((ndev // 2, 3)), dma, dma],
            compiler_params=pltpu.CompilerParams(collective_id=0, has_side_effects=True, vmem_limit_bytes=61 * 2 ** 20),
            name='lamb_step',
        )(*acts, ln_grad.reshape(4, width), flat(weights), flat(moment_one), flat(moment_two))
        new_w, new_m, new_v, params = pl.pallas_call(
            write_kernel, out_shape=out_shape, in_specs=[whole] * 4, out_specs=(hbm,) * 4,
            scratch_shapes=[dma((4,))], name='write_out')(*[pltpu.with_memory_space_constraint(a, pltpu.VMEM) for a in outs])
        return new_w.reshape(-1), new_m.reshape(-1), new_v.reshape(-1), params.reshape(-1)

    row_spec = P('dp', None)
    in_specs = (P('dp'), P('dp'), P('dp'), row_spec, row_spec, row_spec, row_spec, row_spec, row_spec, row_spec, row_spec, P('dp', None, None))
    out_specs = (P('dp'), P('dp'), P('dp'), P())
    return jax.shard_map(local_step, mesh=mesh, in_specs=in_specs, out_specs=out_specs, check_vma=False)
```

```python
import functools

import jax
import jax.numpy as jnp
from jax import lax
from jax.experimental import pallas as pl
from jax.experimental.pallas import tpu as pltpu
from jax.sharding import PartitionSpec as P

STEP = 10
LEARN_RATE = 0.5
BETA_ONE = 0.9
BETA_TWO = 0.999
EPSILON = 1e-6
DECAY = 0.01
CORR_ONE = 1.0 - BETA_ONE ** STEP
CORR_TWO = 1.0 - BETA_TWO ** STEP

LANES = 128
CHUNKS = 2
PARTS = 4
F32 = jnp.float32
BF16 = jnp.bfloat16


def tensor_sizes(width):
    return [3 * width * width, 3 * width, width * width, width, width, width,
            4 * width * width, 4 * width, 4 * width * width, width, width, width]


def row_ends(width):
    ends, total = [], 0
    for size in tensor_sizes(width):
        total += size // LANES
        ends.append(total)
    return ends


def scoped(name, fn, *args):
    with jax.named_scope(name):
        return fn(*args)


def comm_kernel(dims, x_qkv, dy_qkv, x_proj, dy_proj, x_inter, dy_inter, x_out, dy_out, ln, w_in, m_in, v_in,
                nw_out, nm_out, nv_out, par_out,
                xb, yb, ln_v, w_v, m_v, v_v, acc, bias_out, gflat, r_d, r_1, r_2, r_z, stat1, stat2, wfull,
                in_sem, in2_sem, st_sem, sd_s, sd_r, s1_s, s1_r, s2_s, s2_r, sz_s, sz_r,
                t1_s, t1_r, t2_s, t2_r, ag_s, ag_r, agp_r, agz_s):
    width, shard, ndev, rows = dims
    tokens = x_qkv.shape[0]
    step = tokens // CHUNKS
    ends = row_ends(width)
    me = lax.axis_index('dp')
    core, xx, yy, zz = me % 2, (me // 2) % 2, (me // 4) % 2, me // 8
    partner = me + 1 - 2 * core
    first = xx * (1 - core) + yy * core
    second = yy * (1 - core) + xx * core
    peer1 = me + (1 - 2 * first) * (2 * (1 - core) + 4 * core)
    peer2 = me + (1 - 2 * second) * (4 * (1 - core) + 2 * core)

    def slot(a, b):
        return (1 - core) * (2 * b + a) + core * (2 * a + b)

    small = [pltpu.make_async_copy(s, d, st_sem.at[i])
             for i, (s, d) in enumerate(((ln, ln_v), (w_in, w_v), (m_in, m_v), (v_in, v_v)))]
    for copy in small:
        copy.start()
    wide = 4 * width
    cut = 3 * width
    groups = (((dy_out, xb, 0, 0), (x_out, yb, 0, 0)),
              ((x_qkv, xb, 1, 0), (x_proj, xb, 2, 0), (dy_qkv, yb, 1, 0), (dy_proj, yb, 1, cut)),
              ((x_inter, xb, 3, 0), (dy_inter, yb, 2, 0)))
    for m, group in enumerate(groups):
        def start(k, _, m=m, group=group):
            at = pl.ds(pl.multiple_of(k * step, step), step)
            for src, dst, slab, col in group:
                to = dst.at[slab, at] if src.shape[1] == dst.shape[2] else dst.at[slab, at, pl.ds(col, src.shape[1])]
                sem = in2_sem.at[k] if slab == 2 and dst is xb else in_sem.at[m * CHUNKS + k]
                pltpu.make_async_copy(src.at[at], to, sem).start()
            return 0

        lax.fori_loop(0, CHUNKS, start, 0)

    barrier = pltpu.get_barrier_semaphore()
    stat2[...] = jnp.zeros(stat2.shape, F32)

    def hello(i, _):
        pl.semaphore_signal(barrier, inc=1, device_id=((me + i) % ndev,), device_id_type=pl.DeviceIdType.MESH)
        return 0

    lax.fori_loop(1, ndev, hello, 0)

    def remote(src, dst, s_sem, r_sem, dev):
        return pltpu.make_async_remote_copy(src_ref=src, dst_ref=dst, send_sem=s_sem, recv_sem=r_sem,
                                            device_id=(dev,), device_id_type=pl.DeviceIdType.MESH)

    ones = jnp.ones((16, step), BF16)
    acc[...] = jnp.zeros(acc.shape, F32)
    bias_out[...] = jnp.zeros(bias_out.shape, F32)

    def products(i, _):
        m, k = i // CHUNKS, i % CHUNKS
        both = yb.at[0, pl.ds(0, step * 5 // 4)]
        pltpu.make_async_copy(both, both, in_sem.at[i]).wait()

        @pl.when(m == 1)
        def _():
            half = xb.at[2, pl.ds(0, step)]
            pltpu.make_async_copy(half, half, in2_sem.at[k]).wait()

        at = pl.ds(pl.multiple_of(k * step, step), step)
        lhs1 = jnp.concatenate([xb[m + m // 2, at, :].T, ones], axis=0)
        acc[m, :, 0:cut] += jnp.dot(lhs1, yb[m, at, 0:cut], preferred_element_type=F32)
        lhs2 = jnp.concatenate([xb[2 * m - m // 2, at, :].T, ones], axis=0)
        acc[m, :, cut:wide] += jnp.dot(lhs2, yb[m, at, cut:wide], preferred_element_type=F32)

        @pl.when(m == 0)
        def _():
            bias_out[...] += jnp.dot(ones, xb[0, at, :], preferred_element_type=F32)

        for at_i, fn in services.items():
            pl.when(i == at_i)(fn)
        return 0

    def spread(base, m, lo, n):
        cols = n // LANES
        for j in range(cols):
            at = slice(lo + j * LANES, lo + (j + 1) * LANES)
            gflat[pl.ds(base + j, width, stride=cols), :] = acc[m, 0:width, at]
            gflat[pl.ds(base + cols * width + j, 1), :] = acc[m, width:width + 1, at]

    def spread_out():
        cols = width // LANES
        for j in range(cols):
            at = slice(j * LANES, (j + 1) * LANES)
            gflat[pl.ds(ends[7] + j, wide, stride=cols), :] = acc[0, at, :].T
            gflat[pl.ds(ends[8] + j, 1), :] = bias_out[0:1, at]
        small[0].wait()
        for r, start in enumerate((ends[3], ends[4], ends[9], ends[10])):
            for j in range(cols):
                gflat[pl.ds(start + j, 1), :] = ln_v[r:r + 1, j * LANES:(j + 1) * LANES]
        gflat[pl.ds(ends[11], rows - ends[11]), :] = jnp.zeros((rows - ends[11], LANES), F32)

    def send_d(g):
        for i, q in enumerate((slot(1 - first, 1 - second), slot(first, 1 - second),
                               slot(1 - first, second), slot(first, second))):
            s = g * 8 + q * 2 + 1 - core
            remote(gflat.at[pl.ds(s * shard, shard)], r_d.at[g * 4 + q, pl.ds(0, shard)],
                   sd_s, sd_r.at[g, i // 2], partner).start()

    def copy_1(g, b):
        return remote(r_d.at[g * 4 + slot(1 - first, b), pl.ds(0, shard)], r_1.at[g * 2 + b, pl.ds(0, shard)],
                      s1_s, s1_r.at[g * 2 + b], peer1)

    def copy_2(g):
        return remote(r_1.at[g * 2 + 1 - second, pl.ds(0, shard)], r_2.at[g, pl.ds(0, shard)],
                      s2_s, s2_r.at[g], peer2)

    def add_d(a, b, g):
        q = slot(a, b)
        i = g * 4 + q
        r_d[i, 0:shard, :] += gflat[pl.ds((g * 8 + q * 2 + core) * shard, shard), :]

    def d_to_1(g):
        two = gflat.at[pl.ds(0, 2 * shard)]
        pltpu.make_async_copy(two, two, sd_r.at[g, 0]).wait()
        for b in (1 - second, second):
            add_d(1 - first, b, g)
            copy_1(g, b).start()
        pltpu.make_async_copy(two, two, sd_r.at[g, 1]).wait()
        for b in range(2):
            add_d(first, b, g)

    def one_to_2(g):
        for b in (1 - second, second):
            i = g * 2 + b
            remote(r_d.at[0, pl.ds(0, shard)], r_1.at[i, pl.ds(0, shard)], s1_s, s1_r.at[i], peer1).wait_recv()
            r_1[i, 0:shard, :] += r_d[g * 4 + slot(first, b), 0:shard, :]
            if b is not second:
                copy_2(g).start()

    def two_to_z(g):
        copy_2(g).wait_recv()
        r_2[g, 0:shard, :] += r_1[g * 2 + second, 0:shard, :]

        @pl.when(zz != g)
        def _():
            remote(r_2.at[g, pl.ds(0, shard)], r_z.at[zz, pl.ds(0, shard)], sz_s, sz_r.at[zz],
                   me + (g - zz) * 8).start()

    def after_out():
        scoped('spread_out', spread_out)
        scoped('barrier', pl.semaphore_wait, barrier, ndev - 1)
        send_d(3)

    def after_qkv():
        scoped('spread_qkv', spread, 0, 1, 0, cut)
        scoped('spread_proj', spread, ends[1], 1, cut, width)
        send_d(0)

    services = {CHUNKS - 1: after_out,
                CHUNKS: lambda: scoped('in_d1_3', d_to_1, 3),
                2 * CHUNKS - 1: after_qkv,
                2 * CHUNKS: lambda: scoped('in_d1_0', d_to_1, 0)}
    scoped('products', lax.fori_loop, 0, 3 * CHUNKS, products, 0)
    scoped('spread_inter', spread, ends[5], 2, 0, wide)
    scoped('send_d_1', send_d, 1)
    scoped('send_d_2', send_d, 2)
    scoped('one_to_2_3', one_to_2, 3)
    scoped('d_to_1_1', d_to_1, 1)
    scoped('d_to_1_2', d_to_1, 2)
    scoped('one_to_2_0', one_to_2, 0)
    scoped('two_to_z_3', two_to_z, 3)
    scoped('one_to_2_1', one_to_2, 1)
    scoped('two_to_z_0', two_to_z, 0)
    scoped('one_to_2_2', one_to_2, 2)
    scoped('two_to_z_1', two_to_z, 1)
    scoped('two_to_z_2', two_to_z, 2)

    for copy in small[1:]:
        scoped('wait_state', copy.wait)
    lane = lax.broadcasted_iota(jnp.int32, (shard, LANES), 1)
    row = lax.broadcasted_iota(jnp.int32, (shard, LANES), 0) + me * shard
    seg = jnp.zeros((shard, LANES), jnp.int32)
    for end in ends:
        seg = seg + jnp.where(row >= end, 1, 0)
    mine = lane == seg
    w = w_v[...]

    def seg_sums(val):
        per_row = jnp.sum(val, axis=1, keepdims=True)
        return jnp.sum(jnp.where(mine, per_row, 0.0), axis=0, keepdims=True)

    w_sums = seg_sums(w * w)

    g = r_2[zz, 0:shard, :]
    for d in range(1, PARTS):
        src = (zz + d) % PARTS
        scoped('wait_z', remote(r_2.at[0, pl.ds(0, shard)], r_z.at[src, pl.ds(0, shard)], sz_s, sz_r.at[src], me).wait_recv)
        g = g + r_z[src, 0:shard, :]
    g = g * (1.0 / ndev)

    def put(stat, value, s_sem, r_sem, lo, hi):
        stat[pl.ds(me, 1), :] = value

        def send(i, _):
            remote(stat.at[pl.ds(me, 1)], stat.at[pl.ds(me, 1)], s_sem, r_sem, (me + i) % ndev).start()
            return 0

        lax.fori_loop(lo, hi, send, 0)

    def rows_in(stat, count, sem):
        return pltpu.make_async_copy(stat.at[pl.ds(0, count)], stat.at[pl.ds(0, count)], sem)

    one_lane = lax.broadcasted_iota(jnp.int32, (1, LANES), 1)
    g_sq = jnp.sum(jnp.sum(g * g, axis=0, keepdims=True), axis=1, keepdims=True)
    put(stat1, jnp.where(one_lane == 64, g_sq, w_sums), t1_s, t1_r, 1, ndev)
    scoped('wait_stat1', rows_in(stat1, ndev - 1, t1_r).wait)
    total1 = jnp.sum(stat1[...], axis=0, keepdims=True)
    gn = jnp.sqrt(jnp.sum(jnp.where(one_lane == 64, total1, 0.0), axis=1, keepdims=True))
    h = g / jnp.maximum(1.0, gn)
    new_m = BETA_ONE * m_v[...] + (1.0 - BETA_ONE) * h
    new_v = BETA_TWO * v_v[...] + (1.0 - BETA_TWO) * h * h
    decay = jnp.where((seg == 0) | (seg == 2) | (seg == 6) | (seg == 8), DECAY, 0.0)
    u = (new_m / CORR_ONE) / (jnp.sqrt(new_v / CORR_TWO) + EPSILON) + decay * w
    plane = ndev // PARTS
    starts = [0] + ends[:-1]
    assert all((end - 1) // (plane * shard) - start // (plane * shard) <= 1 for start, end in zip(starts, ends))
    stat2[pl.ds(me, 1), :] = seg_sums(u * u)

    def send2(i, _, d):
        to = zz * plane + i

        @pl.when((to >= 0) & (to < ndev) & (to != me))
        def _():
            remote(stat2.at[pl.ds(me, 1)], stat2.at[pl.ds(me, 1)], t2_s.at[d + 1], t2_r.at[zz], to).start()

        return 0

    for d in (-1, 1, 0):
        lax.fori_loop(d * plane, (d + 1) * plane, functools.partial(send2, d=d), 0)

    def each_plane(fn):
        fn(1, zz, plane - 1)
        pl.when(zz > 0)(lambda: fn(0, zz - 1, plane))
        pl.when(zz < PARTS - 1)(lambda: fn(2, zz + 1, plane))

    scoped('wait_stat2', each_plane, lambda d, src, count: rows_in(stat2, count, t2_r.at[src]).wait())
    total2 = jnp.sum(stat2[...], axis=0, keepdims=True)
    nm_out[...] = new_m
    nv_out[...] = new_v
    w_norm, u_norm = jnp.sqrt(total1), jnp.sqrt(total2)
    ratio = jnp.where((w_norm > 0) & (u_norm > 0), w_norm / jnp.where(u_norm > 0, u_norm, 1.0), 1.0)
    per_row = jnp.sum(jnp.where(mine, ratio, 0.0), axis=1, keepdims=True)
    new_w = w - LEARN_RATE * per_row * u
    nw_out[...] = new_w
    wfull[pl.ds(me * shard, shard), :] = new_w
    late = shard // 5 + 1
    split = (shard - late + 1) // 2
    parts = ((0, split), (split, shard - late - split), (shard - late, late))

    def part_at(s, h):
        return wfull.at[pl.ds(s * shard + parts[h][0], parts[h][1])]

    sent = []

    def push(s, h, *devs):
        for dev in devs:
            sem = agp_r if dev is partner else ag_r.at[s // 2, h]
            remote(part_at(s, h), part_at(s, h), ag_s, sem, dev).start()
            sent.append(parts[h][1])

    def arrived(s, h):
        remote(part_at(s, h), part_at(s, h), ag_s, ag_r.at[s // 2, h], me).wait_recv()

    zs = [zz, zz + 1 - 2 * (zz % 2), 2 - zz // 2, 3 - 3 * (zz // 2)]
    inner = (zz == 1) | (zz == 2)
    diag = peer1 + peer2 - me

    def shifted(s, j):
        return s + (zs[j] - zz) * 8

    push(me, 2, peer2, peer1)
    for h in range(2):
        push(me, h, shifted(me, 1), peer2, peer1)
    for h in range(2):
        push(me, h, shifted(me, 2), partner)
    push(me, 2, partner)

    passed = []

    def relay(base, j, h):
        passed.append(parts[h][1])

        @pl.when(inner)
        def _():
            s = shifted(base, j)
            scoped('relay_%d%d' % (j, h), arrived, s, h)
            remote(part_at(s, h), part_at(s, h), agz_s, ag_r.at[s // 2, h], shifted(me, 1)).start()

    def got(base, j, h, name, relayed=False):
        s = shifted(base, j)
        if relayed:
            pl.when(jnp.logical_not(inner))(lambda: scoped('got_%s%d%d' % (name, j, h), arrived, s, h))
        else:
            scoped('got_%s%d%d' % (name, j, h), arrived, s, h)
        return s

    column = (me, peer1, peer2, diag)
    for h in range(2):
        relay(me, 2, h)
    push(got(peer1, 0, 2, 'a'), 2, peer2, partner)
    for h in range(2):
        push(got(peer1, 0, h, 'a'), h, peer2, partner)
    for j in (1, 2):
        for h in range(2):
            push(got(me, j, h, 'z', j > 1), h, peer2, peer1, partner)
    for h in range(2):
        relay(me, 3, h)
    for base in (peer2, diag):
        push(got(base, 0, 2, 'b'), 2, partner)
    for base in column:
        for j in (1, 2):
            push(base, 2, shifted(me, j))
    for h in range(2):
        push(got(peer1, 1, h, 'a'), h, peer2, partner)
    for h in range(2):
        push(got(me, 3, h, 'z', True), h, peer2, peer1, partner)
    for j in (2, 3):
        for h in range(2):
            push(got(peer1, j, h, 'a'), h, peer2, partner)
            for base in column[2 * h:2 * h + 2]:
                relay(base, j, 2)
    for j in range(1, PARTS):
        for base in column:
            push(got(base, j, 2, 'c', j > 1), 2, partner)
    for j in range(PARTS):
        for base, name in ((peer2, 'b'), (diag, 'd')):
            for h in range(2):
                push(got(base, j, h, name), h, partner)

    theirs = wfull.at[pl.ds(0, ndev // 2 * shard)]
    scoped('got_rest', pltpu.make_async_copy(theirs, theirs, agp_r).wait)
    par_out[...] = wfull[...].astype(BF16)

    def all_sent(buf, count, sem):
        pltpu.make_async_copy(buf.at[pl.ds(0, count)], buf.at[pl.ds(0, count)], sem).wait()

    scoped('all_sent_gflat', all_sent, gflat, 16 * shard, sd_s)
    scoped('all_sent_gflat', all_sent, gflat, 8 * shard, s1_s)
    scoped('all_sent_gflat', all_sent, gflat, 4 * shard, s2_s)
    scoped('all_sent_gflat', all_sent, gflat, 3 * shard, sz_s)
    scoped('all_sent_stat1', all_sent, stat1, ndev - 1, t1_s)
    each_plane(lambda d, src, count: rows_in(stat2, count, t2_s.at[d]).wait())
    scoped('all_sent_wfull', all_sent, wfull, sum(sent), ag_s)
    pl.when(inner)(lambda: all_sent(wfull, sum(passed), agz_s))


def write_kernel(*refs):
    sem = refs[-1]
    half = len(refs) // 2
    copies = [pltpu.make_async_copy(src, dst, sem.at[i]) for i, (src, dst) in enumerate(zip(refs[:half], refs[half:-1]))]
    for copy in reversed(copies):
        copy.start()
    for copy in copies:
        copy.wait()


def solution(mesh):
    ndev = mesh.shape['dp']

    def local_step(weights, moment_one, moment_two, x_qkv, dy_qkv, x_proj, dy_proj, x_inter, dy_inter, x_out, dy_out, ln_grad):
        tokens, width = x_qkv.shape
        shard = weights.shape[0] // LANES
        rows = shard * ndev
        flat = lambda a: a.reshape(-1, LANES)
        acts = (x_qkv, dy_qkv, x_proj, dy_proj, x_inter, dy_inter, x_out, dy_out)
        vm = pltpu.VMEM
        pad = -(-shard // 8) * 8
        state = jax.ShapeDtypeStruct((shard, LANES), F32)
        mid = (vm((shard, LANES), F32),) * 3 + (vm((rows, LANES), BF16),)
        dma = pltpu.SemaphoreType.DMA
        hbm = pl.BlockSpec(memory_space=pltpu.HBM)
        whole = pl.BlockSpec(memory_space=pltpu.VMEM)
        out_shape = (state, state, state, jax.ShapeDtypeStruct((rows, LANES), BF16))
        outs = pl.pallas_call(
            functools.partial(comm_kernel, (width, shard, ndev, rows)),
            out_shape=mid,
            in_specs=[hbm] * 12,
            out_specs=(whole,) * 4,
            scratch_shapes=[
                vm((4, tokens, width), BF16), vm((3, tokens, 4 * width), BF16), vm((4, width), F32)] + [
                vm((shard, LANES), F32)] * 3 + [
                vm((3, width + 16, 4 * width), F32), vm((16, width), F32), vm((rows, LANES), F32),
                vm((16, pad, LANES), F32), vm((8, pad, LANES), F32), vm((4, pad, LANES), F32), vm((4, pad, LANES), F32),
                vm((ndev, LANES), F32), vm((ndev, LANES), F32), vm((rows, LANES), F32),
                dma((3 * CHUNKS,)), dma((CHUNKS,)), dma((4,)), dma, dma((4, 2)), dma, dma((8,)), dma, dma((4,)), dma, dma((4,)),
                dma, dma, dma((3,)), dma((PARTS,)), dma, dma((ndev // 2, 3)), dma, dma],
            compiler_params=pltpu.CompilerParams(collective_id=0, has_side_effects=True, vmem_limit_bytes=61 * 2 ** 20),
            name='lamb_step',
        )(*acts, ln_grad.reshape(4, width), flat(weights), flat(moment_one), flat(moment_two))
        new_w, new_m, new_v, params = pl.pallas_call(
            write_kernel, out_shape=out_shape, in_specs=[whole] * 4, out_specs=(hbm,) * 4,
            scratch_shapes=[dma((4,))], name='write_out')(*[pltpu.with_memory_space_constraint(a, pltpu.VMEM) for a in outs])
        return new_w.reshape(-1), new_m.reshape(-1), new_v.reshape(-1), params.reshape(-1)

    row_spec = P('dp', None)
    in_specs = (P('dp'), P('dp'), P('dp'), row_spec, row_spec, row_spec, row_spec, row_spec, row_spec, row_spec, row_spec, P('dp', None, None))
    out_specs = (P('dp'), P('dp'), P('dp'), P())
    return jax.shard_map(local_step, mesh=mesh, in_specs=in_specs, out_specs=out_specs, check_vma=False)
```

```python
import functools

import jax
import jax.numpy as jnp
from jax import lax
from jax.experimental import pallas as pl
from jax.experimental.pallas import tpu as pltpu
from jax.sharding import PartitionSpec as P

STEP = 10
LEARN_RATE = 0.5
BETA_ONE = 0.9
BETA_TWO = 0.999
EPSILON = 1e-6
DECAY = 0.01
CORR_ONE = 1.0 - BETA_ONE ** STEP
CORR_TWO = 1.0 - BETA_TWO ** STEP

LANES = 128
CHUNKS = 2
PARTS = 4
F32 = jnp.float32
BF16 = jnp.bfloat16


def tensor_sizes(width):
    return [3 * width * width, 3 * width, width * width, width, width, width,
            4 * width * width, 4 * width, 4 * width * width, width, width, width]


def row_ends(width):
    ends, total = [], 0
    for size in tensor_sizes(width):
        total += size // LANES
        ends.append(total)
    return ends


def scoped(name, fn, *args):
    with jax.named_scope(name):
        return fn(*args)


def comm_kernel(dims, x_qkv, dy_qkv, x_proj, dy_proj, x_inter, dy_inter, x_out, dy_out, ln, w_in, m_in, v_in,
                nw_out, nm_out, nv_out, par_out,
                xb, yb, ln_v, w_v, m_v, v_v, acc, bias_out, gflat, r_d, r_1, r_2, r_z, stat1, stat2, wfull,
                in_sem, in2_sem, st_sem, sd_s, sd_r, s1_s, s1_r, s2_s, s2_r, sz_s, sz_r,
                t1_s, t1_r, t2_s, t2_r, ag_s, ag_r, agp_r, agz_s):
    width, shard, ndev, rows = dims
    tokens = x_qkv.shape[0]
    step = tokens // CHUNKS
    ends = row_ends(width)
    me = lax.axis_index('dp')
    core, xx, yy, zz = me % 2, (me // 2) % 2, (me // 4) % 2, me // 8
    partner = me + 1 - 2 * core
    first = xx * (1 - core) + yy * core
    second = yy * (1 - core) + xx * core
    peer1 = me + (1 - 2 * first) * (2 * (1 - core) + 4 * core)
    peer2 = me + (1 - 2 * second) * (4 * (1 - core) + 2 * core)

    def slot(a, b):
        return (1 - core) * (2 * b + a) + core * (2 * a + b)

    small = [pltpu.make_async_copy(s, d, st_sem.at[i])
             for i, (s, d) in enumerate(((ln, ln_v), (w_in, w_v), (m_in, m_v), (v_in, v_v)))]
    for copy in small:
        copy.start()
    wide = 4 * width
    cut = 3 * width
    groups = (((dy_out, xb, 0, 0), (x_out, yb, 0, 0)),
              ((x_qkv, xb, 1, 0), (x_proj, xb, 2, 0), (dy_qkv, yb, 1, 0), (dy_proj, yb, 1, cut)),
              ((x_inter, xb, 3, 0), (dy_inter, yb, 2, 0)))
    for m, group in enumerate(groups):
        def start(k, _, m=m, group=group):
            at = pl.ds(pl.multiple_of(k * step, step), step)
            for src, dst, slab, col in group:
                to = dst.at[slab, at] if src.shape[1] == dst.shape[2] else dst.at[slab, at, pl.ds(col, src.shape[1])]
                sem = in2_sem.at[k] if slab == 2 and dst is xb else in_sem.at[m * CHUNKS + k]
                pltpu.make_async_copy(src.at[at], to, sem).start()
            return 0

        lax.fori_loop(0, CHUNKS, start, 0)

    barrier = pltpu.get_barrier_semaphore()
    stat2[...] = jnp.zeros(stat2.shape, F32)

    def hello(i, _):
        pl.semaphore_signal(barrier, inc=1, device_id=((me + i) % ndev,), device_id_type=pl.DeviceIdType.MESH)
        return 0

    lax.fori_loop(1, ndev, hello, 0)

    def remote(src, dst, s_sem, r_sem, dev):
        return pltpu.make_async_remote_copy(src_ref=src, dst_ref=dst, send_sem=s_sem, recv_sem=r_sem,
                                            device_id=(dev,), device_id_type=pl.DeviceIdType.MESH)

    ones = jnp.ones((16, step), BF16)
    acc[...] = jnp.zeros(acc.shape, F32)
    bias_out[...] = jnp.zeros(bias_out.shape, F32)

    def products(i, _):
        m, k = i // CHUNKS, i % CHUNKS
        both = yb.at[0, pl.ds(0, step * 5 // 4)]
        pltpu.make_async_copy(both, both, in_sem.at[i]).wait()

        @pl.when(m == 1)
        def _():
            half = xb.at[2, pl.ds(0, step)]
            pltpu.make_async_copy(half, half, in2_sem.at[k]).wait()

        at = pl.ds(pl.multiple_of(k * step, step), step)
        lhs1 = jnp.concatenate([xb[m + m // 2, at, :].T, ones], axis=0)
        acc[m, :, 0:cut] += jnp.dot(lhs1, yb[m, at, 0:cut], preferred_element_type=F32)
        lhs2 = jnp.concatenate([xb[2 * m - m // 2, at, :].T, ones], axis=0)
        acc[m, :, cut:wide] += jnp.dot(lhs2, yb[m, at, cut:wide], preferred_element_type=F32)

        @pl.when(m == 0)
        def _():
            bias_out[...] += jnp.dot(ones, xb[0, at, :], preferred_element_type=F32)

        for at_i, fn in services.items():
            pl.when(i == at_i)(fn)
        return 0

    def spread(base, m, lo, n):
        cols = n // LANES
        for j in range(cols):
            at = slice(lo + j * LANES, lo + (j + 1) * LANES)
            gflat[pl.ds(base + j, width, stride=cols), :] = acc[m, 0:width, at]
            gflat[pl.ds(base + cols * width + j, 1), :] = acc[m, width:width + 1, at]

    def spread_out():
        cols = width // LANES
        for j in range(cols):
            at = slice(j * LANES, (j + 1) * LANES)
            gflat[pl.ds(ends[7] + j, wide, stride=cols), :] = acc[0, at, :].T
            gflat[pl.ds(ends[8] + j, 1), :] = bias_out[0:1, at]
        small[0].wait()
        for r, start in enumerate((ends[3], ends[4], ends[9], ends[10])):
            for j in range(cols):
                gflat[pl.ds(start + j, 1), :] = ln_v[r:r + 1, j * LANES:(j + 1) * LANES]
        gflat[pl.ds(ends[11], rows - ends[11]), :] = jnp.zeros((rows - ends[11], LANES), F32)

    def send_d(g):
        for i, q in enumerate((slot(1 - first, 1 - second), slot(first, 1 - second),
                               slot(1 - first, second), slot(first, second))):
            s = g * 8 + q * 2 + 1 - core
            remote(gflat.at[pl.ds(s * shard, shard)], r_d.at[g * 4 + q, pl.ds(0, shard)],
                   sd_s, sd_r.at[g, i // 2], partner).start()

    def copy_1(g, b):
        return remote(r_d.at[g * 4 + slot(1 - first, b), pl.ds(0, shard)], r_1.at[g * 2 + b, pl.ds(0, shard)],
                      s1_s, s1_r.at[g * 2 + b], peer1)

    def copy_2(g):
        return remote(r_1.at[g * 2 + 1 - second, pl.ds(0, shard)], r_2.at[g, pl.ds(0, shard)],
                      s2_s, s2_r.at[g], peer2)

    def add_d(a, b, g):
        q = slot(a, b)
        i = g * 4 + q
        r_d[i, 0:shard, :] += gflat[pl.ds((g * 8 + q * 2 + core) * shard, shard), :]

    def d_to_1(g):
        two = gflat.at[pl.ds(0, 2 * shard)]
        pltpu.make_async_copy(two, two, sd_r.at[g, 0]).wait()
        for b in (1 - second, second):
            add_d(1 - first, b, g)
            copy_1(g, b).start()
        pltpu.make_async_copy(two, two, sd_r.at[g, 1]).wait()
        for b in range(2):
            add_d(first, b, g)

    def one_to_2(g):
        for b in (1 - second, second):
            i = g * 2 + b
            remote(r_d.at[0, pl.ds(0, shard)], r_1.at[i, pl.ds(0, shard)], s1_s, s1_r.at[i], peer1).wait_recv()
            r_1[i, 0:shard, :] += r_d[g * 4 + slot(first, b), 0:shard, :]
            if b is not second:
                copy_2(g).start()

    def two_to_z(g):
        copy_2(g).wait_recv()
        r_2[g, 0:shard, :] += r_1[g * 2 + second, 0:shard, :]

        @pl.when(zz != g)
        def _():
            remote(r_2.at[g, pl.ds(0, shard)], r_z.at[zz, pl.ds(0, shard)], sz_s, sz_r.at[zz],
                   me + (g - zz) * 8).start()

    def after_out():
        scoped('spread_out', spread_out)
        scoped('barrier', pl.semaphore_wait, barrier, ndev - 1)
        send_d(3)

    def after_qkv():
        scoped('spread_qkv', spread, 0, 1, 0, cut)
        scoped('spread_proj', spread, ends[1], 1, cut, width)
        send_d(0)

    services = {CHUNKS - 1: after_out,
                CHUNKS: lambda: scoped('in_d1_3', d_to_1, 3),
                2 * CHUNKS - 1: after_qkv,
                2 * CHUNKS: lambda: scoped('in_d1_0', d_to_1, 0)}
    scoped('products', lax.fori_loop, 0, 3 * CHUNKS, products, 0)
    scoped('spread_inter', spread, ends[5], 2, 0, wide)
    scoped('send_d_1', send_d, 1)
    scoped('send_d_2', send_d, 2)
    scoped('one_to_2_3', one_to_2, 3)
    scoped('d_to_1_1', d_to_1, 1)
    scoped('d_to_1_2', d_to_1, 2)
    scoped('one_to_2_0', one_to_2, 0)
    scoped('two_to_z_3', two_to_z, 3)
    scoped('one_to_2_1', one_to_2, 1)
    scoped('two_to_z_0', two_to_z, 0)
    scoped('one_to_2_2', one_to_2, 2)
    scoped('two_to_z_1', two_to_z, 1)
    scoped('two_to_z_2', two_to_z, 2)

    for copy in small[1:]:
        scoped('wait_state', copy.wait)
    lane = lax.broadcasted_iota(jnp.int32, (shard, LANES), 1)
    row = lax.broadcasted_iota(jnp.int32, (shard, LANES), 0) + me * shard
    seg = jnp.zeros((shard, LANES), jnp.int32)
    for end in ends:
        seg = seg + jnp.where(row >= end, 1, 0)
    mine = lane == seg
    w = w_v[...]

    def seg_sums(val):
        per_row = jnp.sum(val, axis=1, keepdims=True)
        return jnp.sum(jnp.where(mine, per_row, 0.0), axis=0, keepdims=True)

    w_sums = seg_sums(w * w)

    g = r_2[zz, 0:shard, :]
    for d in range(1, PARTS):
        src = (zz + d) % PARTS
        scoped('wait_z', remote(r_2.at[0, pl.ds(0, shard)], r_z.at[src, pl.ds(0, shard)], sz_s, sz_r.at[src], me).wait_recv)
        g = g + r_z[src, 0:shard, :]
    g = g * (1.0 / ndev)

    def put(stat, value, s_sem, r_sem, lo, hi):
        stat[pl.ds(me, 1), :] = value

        def send(i, _):
            remote(stat.at[pl.ds(me, 1)], stat.at[pl.ds(me, 1)], s_sem, r_sem, (me + i) % ndev).start()
            return 0

        lax.fori_loop(lo, hi, send, 0)

    def rows_in(stat, count, sem):
        return pltpu.make_async_copy(stat.at[pl.ds(0, count)], stat.at[pl.ds(0, count)], sem)

    one_lane = lax.broadcasted_iota(jnp.int32, (1, LANES), 1)
    g_sq = jnp.sum(jnp.sum(g * g, axis=0, keepdims=True), axis=1, keepdims=True)
    put(stat1, jnp.where(one_lane == 64, g_sq, w_sums), t1_s, t1_r, 1, ndev)
    scoped('wait_stat1', rows_in(stat1, ndev - 1, t1_r).wait)
    total1 = jnp.sum(stat1[...], axis=0, keepdims=True)
    gn = jnp.sqrt(jnp.sum(jnp.where(one_lane == 64, total1, 0.0), axis=1, keepdims=True))
    h = g / jnp.maximum(1.0, gn)
    new_m = BETA_ONE * m_v[...] + (1.0 - BETA_ONE) * h
    new_v = BETA_TWO * v_v[...] + (1.0 - BETA_TWO) * h * h
    decay = jnp.where((seg == 0) | (seg == 2) | (seg == 6) | (seg == 8), DECAY, 0.0)
    u = (new_m / CORR_ONE) / (jnp.sqrt(new_v / CORR_TWO) + EPSILON) + decay * w
    plane = ndev // PARTS
    starts = [0] + ends[:-1]
    assert all((end - 1) // (plane * shard) - start // (plane * shard) <= 1 for start, end in zip(starts, ends))
    stat2[pl.ds(me, 1), :] = seg_sums(u * u)

    def send2(i, _, d):
        to = zz * plane + i

        @pl.when((to >= 0) & (to < ndev) & (to != me))
        def _():
            remote(stat2.at[pl.ds(me, 1)], stat2.at[pl.ds(me, 1)], t2_s.at[d + 1], t2_r.at[zz], to).start()

        return 0

    for d in (-1, 1, 0):
        lax.fori_loop(d * plane, (d + 1) * plane, functools.partial(send2, d=d), 0)

    def each_plane(fn):
        fn(1, zz, plane - 1)
        pl.when(zz > 0)(lambda: fn(0, zz - 1, plane))
        pl.when(zz < PARTS - 1)(lambda: fn(2, zz + 1, plane))

    scoped('wait_stat2', each_plane, lambda d, src, count: rows_in(stat2, count, t2_r.at[src]).wait())
    total2 = jnp.sum(stat2[...], axis=0, keepdims=True)
    nm_out[...] = new_m
    nv_out[...] = new_v
    w_norm, u_norm = jnp.sqrt(total1), jnp.sqrt(total2)
    ratio = jnp.where((w_norm > 0) & (u_norm > 0), w_norm / jnp.where(u_norm > 0, u_norm, 1.0), 1.0)
    per_row = jnp.sum(jnp.where(mine, ratio, 0.0), axis=1, keepdims=True)
    new_w = w - LEARN_RATE * per_row * u
    nw_out[...] = new_w
    wfull[pl.ds(me * shard, shard), :] = new_w
    late = shard // 5 + 1
    split = (shard - late + 1) // 2
    parts = ((0, split), (split, shard - late - split), (shard - late, late))

    def part_at(s, h):
        return wfull.at[pl.ds(s * shard + parts[h][0], parts[h][1])]

    sent = []

    def push(s, h, *devs):
        for dev in devs:
            sem = agp_r if dev is partner else ag_r.at[s // 2, h]
            remote(part_at(s, h), part_at(s, h), ag_s, sem, dev).start()
            sent.append(parts[h][1])

    def arrived(s, h):
        remote(part_at(s, h), part_at(s, h), ag_s, ag_r.at[s // 2, h], me).wait_recv()

    zs = [zz, zz + 1 - 2 * (zz % 2), 2 - zz // 2, 3 - 3 * (zz // 2)]
    inner = (zz == 1) | (zz == 2)
    diag = peer1 + peer2 - me

    def shifted(s, j):
        return s + (zs[j] - zz) * 8

    push(me, 2, peer2, peer1)
    for h in range(2):
        push(me, h, shifted(me, 1), peer2, peer1)
    for h in range(2):
        push(me, h, shifted(me, 2), partner)
    push(me, 2, partner)

    passed = []

    def relay(base, j, h):
        passed.append(parts[h][1])

        @pl.when(inner)
        def _():
            s = shifted(base, j)
            scoped('relay_%d%d' % (j, h), arrived, s, h)
            remote(part_at(s, h), part_at(s, h), agz_s, ag_r.at[s // 2, h], shifted(me, 1)).start()

    def got(base, j, h, name, relayed=False):
        s = shifted(base, j)
        if relayed:
            pl.when(jnp.logical_not(inner))(lambda: scoped('got_%s%d%d' % (name, j, h), arrived, s, h))
        else:
            scoped('got_%s%d%d' % (name, j, h), arrived, s, h)
        return s

    column = (me, peer1, peer2, diag)
    for h in range(2):
        relay(me, 2, h)
    push(got(peer1, 0, 2, 'a'), 2, peer2, partner)
    for h in range(2):
        push(got(peer1, 0, h, 'a'), h, peer2, partner)
    for j in (1, 2):
        for h in range(2):
            push(got(me, j, h, 'z', j > 1), h, peer2, peer1, partner)
    for h in range(2):
        relay(me, 3, h)
    for base in (peer2, diag):
        push(got(base, 0, 2, 'b'), 2, partner)
    for base in column:
        for j in (1, 2):
            push(base, 2, shifted(me, j))
    for h in range(2):
        push(got(peer1, 1, h, 'a'), h, peer2, partner)
    for h in range(2):
        push(got(me, 3, h, 'z', True), h, peer2, peer1, partner)
    for j in (2, 3):
        for base in column:
            relay(base, j, 2)
        for h in range(2):
            push(got(peer1, j, h, 'a'), h, peer2, partner)
    for j in range(1, PARTS):
        for base in column:
            push(got(base, j, 2, 'c', j > 1), 2, partner)
    for j in range(PARTS):
        for base, name in ((peer2, 'b'), (diag, 'd')):
            for h in range(2):
                push(got(base, j, h, name), h, partner)

    theirs = wfull.at[pl.ds(0, ndev // 2 * shard)]
    scoped('got_rest', pltpu.make_async_copy(theirs, theirs, agp_r).wait)
    par_out[...] = wfull[...].astype(BF16)

    def all_sent(buf, count, sem):
        pltpu.make_async_copy(buf.at[pl.ds(0, count)], buf.at[pl.ds(0, count)], sem).wait()

    scoped('all_sent_gflat', all_sent, gflat, 16 * shard, sd_s)
    scoped('all_sent_gflat', all_sent, gflat, 8 * shard, s1_s)
    scoped('all_sent_gflat', all_sent, gflat, 4 * shard, s2_s)
    scoped('all_sent_gflat', all_sent, gflat, 3 * shard, sz_s)
    scoped('all_sent_stat1', all_sent, stat1, ndev - 1, t1_s)
    each_plane(lambda d, src, count: rows_in(stat2, count, t2_s.at[d]).wait())
    scoped('all_sent_wfull', all_sent, wfull, sum(sent), ag_s)
    pl.when(inner)(lambda: all_sent(wfull, sum(passed), agz_s))


def write_kernel(*refs):
    sem = refs[-1]
    half = len(refs) // 2
    copies = [pltpu.make_async_copy(src, dst, sem.at[i]) for i, (src, dst) in enumerate(zip(refs[:half], refs[half:-1]))]
    for copy in reversed(copies):
        copy.start()
    for copy in copies:
        copy.wait()


def solution(mesh):
    ndev = mesh.shape['dp']

    def local_step(weights, moment_one, moment_two, x_qkv, dy_qkv, x_proj, dy_proj, x_inter, dy_inter, x_out, dy_out, ln_grad):
        tokens, width = x_qkv.shape
        shard = weights.shape[0] // LANES
        rows = shard * ndev
        flat = lambda a: a.reshape(-1, LANES)
        acts = (x_qkv, dy_qkv, x_proj, dy_proj, x_inter, dy_inter, x_out, dy_out)
        vm = pltpu.VMEM
        pad = -(-shard // 8) * 8
        state = jax.ShapeDtypeStruct((shard, LANES), F32)
        mid = (vm((shard, LANES), F32),) * 3 + (vm((rows, LANES), BF16),)
        dma = pltpu.SemaphoreType.DMA
        hbm = pl.BlockSpec(memory_space=pltpu.HBM)
        whole = pl.BlockSpec(memory_space=pltpu.VMEM)
        out_shape = (state, state, state, jax.ShapeDtypeStruct((rows, LANES), BF16))
        outs = pl.pallas_call(
            functools.partial(comm_kernel, (width, shard, ndev, rows)),
            out_shape=mid,
            in_specs=[hbm] * 12,
            out_specs=(whole,) * 4,
            scratch_shapes=[
                vm((4, tokens, width), BF16), vm((3, tokens, 4 * width), BF16), vm((4, width), F32)] + [
                vm((shard, LANES), F32)] * 3 + [
                vm((3, width + 16, 4 * width), F32), vm((16, width), F32), vm((rows, LANES), F32),
                vm((16, pad, LANES), F32), vm((8, pad, LANES), F32), vm((4, pad, LANES), F32), vm((4, pad, LANES), F32),
                vm((ndev, LANES), F32), vm((ndev, LANES), F32), vm((rows, LANES), F32),
                dma((3 * CHUNKS,)), dma((CHUNKS,)), dma((4,)), dma, dma((4, 2)), dma, dma((8,)), dma, dma((4,)), dma, dma((4,)),
                dma, dma, dma((3,)), dma((PARTS,)), dma, dma((ndev // 2, 3)), dma, dma],
            compiler_params=pltpu.CompilerParams(collective_id=0, has_side_effects=True, vmem_limit_bytes=61 * 2 ** 20),
            name='lamb_step',
        )(*acts, ln_grad.reshape(4, width), flat(weights), flat(moment_one), flat(moment_two))
        new_w, new_m, new_v, params = pl.pallas_call(
            write_kernel, out_shape=out_shape, in_specs=[whole] * 4, out_specs=(hbm,) * 4,
            scratch_shapes=[dma((4,))], name='write_out')(*[pltpu.with_memory_space_constraint(a, pltpu.VMEM) for a in outs])
        return new_w.reshape(-1), new_m.reshape(-1), new_v.reshape(-1), params.reshape(-1)

    row_spec = P('dp', None)
    in_specs = (P('dp'), P('dp'), P('dp'), row_spec, row_spec, row_spec, row_spec, row_spec, row_spec, row_spec, row_spec, P('dp', None, None))
    out_specs = (P('dp'), P('dp'), P('dp'), P())
    return jax.shard_map(local_step, mesh=mesh, in_specs=in_specs, out_specs=out_specs, check_vma=False)
```

```python
import functools

import jax
import jax.numpy as jnp
from jax import lax
from jax.experimental import pallas as pl
from jax.experimental.pallas import tpu as pltpu
from jax.sharding import PartitionSpec as P

STEP = 10
LEARN_RATE = 0.5
BETA_ONE = 0.9
BETA_TWO = 0.999
EPSILON = 1e-6
DECAY = 0.01
CORR_ONE = 1.0 - BETA_ONE ** STEP
CORR_TWO = 1.0 - BETA_TWO ** STEP

LANES = 128
CHUNKS = 2
PARTS = 4
F32 = jnp.float32
BF16 = jnp.bfloat16


def tensor_sizes(width):
    return [3 * width * width, 3 * width, width * width, width, width, width,
            4 * width * width, 4 * width, 4 * width * width, width, width, width]


def row_ends(width):
    ends, total = [], 0
    for size in tensor_sizes(width):
        total += size // LANES
        ends.append(total)
    return ends


def scoped(name, fn, *args):
    with jax.named_scope(name):
        return fn(*args)


def comm_kernel(dims, x_qkv, dy_qkv, x_proj, dy_proj, x_inter, dy_inter, x_out, dy_out, ln, w_in, m_in, v_in,
                nw_out, nm_out, nv_out, par_out,
                xb, yb, ln_v, w_v, m_v, v_v, acc, bias_out, gflat, r_d, r_1, r_2, r_z, stat1, stat2, wfull,
                in_sem, in2_sem, st_sem, sd_s, sd_r, s1_s, s1_r, s2_s, s2_r, sz_s, sz_r,
                t1_s, t1_r, t2_s, t2_r, ag_s, ag_r, agp_r, agz_s):
    width, shard, ndev, rows = dims
    tokens = x_qkv.shape[0]
    step = tokens // CHUNKS
    ends = row_ends(width)
    me = lax.axis_index('dp')
    core, xx, yy, zz = me % 2, (me // 2) % 2, (me // 4) % 2, me // 8
    partner = me + 1 - 2 * core
    first = xx * (1 - core) + yy * core
    second = yy * (1 - core) + xx * core
    peer1 = me + (1 - 2 * first) * (2 * (1 - core) + 4 * core)
    peer2 = me + (1 - 2 * second) * (4 * (1 - core) + 2 * core)

    def slot(a, b):
        return (1 - core) * (2 * b + a) + core * (2 * a + b)

    small = [pltpu.make_async_copy(s, d, st_sem.at[i])
             for i, (s, d) in enumerate(((ln, ln_v), (w_in, w_v), (m_in, m_v), (v_in, v_v)))]
    for copy in small:
        copy.start()
    wide = 4 * width
    cut = 3 * width
    groups = (((dy_out, xb, 0, 0), (x_out, yb, 0, 0)),
              ((x_qkv, xb, 1, 0), (x_proj, xb, 2, 0), (dy_qkv, yb, 1, 0), (dy_proj, yb, 1, cut)),
              ((x_inter, xb, 3, 0), (dy_inter, yb, 2, 0)))
    for m, group in enumerate(groups):
        def start(k, _, m=m, group=group):
            at = pl.ds(pl.multiple_of(k * step, step), step)
            for src, dst, slab, col in group:
                to = dst.at[slab, at] if src.shape[1] == dst.shape[2] else dst.at[slab, at, pl.ds(col, src.shape[1])]
                sem = in2_sem.at[k] if slab == 2 and dst is xb else in_sem.at[m * CHUNKS + k]
                pltpu.make_async_copy(src.at[at], to, sem).start()
            return 0

        lax.fori_loop(0, CHUNKS, start, 0)

    barrier = pltpu.get_barrier_semaphore()
    stat2[...] = jnp.zeros(stat2.shape, F32)

    def hello(i, _):
        pl.semaphore_signal(barrier, inc=1, device_id=((me + i) % ndev,), device_id_type=pl.DeviceIdType.MESH)
        return 0

    lax.fori_loop(1, ndev, hello, 0)

    def remote(src, dst, s_sem, r_sem, dev):
        return pltpu.make_async_remote_copy(src_ref=src, dst_ref=dst, send_sem=s_sem, recv_sem=r_sem,
                                            device_id=(dev,), device_id_type=pl.DeviceIdType.MESH)

    ones = jnp.ones((16, step), BF16)
    acc[...] = jnp.zeros(acc.shape, F32)
    bias_out[...] = jnp.zeros(bias_out.shape, F32)

    def products(i, _):
        m, k = i // CHUNKS, i % CHUNKS
        both = yb.at[0, pl.ds(0, step * 5 // 4)]
        pltpu.make_async_copy(both, both, in_sem.at[i]).wait()

        @pl.when(m == 1)
        def _():
            half = xb.at[2, pl.ds(0, step)]
            pltpu.make_async_copy(half, half, in2_sem.at[k]).wait()

        at = pl.ds(pl.multiple_of(k * step, step), step)
        lhs1 = jnp.concatenate([xb[m + m // 2, at, :].T, ones], axis=0)
        acc[m, :, 0:cut] += jnp.dot(lhs1, yb[m, at, 0:cut], preferred_element_type=F32)
        lhs2 = jnp.concatenate([xb[2 * m - m // 2, at, :].T, ones], axis=0)
        acc[m, :, cut:wide] += jnp.dot(lhs2, yb[m, at, cut:wide], preferred_element_type=F32)

        @pl.when(m == 0)
        def _():
            bias_out[...] += jnp.dot(ones, xb[0, at, :], preferred_element_type=F32)

        for at_i, fn in services.items():
            pl.when(i == at_i)(fn)
        return 0

    def spread(base, m, lo, n):
        cols = n // LANES
        for j in range(cols):
            at = slice(lo + j * LANES, lo + (j + 1) * LANES)
            gflat[pl.ds(base + j, width, stride=cols), :] = acc[m, 0:width, at]
            gflat[pl.ds(base + cols * width + j, 1), :] = acc[m, width:width + 1, at]

    def spread_out():
        cols = width // LANES
        for j in range(cols):
            at = slice(j * LANES, (j + 1) * LANES)
            gflat[pl.ds(ends[7] + j, wide, stride=cols), :] = acc[0, at, :].T
            gflat[pl.ds(ends[8] + j, 1), :] = bias_out[0:1, at]
        small[0].wait()
        for r, start in enumerate((ends[3], ends[4], ends[9], ends[10])):
            for j in range(cols):
                gflat[pl.ds(start + j, 1), :] = ln_v[r:r + 1, j * LANES:(j + 1) * LANES]
        gflat[pl.ds(ends[11], rows - ends[11]), :] = jnp.zeros((rows - ends[11], LANES), F32)

    def send_d(g):
        for q in range(4):
            s = g * 8 + q * 2 + 1 - core
            remote(gflat.at[pl.ds(s * shard, shard)], r_d.at[g * 4 + q, pl.ds(0, shard)],
                   sd_s, sd_r.at[g], partner).start()

    def copy_1(g, b):
        return remote(r_d.at[g * 4 + slot(1 - first, b), pl.ds(0, shard)], r_1.at[g * 2 + b, pl.ds(0, shard)],
                      s1_s, s1_r.at[g * 2 + b], peer1)

    def copy_2(g):
        return remote(r_1.at[g * 2 + 1 - second, pl.ds(0, shard)], r_2.at[g, pl.ds(0, shard)],
                      s2_s, s2_r.at[g], peer2)

    def add_d(a, b, g):
        q = slot(a, b)
        i = g * 4 + q
        r_d[i, 0:shard, :] += gflat[pl.ds((g * 8 + q * 2 + core) * shard, shard), :]

    def d_to_1(g):
        four = gflat.at[pl.ds(0, 4 * shard)]
        pltpu.make_async_copy(four, four, sd_r.at[g]).wait()
        for b in (1 - second, second):
            add_d(1 - first, b, g)
            copy_1(g, b).start()
        for b in range(2):
            add_d(first, b, g)

    def one_to_2(g):
        for b in (1 - second, second):
            i = g * 2 + b
            remote(r_d.at[0, pl.ds(0, shard)], r_1.at[i, pl.ds(0, shard)], s1_s, s1_r.at[i], peer1).wait_recv()
            r_1[i, 0:shard, :] += r_d[g * 4 + slot(first, b), 0:shard, :]
            if b is not second:
                copy_2(g).start()

    def two_to_z(g):
        copy_2(g).wait_recv()
        r_2[g, 0:shard, :] += r_1[g * 2 + second, 0:shard, :]

        @pl.when(zz != g)
        def _():
            remote(r_2.at[g, pl.ds(0, shard)], r_z.at[zz, pl.ds(0, shard)], sz_s, sz_r.at[zz],
                   me + (g - zz) * 8).start()

    def after_out():
        scoped('spread_out', spread_out)
        scoped('barrier', pl.semaphore_wait, barrier, ndev - 1)
        send_d(3)

    def after_qkv():
        scoped('spread_qkv', spread, 0, 1, 0, cut)
        scoped('spread_proj', spread, ends[1], 1, cut, width)
        send_d(0)

    services = {CHUNKS - 1: after_out,
                CHUNKS: lambda: scoped('in_d1_3', d_to_1, 3),
                2 * CHUNKS - 1: after_qkv,
                2 * CHUNKS: lambda: scoped('in_d1_0', d_to_1, 0)}
    scoped('products', lax.fori_loop, 0, 3 * CHUNKS, products, 0)
    scoped('spread_inter', spread, ends[5], 2, 0, wide)
    scoped('send_d_1', send_d, 1)
    scoped('send_d_2', send_d, 2)
    scoped('one_to_2_3', one_to_2, 3)
    scoped('d_to_1_1', d_to_1, 1)
    scoped('d_to_1_2', d_to_1, 2)
    scoped('one_to_2_0', one_to_2, 0)
    scoped('two_to_z_3', two_to_z, 3)
    scoped('one_to_2_1', one_to_2, 1)
    scoped('two_to_z_0', two_to_z, 0)
    scoped('one_to_2_2', one_to_2, 2)
    scoped('two_to_z_1', two_to_z, 1)
    scoped('two_to_z_2', two_to_z, 2)

    for copy in small[1:]:
        scoped('wait_state', copy.wait)
    lane = lax.broadcasted_iota(jnp.int32, (shard, LANES), 1)
    row = lax.broadcasted_iota(jnp.int32, (shard, LANES), 0) + me * shard
    seg = jnp.zeros((shard, LANES), jnp.int32)
    for end in ends:
        seg = seg + jnp.where(row >= end, 1, 0)
    mine = lane == seg
    w = w_v[...]

    def seg_sums(val):
        per_row = jnp.sum(val, axis=1, keepdims=True)
        return jnp.sum(jnp.where(mine, per_row, 0.0), axis=0, keepdims=True)

    w_sums = seg_sums(w * w)

    g = r_2[zz, 0:shard, :]
    for d in range(1, PARTS):
        src = (zz + d) % PARTS
        scoped('wait_z', remote(r_2.at[0, pl.ds(0, shard)], r_z.at[src, pl.ds(0, shard)], sz_s, sz_r.at[src], me).wait_recv)
        g = g + r_z[src, 0:shard, :]
    g = g * (1.0 / ndev)

    def put(stat, value, s_sem, r_sem, lo, hi):
        stat[pl.ds(me, 1), :] = value

        def send(i, _):
            remote(stat.at[pl.ds(me, 1)], stat.at[pl.ds(me, 1)], s_sem, r_sem, (me + i) % ndev).start()
            return 0

        lax.fori_loop(lo, hi, send, 0)

    def rows_in(stat, count, sem):
        return pltpu.make_async_copy(stat.at[pl.ds(0, count)], stat.at[pl.ds(0, count)], sem)

    one_lane = lax.broadcasted_iota(jnp.int32, (1, LANES), 1)
    g_sq = jnp.sum(jnp.sum(g * g, axis=0, keepdims=True), axis=1, keepdims=True)
    put(stat1, jnp.where(one_lane == 64, g_sq, w_sums), t1_s, t1_r, 1, ndev)
    scoped('wait_stat1', rows_in(stat1, ndev - 1, t1_r).wait)
    total1 = jnp.sum(stat1[...], axis=0, keepdims=True)
    gn = jnp.sqrt(jnp.sum(jnp.where(one_lane == 64, total1, 0.0), axis=1, keepdims=True))
    h = g / jnp.maximum(1.0, gn)
    new_m = BETA_ONE * m_v[...] + (1.0 - BETA_ONE) * h
    new_v = BETA_TWO * v_v[...] + (1.0 - BETA_TWO) * h * h
    decay = jnp.where((seg == 0) | (seg == 2) | (seg == 6) | (seg == 8), DECAY, 0.0)
    u = (new_m / CORR_ONE) / (jnp.sqrt(new_v / CORR_TWO) + EPSILON) + decay * w
    plane = ndev // PARTS
    starts = [0] + ends[:-1]
    assert all((end - 1) // (plane * shard) - start // (plane * shard) <= 1 for start, end in zip(starts, ends))
    stat2[pl.ds(me, 1), :] = seg_sums(u * u)

    def send2(i, _, d):
        to = zz * plane + i

        @pl.when((to >= 0) & (to < ndev) & (to != me))
        def _():
            remote(stat2.at[pl.ds(me, 1)], stat2.at[pl.ds(me, 1)], t2_s.at[d + 1], t2_r.at[zz], to).start()

        return 0

    for d in (-1, 1, 0):
        lax.fori_loop(d * plane, (d + 1) * plane, functools.partial(send2, d=d), 0)

    def each_plane(fn):
        fn(1, zz, plane - 1)
        pl.when(zz > 0)(lambda: fn(0, zz - 1, plane))
        pl.when(zz < PARTS - 1)(lambda: fn(2, zz + 1, plane))

    scoped('wait_stat2', each_plane, lambda d, src, count: rows_in(stat2, count, t2_r.at[src]).wait())
    total2 = jnp.sum(stat2[...], axis=0, keepdims=True)
    nm_out[...] = new_m
    nv_out[...] = new_v
    w_norm, u_norm = jnp.sqrt(total1), jnp.sqrt(total2)
    ratio = jnp.where((w_norm > 0) & (u_norm > 0), w_norm / jnp.where(u_norm > 0, u_norm, 1.0), 1.0)
    per_row = jnp.sum(jnp.where(mine, ratio, 0.0), axis=1, keepdims=True)
    new_w = w - LEARN_RATE * per_row * u
    nw_out[...] = new_w
    wfull[pl.ds(me * shard, shard), :] = new_w
    late = shard // 5 + 1
    split = (shard - late + 1) // 2
    parts = ((0, split), (split, shard - late - split), (shard - late, late))

    def part_at(s, h):
        return wfull.at[pl.ds(s * shard + parts[h][0], parts[h][1])]

    sent = []

    def push(s, h, *devs):
        for dev in devs:
            sem = agp_r if dev is partner else ag_r.at[s // 2, h]
            remote(part_at(s, h), part_at(s, h), ag_s, sem, dev).start()
            sent.append(parts[h][1])

    def arrived(s, h):
        remote(part_at(s, h), part_at(s, h), ag_s, ag_r.at[s // 2, h], me).wait_recv()

    zs = [zz, zz + 1 - 2 * (zz % 2), 2 - zz // 2, 3 - 3 * (zz // 2)]
    inner = (zz == 1) | (zz == 2)
    diag = peer1 + peer2 - me

    def shifted(s, j):
        return s + (zs[j] - zz) * 8

    push(me, 2, peer2, peer1)
    for h in range(2):
        push(me, h, shifted(me, 1), peer2, peer1)
    for h in range(2):
        push(me, h, shifted(me, 2), partner)
    push(me, 2, partner)

    passed = []

    def relay(base, j, h):
        passed.append(parts[h][1])

        @pl.when(inner)
        def _():
            s = shifted(base, j)
            scoped('relay_%d%d' % (j, h), arrived, s, h)
            remote(part_at(s, h), part_at(s, h), agz_s, ag_r.at[s // 2, h], shifted(me, 1)).start()

    def got(base, j, h, name, relayed=False):
        s = shifted(base, j)
        if relayed:
            pl.when(jnp.logical_not(inner))(lambda: scoped('got_%s%d%d' % (name, j, h), arrived, s, h))
        else:
            scoped('got_%s%d%d' % (name, j, h), arrived, s, h)
        return s

    column = (me, peer1, peer2, diag)
    for h in range(2):
        relay(me, 2, h)
    push(got(peer1, 0, 2, 'a'), 2, peer2, partner)
    for h in range(2):
        push(got(peer1, 0, h, 'a'), h, peer2, partner)
    for j in (1, 2):
        for h in range(2):
            push(got(me, j, h, 'z', j > 1), h, peer2, peer1, partner)
    for h in range(2):
        relay(me, 3, h)
    for base in column[:2]:
        for j in (1, 2):
            push(base, 2, shifted(me, j))
    for base in column[2:]:
        push(got(base, 0, 2, 'b'), 2, shifted(me, 1), shifted(me, 2), partner)
    for h in range(2):
        push(got(peer1, 1, h, 'a'), h, peer2, partner)
    for h in range(2):
        push(got(me, 3, h, 'z', True), h, peer2, peer1, partner)
    for j in (2, 3):
        for base in column[:2]:
            relay(base, j, 2)
        for h in range(2):
            push(got(peer1, j, h, 'a'), h, peer2, partner)
        for base in column[2:]:
            relay(base, j, 2)
    for j in range(1, PARTS):
        for base in column:
            push(got(base, j, 2, 'c', j > 1), 2, partner)
    for j in range(PARTS):
        for base, name in ((peer2, 'b'), (diag, 'd')):
            for h in range(2):
                push(got(base, j, h, name), h, partner)

    theirs = wfull.at[pl.ds(0, ndev // 2 * shard)]
    scoped('got_rest', pltpu.make_async_copy(theirs, theirs, agp_r).wait)
    par_out[...] = wfull[...].astype(BF16)

    def all_sent(buf, count, sem):
        pltpu.make_async_copy(buf.at[pl.ds(0, count)], buf.at[pl.ds(0, count)], sem).wait()

    scoped('all_sent_gflat', all_sent, gflat, 16 * shard, sd_s)
    scoped('all_sent_gflat', all_sent, gflat, 8 * shard, s1_s)
    scoped('all_sent_gflat', all_sent, gflat, 4 * shard, s2_s)
    scoped('all_sent_gflat', all_sent, gflat, 3 * shard, sz_s)
    scoped('all_sent_stat1', all_sent, stat1, ndev - 1, t1_s)
    each_plane(lambda d, src, count: rows_in(stat2, count, t2_s.at[d]).wait())
    scoped('all_sent_wfull', all_sent, wfull, sum(sent), ag_s)
    pl.when(inner)(lambda: all_sent(wfull, sum(passed), agz_s))


def write_kernel(*refs):
    sem = refs[-1]
    half = len(refs) // 2
    copies = [pltpu.make_async_copy(src, dst, sem.at[i]) for i, (src, dst) in enumerate(zip(refs[:half], refs[half:-1]))]
    for copy in reversed(copies):
        copy.start()
    for copy in copies:
        copy.wait()


def solution(mesh):
    ndev = mesh.shape['dp']

    def local_step(weights, moment_one, moment_two, x_qkv, dy_qkv, x_proj, dy_proj, x_inter, dy_inter, x_out, dy_out, ln_grad):
        tokens, width = x_qkv.shape
        shard = weights.shape[0] // LANES
        rows = shard * ndev
        flat = lambda a: a.reshape(-1, LANES)
        acts = (x_qkv, dy_qkv, x_proj, dy_proj, x_inter, dy_inter, x_out, dy_out)
        vm = pltpu.VMEM
        pad = -(-shard // 8) * 8
        state = jax.ShapeDtypeStruct((shard, LANES), F32)
        mid = (vm((shard, LANES), F32),) * 3 + (vm((rows, LANES), BF16),)
        dma = pltpu.SemaphoreType.DMA
        hbm = pl.BlockSpec(memory_space=pltpu.HBM)
        whole = pl.BlockSpec(memory_space=pltpu.VMEM)
        out_shape = (state, state, state, jax.ShapeDtypeStruct((rows, LANES), BF16))
        outs = pl.pallas_call(
            functools.partial(comm_kernel, (width, shard, ndev, rows)),
            out_shape=mid,
            in_specs=[hbm] * 12,
            out_specs=(whole,) * 4,
            scratch_shapes=[
                vm((4, tokens, width), BF16), vm((3, tokens, 4 * width), BF16), vm((4, width), F32)] + [
                vm((shard, LANES), F32)] * 3 + [
                vm((3, width + 16, 4 * width), F32), vm((16, width), F32), vm((rows, LANES), F32),
                vm((16, pad, LANES), F32), vm((8, pad, LANES), F32), vm((4, pad, LANES), F32), vm((4, pad, LANES), F32),
                vm((ndev, LANES), F32), vm((ndev, LANES), F32), vm((rows, LANES), F32),
                dma((3 * CHUNKS,)), dma((CHUNKS,)), dma((4,)), dma, dma((4,)), dma, dma((8,)), dma, dma((4,)), dma, dma((4,)),
                dma, dma, dma((3,)), dma((PARTS,)), dma, dma((ndev // 2, 3)), dma, dma],
            compiler_params=pltpu.CompilerParams(collective_id=0, has_side_effects=True, vmem_limit_bytes=61 * 2 ** 20),
            name='lamb_step',
        )(*acts, ln_grad.reshape(4, width), flat(weights), flat(moment_one), flat(moment_two))
        new_w, new_m, new_v, params = pl.pallas_call(
            write_kernel, out_shape=out_shape, in_specs=[whole] * 4, out_specs=(hbm,) * 4,
            scratch_shapes=[dma((4,))], name='write_out')(*[pltpu.with_memory_space_constraint(a, pltpu.VMEM) for a in outs])
        return new_w.reshape(-1), new_m.reshape(-1), new_v.reshape(-1), params.reshape(-1)

    row_spec = P('dp', None)
    in_specs = (P('dp'), P('dp'), P('dp'), row_spec, row_spec, row_spec, row_spec, row_spec, row_spec, row_spec, row_spec, P('dp', None, None))
    out_specs = (P('dp'), P('dp'), P('dp'), P())
    return jax.shard_map(local_step, mesh=mesh, in_specs=in_specs, out_specs=out_specs, check_vma=False)
```
